32 devices in a mesh: groups: 2 (over x), expert: 16 (over z, y, core).
Axes of the slice: x: 2, y: 2, z: 4, core: 2. Of those that a mesh axis runs over, the one named last changes fastest.
Arguments:
- queries: bfloat16 [256, 4096], P(('groups', 'expert')), parts along dimension 0, may hold values from -150 to 150
- key_cache: bfloat16 [256, 64, 512], P(('groups', 'expert')), parts along dimension 0, may hold values from -7 to 7
- value_cache: bfloat16 [256, 64, 512], P(('groups', 'expert')), parts along dimension 0, may hold values from -6 to 6
- new_key: bfloat16 [256, 512], P(('groups', 'expert')), parts along dimension 0, may hold values from -6 to 6
- new_value: bfloat16 [256, 512], P(('groups', 'expert')), parts along dimension 0, may hold values from -6 to 6
- cache_lengths: int32 [256], P(('groups', 'expert')), parts along dimension 0, may hold values from 2 to 64, as said below
- hidden_in: bfloat16 [2048, 2048], P(('groups', 'expert')), parts along dimension 0, may hold values from -6 to 6
- norm_gain: bfloat16 [2048], replicated, may hold values from 0.5 to 1.5
- router_weight: bfloat16 [2048, 16], replicated, may hold values from -0.125 to 0.125
- expert_ids: int32 [2048, 8], P(('groups', 'expert')), parts along dimension 0, may hold values from 0 to 15, all different within a row; in each aligned block of 64 rows (0 to 63, 64 to 127, ...) at most 64 rows name the same one
- gate_train: bfloat16 [16, 2048, 768], P(None, 'expert'), may hold values from -0.125 to 0.125
- up_train: bfloat16 [16, 2048, 768], P(None, 'expert'), may hold values from -0.125 to 0.125
- down_train: bfloat16 [16, 768, 2048], P(None, 'expert'), may hold values from -0.21875 to 0.21875
Outputs:
- attended: bfloat16 [256, 4096], P(('groups', 'expert')), parts along dimension 0
- expert_mix: bfloat16 [2048, 2048], P(('groups', 'expert')), parts along dimension 0
The draws below stay inside these ranges and needn't reach their ends.
There are 2 independent parts, one for each index of `groups`. The reference program is written for one: setup_inputs(seed, part) draws one part's arguments, and reference() takes and returns one part's arrays. A program takes and returns all parts, laid end to end along the dimension named above; an argument that names none is the same for every part. Nothing has to cross between parts.
Inputs may be any that keep to these rules, and one draw needn't show every extreme that they name: `expert_ids`: each row names 8 different experts; within the rows of one device no expert is named more than 64 times. `cache_lengths`: the first sequence of each device's 8 has all 64 positions filled.
All inputs are finite; a program needn't handle non-finite values.
Results may differ from the reference program's by a relative error of at most 0.0074.
Values may be sent and summed in bfloat16 or wider, within the bound.
A program may use at most 128 MiB of HBM per device.

```python
import math
import jax
import jax.numpy as jnp
import numpy as np
from jax import lax

D = 2048
FF = 768
HEADS = 32
KV_HEADS = 4
HEAD_DIM = 128
TOP = 8
TOK_DEV = 64
ATT_DEV = 8
CTX = 64
EXPERTS = 16
TOKENS = 1024
SEQS = 128
CAP = 64
N_EXPERT = 16


def cache_base(key):
    return jnp.clip(jax.random.normal(jax.random.fold_in(key, 7), (SEQS, CTX, KV_HEADS * HEAD_DIM), jnp.float32), -6.0, 6.0)


def draw_key_cache(key, part):
    values = cache_base(key)
    return values.astype(jnp.bfloat16)


def draw_queries(key, part):
    values = jnp.clip(jax.random.normal(jax.random.fold_in(key, 9), (SEQS, HEADS * HEAD_DIM), jnp.float32), -6.0, 6.0)
    return values.astype(jnp.bfloat16)


def draw_cache_lengths(key, part):
    lengths = jax.random.randint(jax.random.fold_in(key, 12), (SEQS,), 2, CTX + 1, jnp.int32)
    return lengths.at[::ATT_DEV].set(CTX)


def levels(rng, shape, shards, low, top_value):
    loudness, own = 1.0, jax.random.fold_in(rng, 6)
    for dim, blocks in shards:
        heights = jnp.exp(jax.random.uniform(jax.random.fold_in(own, dim), (blocks,), jnp.float32, low / len(shards), top_value / len(shards)))
        loudness = loudness * jnp.repeat(heights, shape[dim] // blocks).reshape([-1 if axis == dim else 1 for axis in range(len(shape))])
    return loudness


def shared_out(key, own, number, rows, amount, top, bound, slope):
    order = jax.random.permutation(key, amount)
    heavy_load, common = shares(amount, rows * top, bound, slope, True), shares(amount, rows * top, bound, slope, False)
    places = jnp.arange(amount)

    def named(sizes, offset_by):
        used = int((sizes > 0).sum())
        fixed = max(1, used // 4)
        moved = fixed + (places - fixed + offset_by * (used - fixed)) % max(1, amount - fixed)
        return jnp.zeros((amount,), jnp.int32).at[order[jnp.where(places < fixed, places, moved)]].set(jnp.asarray(sizes, jnp.int32))

    sizes = jnp.where(number % 4 == 0, named(heavy_load, number // 4), named(common, number - number // 4 - 1))
    mixed = jax.random.permutation(jax.random.fold_in(own, 3), amount)
    giver, taker = mixed[0:amount // 2 * 2:2], mixed[1:amount // 2 * 2:2]
    margin = jnp.minimum(sizes[giver] - 1, bound - sizes[taker]) // 2
    margin = jnp.where((giver == order[0]) | (taker == order[0]) | (sizes[taker] == 0), 0, jnp.maximum(margin, 0))
    moved = jax.random.randint(jax.random.fold_in(own, 4), (amount // 2,), 0, 1 << 20) % (margin + 1)
    sizes = sizes.at[giver].add(-moved).at[taker].add(moved)
    labels = jnp.searchsorted(jnp.cumsum(sizes), jnp.arange(rows * top), side="right").astype(jnp.int32)
    listing = labels.reshape(top, rows).T
    listing = listing[jax.random.permutation(jax.random.fold_in(own, 1), rows)]
    offset_by = jax.random.randint(jax.random.fold_in(own, 2), (rows, 1), 0, top)
    return jnp.take_along_axis(listing, (jnp.arange(top)[None, :] + offset_by) % top, axis=1)


def shares(amount, total, reach, slope, full):
    loads = [(1 << 20) // math.isqrt(rank ** slope) + 1 for rank in range(1, amount + 1)]
    largest = reach if full else min(reach, max(-(-total // amount), total * loads[0] // sum(loads)))
    least = 1 if total - largest >= amount - 1 else 0
    holding, spare = [largest] + [least] * (amount - 1), total - largest - least * (amount - 1)
    while spare > 0:
        movable = [i for i in range(1, amount) if holding[i] < largest] or [i for i in range(1, amount) if holding[i] < reach]
        whole, left = sum([loads[i] for i in movable]), spare
        for i in movable:
            addition = min(reach - holding[i], max(1, left * loads[i] // whole), spare)
            holding[i] = holding[i] + addition
            spare = spare - addition
    return np.array(holding)


def centred(key, dims, width, limit, cuts=(), kind=jnp.bfloat16):
    result = width * jax.random.normal(key, dims, jnp.float32)
    if cuts:
        result = result * levels(key, dims, cuts, -0.22, 0.18)
    return jnp.clip(result, -limit, limit).astype(kind)


def setup_inputs(seed: int = 0, part: int = 0) -> dict:
    keys = jax.random.split(jax.random.key(seed), 14)
    part_keys = jax.random.split(jax.random.fold_in(keys[13], part), 14)
    queries = draw_queries(jax.random.fold_in(jax.random.fold_in(keys[13], part), 71), part)
    key_cache = draw_key_cache(jax.random.fold_in(jax.random.fold_in(keys[13], part), 71), part)
    value_cache = centred(part_keys[2], (SEQS, CTX, KV_HEADS * HEAD_DIM), 1.0, 6.0, ((0, 16),))
    new_key = centred(part_keys[3], (SEQS, KV_HEADS * HEAD_DIM), 1.0, 6.0, ((0, 16),))
    new_value = centred(part_keys[4], (SEQS, KV_HEADS * HEAD_DIM), 1.0, 6.0, ((0, 16),))
    cache_lengths = draw_cache_lengths(jax.random.fold_in(jax.random.fold_in(keys[13], part), 71), part)
    hidden_in = centred(part_keys[6], (TOKENS, D), 1.0, 6.0, ((0, 16),))
    norm_gain = jnp.clip(1.0 + 0.1 * jax.random.normal(keys[7], (D,), jnp.float32), 0.5, 1.5).astype(jnp.bfloat16)
    router_weight = centred(keys[8], (D, EXPERTS), D ** -0.5, 0.125)
    expert_ids_keys = jax.random.split(jax.random.fold_in(part_keys[9], 1), TOKENS // TOK_DEV)
    expert_ids_turns = jax.random.permutation(jax.random.fold_in(part_keys[9], 3), TOKENS // TOK_DEV)
    expert_ids = jax.vmap(lambda own, number: shared_out(jax.random.fold_in(part_keys[9], 2), own, number, TOK_DEV, EXPERTS, TOP, CAP, 1))(expert_ids_keys, expert_ids_turns).reshape((TOKENS, TOP))
    gate_train = centred(keys[10], (EXPERTS, D, FF), D ** -0.5, 0.125, ((1, 16),))
    up_train = centred(keys[11], (EXPERTS, D, FF), D ** -0.5, 0.125, ((1, 16),))
    down_train = centred(keys[12], (EXPERTS, FF, D), FF ** -0.5, 0.21875, ((1, 16),))
    return dict(queries=queries, key_cache=key_cache, value_cache=value_cache, new_key=new_key, new_value=new_value, cache_lengths=cache_lengths, hidden_in=hidden_in, norm_gain=norm_gain, router_weight=router_weight, expert_ids=expert_ids, gate_train=gate_train, up_train=up_train, down_train=down_train)


EPSILON = 1e-06

def rms_normed(hidden_in, norm_gain):
    values = hidden_in.astype(jnp.float32)
    mean_square = lax.optimization_barrier(jnp.mean(values * values, axis=-1, keepdims=True))
    return (values * lax.rsqrt(mean_square + EPSILON) * norm_gain.astype(jnp.float32)).astype(jnp.bfloat16)

def attend(queries, key_cache, value_cache, new_key, new_value, cache_lengths):
    seq_count = queries.shape[0]
    group_size = HEADS // KV_HEADS
    query_blocks = queries.astype(jnp.float32).reshape(seq_count, KV_HEADS, group_size, HEAD_DIM)
    cached_keys = key_cache.astype(jnp.float32).reshape(seq_count, CTX, KV_HEADS, HEAD_DIM)
    cached_values = value_cache.astype(jnp.float32).reshape(seq_count, CTX, KV_HEADS, HEAD_DIM)
    fresh_keys = new_key.astype(jnp.float32).reshape(seq_count, KV_HEADS, HEAD_DIM)
    fresh_values = new_value.astype(jnp.float32).reshape(seq_count, KV_HEADS, HEAD_DIM)
    score_scale = 1.0 / math.sqrt(HEAD_DIM)
    scores = jnp.einsum('sgrd,scgd->sgrc', query_blocks, cached_keys) * score_scale
    own_score = jnp.einsum('sgrd,sgd->sgr', query_blocks, fresh_keys) * score_scale
    positions = jnp.arange(CTX, dtype=jnp.int32)
    visible = positions[None, :] < cache_lengths.astype(jnp.int32)[:, None]
    scores = jnp.where(visible[:, None, None, :], scores, -1e+30)
    largest = jnp.maximum(lax.optimization_barrier(jnp.max(scores, axis=-1)), own_score)
    cached_exp = jnp.exp(scores - largest[..., None])
    own_exp = jnp.exp(own_score - largest)
    prob_total = lax.optimization_barrier(jnp.sum(cached_exp, axis=-1)) + own_exp
    cached_prob = lax.optimization_barrier((cached_exp / prob_total[..., None]).astype(jnp.bfloat16)).astype(jnp.float32)
    own_prob = lax.optimization_barrier((own_exp / prob_total).astype(jnp.bfloat16)).astype(jnp.float32)
    context = jnp.einsum('sgrc,scgd->sgrd', cached_prob, cached_values)
    context = context + own_prob[..., None] * fresh_values[:, :, None, :]
    return context.reshape(seq_count, HEADS * HEAD_DIM).astype(jnp.bfloat16)

def expert_block(operands):
    token_rows, gate_weight, up_weight, down_weight = operands
    gate_proj = jnp.dot(token_rows, gate_weight, preferred_element_type=jnp.float32)
    up_proj = jnp.dot(token_rows, up_weight, preferred_element_type=jnp.float32)
    hidden_units = (jax.nn.silu(gate_proj) * up_proj).astype(jnp.bfloat16)
    return jnp.dot(hidden_units, down_weight, preferred_element_type=jnp.float32).astype(jnp.bfloat16)

def mix_experts(hidden_in, norm_gain, router_weight, expert_ids, gate_train, up_train, down_train):
    normed = rms_normed(hidden_in, norm_gain)
    logits = jnp.dot(normed, router_weight, preferred_element_type=jnp.float32)
    expert_range = jnp.arange(EXPERTS, dtype=jnp.int32)
    picked = expert_ids.astype(jnp.int32)[:, :, None] == expert_range[None, None, :]
    chosen = lax.optimization_barrier(jnp.sum(jnp.where(picked, logits[:, None, :], 0.0), axis=-1))
    mixing = jax.nn.softmax(chosen, axis=-1)
    onehot_int = picked.astype(jnp.int32).reshape(N_EXPERT, TOK_DEV * TOP, EXPERTS)
    rank_values = lax.optimization_barrier(jnp.sum((jnp.cumsum(onehot_int, axis=1).astype(jnp.int32) - 1) * onehot_int, axis=-1)).astype(jnp.int32)
    sources = jnp.arange(N_EXPERT, dtype=jnp.int32)[:, None]
    slot_index = (sources * CAP + rank_values).reshape(-1).astype(jnp.int32)
    flat_ids = expert_ids.reshape(-1).astype(jnp.int32)
    repeated = jnp.repeat(normed, TOP, axis=0)
    buffers = jnp.zeros((EXPERTS, N_EXPERT * CAP, D), jnp.bfloat16).at[flat_ids, slot_index].set(repeated)
    outputs = lax.map(expert_block, (buffers, gate_train, up_train, down_train))
    returned = outputs[flat_ids, slot_index].astype(jnp.float32).reshape(TOKENS, TOP, D)
    return lax.optimization_barrier(jnp.sum(mixing[:, :, None] * returned, axis=1)).astype(jnp.bfloat16)

def reference(queries, key_cache, value_cache, new_key, new_value, cache_lengths, hidden_in, norm_gain, router_weight, expert_ids, gate_train, up_train, down_train):
    attended = attend(queries, key_cache, value_cache, new_key, new_value, cache_lengths)
    expert_mix = mix_experts(hidden_in, norm_gain, router_weight, expert_ids, gate_train, up_train, down_train)
    return (attended, expert_mix)
```

```python
import functools
import math

import jax
import jax.numpy as jnp
from jax import lax
from jax.experimental import pallas as pl
from jax.experimental.pallas import tpu as pltpu
from jax.sharding import PartitionSpec as P

HEADS = 32
KV_HEADS = 4
HEAD_DIM = 128
CTX = 64


EPSILON = 1e-06


def rms_normed(hidden_in, norm_gain):
    values = hidden_in.astype(jnp.float32)
    mean_square = jnp.mean(values * values, axis=-1, keepdims=True)
    return (values * lax.rsqrt(mean_square + EPSILON) * norm_gain.astype(jnp.float32)).astype(
        jnp.bfloat16
    )


def attend(queries, key_cache, value_cache, new_key, new_value, cache_lengths):
    seq_count = queries.shape[0]
    group_size = HEADS // KV_HEADS
    query_blocks = queries.reshape(seq_count, KV_HEADS, group_size, HEAD_DIM)
    cached_keys = key_cache.reshape(seq_count, CTX, KV_HEADS, HEAD_DIM)
    cached_values = value_cache.reshape(seq_count, CTX, KV_HEADS, HEAD_DIM)
    fresh_keys = new_key.reshape(seq_count, KV_HEADS, HEAD_DIM)
    fresh_values = new_value.astype(jnp.float32).reshape(seq_count, KV_HEADS, HEAD_DIM)
    score_scale = 1.0 / math.sqrt(HEAD_DIM)
    scores = (
        jnp.einsum("sgrd,scgd->sgrc", query_blocks, cached_keys, preferred_element_type=jnp.float32)
        * score_scale
    )
    own_score = (
        jnp.einsum("sgrd,sgd->sgr", query_blocks, fresh_keys, preferred_element_type=jnp.float32)
        * score_scale
    )
    positions = jnp.arange(CTX, dtype=jnp.int32)
    visible = positions[None, :] < cache_lengths[:, None]
    scores = jnp.where(visible[:, None, None, :], scores, -1e30)
    largest = jnp.maximum(jnp.max(scores, axis=-1), own_score)
    cached_exp = jnp.exp(scores - largest[..., None])
    own_exp = jnp.exp(own_score - largest)
    prob_total = jnp.sum(cached_exp, axis=-1) + own_exp
    cached_prob = (cached_exp / prob_total[..., None]).astype(jnp.bfloat16)
    own_prob = (own_exp / prob_total).astype(jnp.bfloat16).astype(jnp.float32)
    context = jnp.einsum(
        "sgrc,scgd->sgrd", cached_prob, cached_values, preferred_element_type=jnp.float32
    )
    context = context + own_prob[..., None] * fresh_values[:, :, None, :]
    return context.reshape(seq_count, HEADS * HEAD_DIM).astype(jnp.bfloat16)


def dense_mixing(normed, router_weight, expert_ids):
    logits = jnp.dot(normed, router_weight, preferred_element_type=jnp.float32)
    expert_range = jnp.arange(router_weight.shape[1], dtype=jnp.int32)
    picked = jnp.any(expert_ids[:, :, None] == expert_range[None, None, :], axis=1)
    masked = jnp.where(picked, logits, -jnp.inf)
    raised = jnp.exp(masked - jnp.max(masked, axis=-1, keepdims=True))
    return raised / jnp.sum(raised, axis=-1, keepdims=True)


MESH = pl.DeviceIdType.MESH
AHEAD = 4
NEAR = 4
LAG = 2


def greet(targets):
    barrier = pltpu.get_barrier_semaphore()

    expected = 0
    for condition, target in targets:
        signal = functools.partial(
            pl.semaphore_signal, barrier, inc=1, device_id=target, device_id_type=MESH
        )
        if condition is None:
            signal()
            expected = expected + 1
        else:
            pl.when(condition)(signal)
            expected = expected + condition.astype(jnp.int32)
    pl.semaphore_wait(barrier, expected)


def move_kernel(
    groups, count,
    gate_ref, up_ref, down_ref, rows_ref,
    hidden_ref, down_out, gate_out, up_out, rows_out,
    send_w, recv_w, send_x, recv_x, local_sem, send_rows, recv_rows,
):
    me = lax.axis_index("expert")
    group = lax.axis_index("groups")
    parts = max(1, groups // 2)
    part_rows = gate_ref.shape[1] // parts
    part_columns = down_ref.shape[2] // groups
    line = count // 4
    layer = me // 4

    others = [(None, (group, me ^ r)) for r in range(1, count)]
    others += [(None, (lax.rem(group + h, groups), me)) for h in range(1, groups)]
    greet(others)

    def remote(src, dst, send, recv, target):
        return pltpu.make_async_remote_copy(
            src_ref=src, dst_ref=dst, send_sem=send, recv_sem=recv, device_id=target, device_id_type=MESH
        )

    def rows_of(owner):
        return pl.ds(pl.multiple_of((owner // 2) * part_rows, part_rows), part_rows)

    def columns_of(owner):
        return pl.ds(pl.multiple_of(owner * part_columns, part_columns), part_columns)

    def row_copy(kind, block, target, own=False):
        source = rows_ref if own else rows_out.at[block]
        return remote(
            source, rows_out.at[block], send_rows.at[kind, block], recv_rows.at[block], (group, target)
        )

    def row_wait(block):
        row_copy(0, block, me ^ 1).wait_recv()

    own_rows = pltpu.make_async_copy(rows_ref, rows_out.at[me], local_sem.at[3])
    own_rows.start()
    has_up, has_down = me + 4 < count, me >= 4

    @pl.when(has_up)
    def _():
        row_copy(0, me, me + 4, True).start()

    @pl.when(has_down)
    def _():
        row_copy(1, me, me - 4, True).start()

    row_copy(2, me, me ^ 2, True).start()
    row_copy(3, me, me ^ 1, True).start()

    def line_step(step):
        below, above = me - 4 * (step + 1), me + 4 * (step + 1)

        @pl.when(below >= 0)
        def _():
            row_wait(below)

            @pl.when(has_up)
            def _():
                row_copy(0, below, me + 4).start()

            row_copy(2, below, me ^ 2).start()
            row_copy(3, below, me ^ 1).start()

        @pl.when(above < count)
        def _():
            row_wait(above)

            @pl.when(has_down)
            def _():
                row_copy(1, above, me - 4).start()

            row_copy(2, above, me ^ 2).start()
            row_copy(3, above, me ^ 1).start()

    def side_step(index):
        block = lax.rem(me, 4) ^ 2
        block = block + 4 * index
        row_wait(block)
        row_copy(3, block, me ^ 1).start()

    def across(kind, r, refs_in, refs_out, which):
        target = me ^ r
        if r < NEAR:
            a, b = ((gate_ref, gate_out), (down_ref, down_out), (up_ref, up_out))[kind]
            send = send_x.at[0, r, 0] if kind == 2 else send_w.at[kind, r]
            recv = recv_x.at[0, r, 0] if kind == 2 else recv_w.at[kind, r]
            return remote(a.at[target], b.at[me], send, recv, (group, target))
        if kind == 0:
            return remote(
                refs_in[which].at[target, rows_of(group)], refs_out[which].at[me, rows_of(group)],
                send_w.at[0, r], recv_w.at[0, r], (group, target),
            )
        return remote(
            down_ref.at[target, :, columns_of(group)], down_out.at[me, :, columns_of(group)],
            send_w.at[1, r], recv_w.at[1, r], (group, target),
        )

    ins, outs = (gate_ref, up_ref), (gate_out, up_out)

    def by_matrix(act):
        pl.when(lax.rem(group, 2) == 0)(functools.partial(act, 0))
        pl.when(lax.rem(group, 2) == 1)(functools.partial(act, 1))

    def start_weight(kind, r):
        if kind == 0 and r >= NEAR:
            by_matrix(lambda which: across(0, r, ins, outs, which).start())
        else:
            across(kind, r, ins, outs, 0).start()

    def onward(kind, r, h, which):
        held = me ^ r
        place = outs[which].at[held, rows_of(group)] if kind == 0 else down_out.at[held, :, columns_of(group)]
        return remote(
            place, place, send_x.at[kind, r, h - 1], recv_x.at[kind, r, h - 1],
            (lax.rem(group + h, groups), me),
        )

    def pass_on(kind, r):
        across(kind, r, ins, outs, 0).wait_recv()
        for h in range(1, groups if r >= NEAR else 1):
            if kind == 0:
                by_matrix(lambda which: onward(0, r, h, which).start())
            else:
                onward(1, r, h, 0).start()

    own_copies = [
        pltpu.make_async_copy(a.at[me], b.at[me], local_sem.at[i])
        for i, (a, b) in enumerate(((gate_ref, gate_out), (up_ref, up_out), (down_ref, down_out)))
    ]
    width = gate_ref.shape[1] * count

    def ready():
        for index in range(line):
            for y in range(2):
                row_wait(4 * index + 2 * y + (lax.rem(me, 2) ^ 1))
        own_rows.wait()
        for copy in own_copies[:2]:
            copy.wait()
        for r in order:
            for h in range(1, groups if r >= NEAR else 1):
                onward(0, r, h, 0).wait_recv()

    def expert_rows(quarter):
        @pl.loop(0, count // 16)
        def _(step):
            at = quarter * (count // 4) + step * 4
            rows = rows_out[pl.ds(at, 4)].reshape(-1, rows_out.shape[2])
            tokens = rows[:, :width]
            shares = rows[:, width:].astype(jnp.float32)
            lane = lax.broadcasted_iota(jnp.int32, shares.shape, 1)
            own = jnp.logical_or(lane == me, lane == me + count)
            own_mix = jnp.sum(jnp.where(own, shares, 0.0), axis=1, keepdims=True)
            gate = gate_out[...].reshape(width, -1)
            gate_proj = jnp.dot(tokens, gate, preferred_element_type=jnp.float32)
            up = up_out[...].reshape(width, -1)
            up_proj = jnp.dot(tokens, up, preferred_element_type=jnp.float32)
            hidden = gate_proj / (1.0 + jnp.exp(-gate_proj)) * up_proj * own_mix
            place = pl.ds(pl.multiple_of(at * rows_out.shape[1], rows.shape[0]), rows.shape[0])
            hidden_ref[place, :] = hidden.astype(hidden_ref.dtype)

    half = count // 2
    order = [r for i in range(half) for r in ((half + i, i) if i else (half,))]
    first = [(kind, r) for r in order for kind in ((0, 2) if r < NEAR else (0,))]
    items = first + [(1, r) for r in order]
    spacing = len(items) // (line + 1)
    side_at = 2 + spacing * (line - 1) + 3

    def advance(i):
        pass_on(*items[i])
        before_last = len(items) - 1 - i
        if before_last % 2 == 0 and before_last < 8:
            if before_last == 6:
                ready()
            expert_rows(3 - before_last // 2)

    for i, item in enumerate(items):
        start_weight(*item)
        if i >= 2 and (i - 2) % spacing == 0 and (i - 2) // spacing < line - 1:
            line_step((i - 2) // spacing)
        if i == side_at:
            for index in range(line):
                side_step(index)
        if i == AHEAD:
            for copy in own_copies:
                copy.start()
        if i >= AHEAD:
            advance(i - AHEAD)
    for i in range(len(items) - AHEAD, len(items)):
        advance(i)

    own_copies[2].wait()
    for kind, r in items:
        across(kind, r, ins, outs, 0).wait_send()
        for h in range(1, groups if r >= NEAR else 1):
            onward(kind, r, h, 0).wait_send()
            if kind == 1:
                onward(kind, r, h, 0).wait_recv()
    for index in range(line):
        block = lax.rem(me, 4) + 4 * index

        @pl.when(jnp.logical_and(has_up, index <= layer))
        def _():
            row_copy(0, block, me ^ 1).wait_send()

        @pl.when(jnp.logical_and(has_down, index >= layer))
        def _():
            row_copy(1, block, me ^ 1).wait_send()

        row_copy(2, block, me ^ 1).wait_send()
        row_copy(3, block, me ^ 1).wait_send()
        row_copy(3, block ^ 2, me ^ 1).wait_send()


def move(groups, gate_train, up_train, down_train, row_block):
    count = gate_train.shape[0]
    anywhere = pl.BlockSpec(memory_space=pl.ANY)
    DMA = pltpu.SemaphoreType.DMA
    return pl.pallas_call(
        functools.partial(move_kernel, groups, count),
        out_shape=[
            jax.ShapeDtypeStruct((count * row_block.shape[0], gate_train.shape[2]), jnp.bfloat16),
            jax.ShapeDtypeStruct(down_train.shape, down_train.dtype),
        ],
        in_specs=[anywhere, anywhere, anywhere, pl.BlockSpec(memory_space=pltpu.VMEM)],
        out_specs=[pl.BlockSpec(memory_space=pltpu.VMEM), anywhere],
        scratch_shapes=[
            pltpu.VMEM(gate_train.shape, gate_train.dtype),
            pltpu.VMEM(up_train.shape, up_train.dtype),
            pltpu.VMEM((count,) + row_block.shape, row_block.dtype),
            DMA((2, count)), DMA((2, count)),
            DMA((2, count, max(1, groups - 1))), DMA((2, count, max(1, groups - 1))),
            DMA((4,)), DMA((4, count)), DMA((count,)),
        ],
        compiler_params=pltpu.CompilerParams(collective_id=0, has_side_effects=True, vmem_limit_bytes=60 * 2**20),
    )(gate_train, up_train, down_train, row_block)


def sum_kernel(
    count, part_ref, out_ref, core_in, side_in, up_in, down_in, side_out, up_out, down_out,
    core_send, core_recv, side_send, side_recv, up_send, up_recv, down_send, down_recv,
):
    me = lax.axis_index("expert")
    group = lax.axis_index("groups")
    line, layer = count // 4, me // 4
    place = lax.rem(me, 4)
    side, core = place // 2, lax.rem(place, 2)
    has_up, has_down = me + 4 < count, me >= 4
    greet([
        (None, (group, me ^ 1)), (None, (group, me ^ 2)),
        (has_up, (group, me + 4)), (has_down, (group, me - 4)),
    ])
    chunk = 16
    row_count = part_ref.shape[1]

    def remote(src, dst, send, recv, target):
        return pltpu.make_async_remote_copy(
            src_ref=src, dst_ref=dst, send_sem=send, recv_sem=recv, device_id=(group, target), device_id_type=MESH
        )

    def add(target, *sources):
        @pl.loop(0, row_count // chunk)
        def _(step):
            rows = pl.ds(pl.multiple_of(step * chunk, chunk), chunk)
            total = sources[0][rows, :].astype(jnp.float32)
            for source in sources[1:]:
                total = total + source[rows, :].astype(jnp.float32)
            target[rows, :] = total.astype(target.dtype)

    def core_copy(at, y):
        slot = at * 2 + y
        return remote(
            part_ref.at[at * 4 + y * 2 + (core ^ 1)], core_in.at[slot], core_send.at[slot], core_recv.at[slot], me ^ 1
        )

    def side_copy(at):
        return remote(side_out.at[at], side_in.at[at], side_send.at[at], side_recv.at[at], me ^ 2)

    def up_copy(at):
        return remote(up_out.at[at], up_in.at[at], up_send.at[at], up_recv.at[at], me + 4)

    def down_copy(at):
        return remote(down_out.at[at], down_in.at[at], down_send.at[at], down_recv.at[at], me - 4)

    def in_order(act):
        for d in range(line - 1, 0, -1):
            pl.when(layer + d < line)(functools.partial(act, layer + d, 1))
            pl.when(layer - d >= 0)(functools.partial(act, layer - d, -1))
        act(layer, 0)

    in_order(lambda at, way: core_copy(at, side ^ 1).start())
    in_order(lambda at, way: core_copy(at, side).start())

    def to_side(at, way):
        core_copy(at, side ^ 1).wait_recv()
        add(side_out.at[at], part_ref.at[at * 4 + (side ^ 1) * 2 + core], core_in.at[at * 2 + (side ^ 1)])
        side_copy(at).start()

    in_order(to_side)

    def along(at, way):
        core_copy(at, side).wait_recv()
        side_copy(at).wait_recv()
        mine = (part_ref.at[at * 4 + place], core_in.at[at * 2 + side], side_in.at[at])
        if way == 1:
            @pl.when(has_down)
            def _():
                up_copy(at).wait_recv()
                add(up_out.at[at], *mine, up_in.at[at])

            @pl.when(jnp.logical_not(has_down))
            def _():
                add(up_out.at[at], *mine)

            up_copy(at).start()
        elif way == -1:
            @pl.when(has_up)
            def _():
                down_copy(at).wait_recv()
                add(down_out.at[at], *mine, down_in.at[at])

            @pl.when(jnp.logical_not(has_up))
            def _():
                add(down_out.at[at], *mine)

            down_copy(at).start()
        else:
            @pl.when(has_down)
            def _():
                up_copy(at).wait_recv()

            @pl.when(has_up)
            def _():
                down_copy(at).wait_recv()

            both = jnp.logical_and(has_down, has_up)

            @pl.when(both)
            def _():
                add(out_ref, *mine, up_in.at[at], down_in.at[at])

            @pl.when(jnp.logical_and(has_down, jnp.logical_not(has_up)))
            def _():
                add(out_ref, *mine, up_in.at[at])

            @pl.when(jnp.logical_and(has_up, jnp.logical_not(has_down)))
            def _():
                add(out_ref, *mine, down_in.at[at])

            @pl.when(jnp.logical_not(jnp.logical_or(has_up, has_down)))
            def _():
                add(out_ref, *mine)

    in_order(along)

    def finish(at, way):
        core_copy(at, side ^ 1).wait_send()
        core_copy(at, side).wait_send()
        side_copy(at).wait_send()
        if way == 1:
            up_copy(at).wait_send()
        if way == -1:
            down_copy(at).wait_send()

    in_order(finish)


def summed(partial_out, count):
    rows, width = partial_out.shape[0] // count, partial_out.shape[1]
    line = count // 4
    DMA = pltpu.SemaphoreType.DMA
    block = lambda amount: pltpu.VMEM((amount, rows, width), jnp.bfloat16)
    return pl.pallas_call(
        functools.partial(sum_kernel, count),
        out_shape=jax.ShapeDtypeStruct((rows, width), jnp.bfloat16),
        in_specs=[pl.BlockSpec(memory_space=pltpu.VMEM)],
        out_specs=pl.BlockSpec(memory_space=pltpu.VMEM),
        scratch_shapes=[block(count // 2)] + [block(line)] * 6
        + [DMA((count // 2,)), DMA((count // 2,))] + [DMA((line,))] * 6,
        compiler_params=pltpu.CompilerParams(collective_id=1, has_side_effects=True, vmem_limit_bytes=60 * 2**20),
    )(partial_out.reshape(count, rows, width))


def dims_fit(groups, count, gate_train, down_train, row_count):
    rows, width = gate_train.shape[1], gate_train.shape[2]
    part = down_train.shape[1]
    return (
        groups == 2
        and count % 8 == 0
        and 2 * count <= 128
        and rows % 128 == 0
        and part % 16 == 0
        and part * count == width
        and width % 256 == 0
        and row_count % 16 == 0
        and (count * row_count) % 512 == 0
    )


def hidden_kernel(
    count, hid_ref, gain_ref, router_ref, ids_ref, gate_ref, up_ref,
    hidden_ref, load, stage, wt, rows, acc,
    load_sem, send_w, recv_w, send_x, recv_x, send_rows, recv_rows,
):
    me = lax.axis_index("expert")
    group = lax.axis_index("groups")
    other_group = 1 - group
    line = count // 4
    layer = me // 4
    row_count, width = hid_ref.shape
    depth = gate_ref.shape[1]
    part = stage.shape[2] // count
    total_f = stage.shape[2]
    tokens = count * row_count

    def loading(m, e):
        return pltpu.make_async_copy((gate_ref, up_ref)[m].at[e], load.at[m, e], load_sem.at[m, e])

    for e in range(count):
        for m in range(2):
            loading(m, e).start()

    barrier = pltpu.get_barrier_semaphore()
    peers = [(group, me ^ r) for r in range(1, count)] + [(other_group, me)]
    for peer in peers:
        pl.semaphore_signal(barrier, inc=1, device_id=peer, device_id_type=MESH)

    values = hid_ref[...].astype(jnp.float32)
    mean_square = jnp.mean(values * values, axis=-1, keepdims=True)
    normed = (values * lax.rsqrt(mean_square + EPSILON) * gain_ref[...].astype(jnp.float32)).astype(jnp.bfloat16)
    rows[me, :, :width] = normed
    logits = jnp.dot(normed, router_ref[...], preferred_element_type=jnp.float32)
    lane = lax.broadcasted_iota(jnp.int32, logits.shape, 1)
    picked = ids_ref[:, 0:1] == lane
    for k in range(1, ids_ref.shape[1]):
        picked = jnp.logical_or(picked, ids_ref[:, k : k + 1] == lane)
    masked = jnp.where(picked, logits, -jnp.inf)
    raised = jnp.exp(masked - jnp.max(masked, axis=-1, keepdims=True))
    mixing = raised / jnp.sum(raised, axis=-1, keepdims=True)
    high = mixing.astype(jnp.bfloat16)
    low = (mixing - high.astype(jnp.float32)).astype(jnp.bfloat16)
    source = lax.broadcasted_iota(jnp.int32, (count, 128), 0)
    place = lax.broadcasted_iota(jnp.int32, (count, 128), 1)
    at_high = jnp.where(place == source, 1.0, 0.0).astype(jnp.bfloat16)
    at_low = jnp.where(place == source + count, 1.0, 0.0).astype(jnp.bfloat16)
    shares = jnp.dot(high, at_high, preferred_element_type=jnp.float32) + jnp.dot(
        low, at_low, preferred_element_type=jnp.float32
    )
    rows[me, :, width:] = shares.astype(jnp.bfloat16)

    pl.semaphore_wait(barrier, len(peers))

    def remote(src, dst, send, recv, target):
        return pltpu.make_async_remote_copy(
            src_ref=src, dst_ref=dst, send_sem=send, recv_sem=recv, device_id=target, device_id_type=MESH
        )

    def row_copy(kind, block, target):
        return remote(
            rows.at[block], rows.at[block], send_rows.at[kind, block], recv_rows.at[block], (group, target)
        )

    def row_wait(block):
        row_copy(0, block, me ^ 1).wait_recv()

    has_up, has_down = me + 4 < count, me >= 4

    @pl.when(has_up)
    def _():
        row_copy(0, me, me + 4).start()

    @pl.when(has_down)
    def _():
        row_copy(1, me, me - 4).start()

    row_copy(2, me, me ^ 2).start()
    row_copy(3, me, me ^ 1).start()

    def line_step(step):
        below, above = me - 4 * (step + 1), me + 4 * (step + 1)

        @pl.when(below >= 0)
        def _():
            row_wait(below)

            @pl.when(has_up)
            def _():
                row_copy(0, below, me + 4).start()

            row_copy(2, below, me ^ 2).start()
            row_copy(3, below, me ^ 1).start()

        @pl.when(above < count)
        def _():
            row_wait(above)

            @pl.when(has_down)
            def _():
                row_copy(1, above, me - 4).start()

            row_copy(2, above, me ^ 2).start()
            row_copy(3, above, me ^ 1).start()

    def side_step():
        for index in range(line):
            block = (lax.rem(me, 4) ^ 2) + 4 * index
            row_wait(block)
            row_copy(3, block, me ^ 1).start()

    def rows_ready():
        for index in range(line):
            for y in range(2):
                row_wait(4 * index + 2 * y + (lax.rem(me, 2) ^ 1))

    def lanes_of(owner):
        return pl.ds(pl.multiple_of(owner * depth, depth), depth)

    def across(m, r):
        target = me ^ r
        index = m if r < NEAR else group
        slot = m if r < NEAR else 0
        return remote(
            stage.at[index, target], wt.at[index, :, lanes_of(me)],
            send_w.at[slot, r], recv_w.at[slot, r], (group, target),
        )

    def onward(r):
        held = me ^ r
        ref = wt.at[group, :, lanes_of(held)]
        return remote(ref, ref, send_x.at[r], recv_x.at[r], (other_group, me))

    def start_weight(r):
        for m in range(2 if r < NEAR else 1):
            across(m, r).start()

    def pass_on(r):
        for m in range(2 if r < NEAR else 1):
            across(m, r).wait_recv()
        if r >= NEAR:
            onward(r).start()

    @pl.loop(0, count)
    def _(e):
        for m in range(2):
            loading(m, e).wait()
            turned = load[m, e].T.reshape(count, part, depth)
            stage[m, :, pl.ds(pl.multiple_of(e * part, part), part), :] = turned

    for m in range(2):
        wt[m, :, lanes_of(me)] = stage[m, me]

    tile = 256
    tiles = total_f // tile
    chunk = 512
    chunks = tokens // chunk
    blocks = chunk // row_count

    def accumulate(r, first):
        for q in (r, r ^ 1):
            if q >= NEAR:
                onward(q).wait_recv()
        base = pl.multiple_of(((me ^ r) // 2) * (2 * depth), 2 * depth)

        @pl.loop(0, 2 * tiles)
        def _(step):
            m, n = step // tiles, step % tiles
            weight = wt[m, pl.ds(pl.multiple_of(n * tile, tile), tile), pl.ds(base, 2 * depth)]

            @pl.loop(0, chunks)
            def _(c):
                x = rows[pl.ds(c * blocks, blocks), :, pl.ds(base, 2 * depth)].reshape(chunk, 2 * depth)
                product = lax.dot_general(
                    x, weight, (((1,), (1,)), ((), ())), preferred_element_type=jnp.float32
                )
                at = pl.ds(pl.multiple_of(c * chunk, chunk), chunk)
                if first:
                    acc[step, at, :] = product
                else:
                    acc[step, at, :] = acc[step, at, :] + product

    half = count // 2
    order = [r for i in range(half) for r in ((half + i, i) if i else (half,))]
    passed, pending, done = {0}, [], 0
    side_at = 2 * line

    def after(i):
        nonlocal done
        r = order[i]
        pass_on(r)
        passed.add(r)
        if r ^ 1 in passed:
            pending.append((i, r))

    started_rows = False

    def compute(i):
        nonlocal done, started_rows
        while pending and (pending[0][0] + LAG <= i):
            _, r = pending.pop(0)
            if not started_rows:
                rows_ready()
                started_rows = True
            accumulate(r, done == 0)
            done += 1

    for i, r in enumerate(order):
        start_weight(r)
        if i % 2 == 1 and i // 2 < line - 1:
            line_step(i // 2)
        if i == side_at:
            side_step()
        if i >= AHEAD:
            after(i - AHEAD)
            if i > side_at:
                compute(i - AHEAD)
    for i in range(len(order) - AHEAD, len(order)):
        after(i)
        compute(i)
    compute(len(order) + LAG)

    spread_at = lax.broadcasted_iota(jnp.int32, (128, total_f), 0)
    column = lax.broadcasted_iota(jnp.int32, (128, total_f), 1)
    expert = jnp.where(spread_at < count, spread_at, spread_at - count)
    inside = jnp.logical_and(column >= expert * part, column < expert * part + part)
    spread = jnp.where(jnp.logical_and(inside, spread_at < 2 * count), 1.0, 0.0).astype(jnp.bfloat16)

    @pl.loop(0, count)
    def _(b):
        mix = jnp.dot(rows[b, :, width:], spread, preferred_element_type=jnp.float32)
        at = pl.ds(pl.multiple_of(b * row_count, row_count), row_count)
        for n in range(tiles):
            gate_proj = acc[n, at, :]
            up_proj = acc[tiles + n, at, :]
            columns = slice(n * tile, (n + 1) * tile)
            hidden = gate_proj / (1.0 + jnp.exp(-gate_proj)) * up_proj * mix[:, columns]
            hidden_ref[at, columns] = hidden.astype(hidden_ref.dtype)

    for r in order:
        for m in range(2 if r < NEAR else 1):
            across(m, r).wait_send()
        if r >= NEAR:
            onward(r).wait_send()
    for index in range(line):
        block = lax.rem(me, 4) + 4 * index

        @pl.when(jnp.logical_and(has_up, index <= layer))
        def _():
            row_copy(0, block, me ^ 1).wait_send()

        @pl.when(jnp.logical_and(has_down, index >= layer))
        def _():
            row_copy(1, block, me ^ 1).wait_send()

        row_copy(2, block, me ^ 1).wait_send()
        row_copy(3, block, me ^ 1).wait_send()
        row_copy(3, block ^ 2, me ^ 1).wait_send()


def hidden_units_of(hidden_in, norm_gain, router_weight, expert_ids, gate_train, up_train):
    count, depth, total_f = gate_train.shape
    row_count, width = hidden_in.shape
    anywhere = pl.BlockSpec(memory_space=pl.ANY)
    near = pl.BlockSpec(memory_space=pltpu.VMEM)
    DMA = pltpu.SemaphoreType.DMA
    return pl.pallas_call(
        functools.partial(hidden_kernel, count),
        out_shape=jax.ShapeDtypeStruct((count * row_count, total_f), jnp.bfloat16),
        in_specs=[near, near, near, near, anywhere, anywhere],
        out_specs=near,
        scratch_shapes=[
            pltpu.VMEM((2, count, depth, total_f), jnp.bfloat16),
            pltpu.VMEM((2, count, total_f, depth), jnp.bfloat16),
            pltpu.VMEM((2, total_f, count * depth), jnp.bfloat16),
            pltpu.VMEM((count, row_count, width + 128), jnp.bfloat16),
            pltpu.VMEM((2 * total_f // 256, count * row_count, 256), jnp.float32),
            DMA((2, count)), DMA((2, count)), DMA((2, count)), DMA((count,)), DMA((count,)),
            DMA((4, count)), DMA((count,)),
        ],
        compiler_params=pltpu.CompilerParams(collective_id=2, has_side_effects=True, vmem_limit_bytes=60 * 2**20),
    )(hidden_in, norm_gain.reshape(1, width), router_weight, expert_ids, gate_train, up_train)


def local(
    queries,
    key_cache,
    value_cache,
    new_key,
    new_value,
    cache_lengths,
    hidden_in,
    norm_gain,
    router_weight,
    expert_ids,
    gate_train,
    up_train,
    down_train,
):
    width = hidden_in.shape[1]
    expert_count = router_weight.shape[1]
    groups = lax.axis_size("groups")
    if dims_fit(groups, expert_count, gate_train, down_train, hidden_in.shape[0]):
        hidden_units = hidden_units_of(hidden_in, norm_gain, router_weight, expert_ids, gate_train, up_train)
        down_moved = down_train
    else:
        normed = rms_normed(hidden_in, norm_gain)
        mixing = dense_mixing(normed, router_weight, expert_ids)
        mixing_high = mixing.astype(jnp.bfloat16)
        mixing_low = (mixing - mixing_high.astype(jnp.float32)).astype(jnp.bfloat16)
        spare = -2 * expert_count % 128
        row_block = jnp.concatenate(
            [normed, mixing_high, mixing_low, jnp.zeros((normed.shape[0], spare), jnp.bfloat16)], axis=1
        )
        hidden_units, down_moved = move(groups, gate_train, up_train, down_train, row_block)
    down_moved = down_moved.reshape(-1, width)
    attended = attend(queries, key_cache, value_cache, new_key, new_value, cache_lengths)
    partial_out = jnp.dot(hidden_units, down_moved, preferred_element_type=jnp.float32).astype(jnp.bfloat16)
    mixed_out = summed(partial_out, expert_count)
    return (attended, mixed_out)


def solution(mesh):
    placed = (
        P(("groups", "expert"), None),
        P(("groups", "expert"), None, None),
        P(("groups", "expert"), None, None),
        P(("groups", "expert"), None),
        P(("groups", "expert"), None),
        P(("groups", "expert")),
        P(("groups", "expert"), None),
        P(),
        P(),
        P(("groups", "expert"), None),
        P(None, "expert", None),
        P(None, "expert", None),
        P(None, "expert", None),
    )
    return jax.shard_map(
        local,
        mesh=mesh,
        in_specs=placed,
        out_specs=(P(("groups", "expert"), None), P(("groups", "expert"), None)),
        check_vma=False,
    )
```

```python
import functools
import math

import jax
import jax.numpy as jnp
from jax import lax
from jax.experimental import pallas as pl
from jax.experimental.pallas import tpu as pltpu
from jax.sharding import PartitionSpec as P

HEADS = 32
KV_HEADS = 4
HEAD_DIM = 128
CTX = 64


EPSILON = 1e-06


def rms_normed(hidden_in, norm_gain):
    values = hidden_in.astype(jnp.float32)
    mean_square = jnp.mean(values * values, axis=-1, keepdims=True)
    return (values * lax.rsqrt(mean_square + EPSILON) * norm_gain.astype(jnp.float32)).astype(
        jnp.bfloat16
    )


def attend(queries, key_cache, value_cache, new_key, new_value, cache_lengths):
    seq_count = queries.shape[0]
    group_size = HEADS // KV_HEADS
    query_blocks = queries.reshape(seq_count, KV_HEADS, group_size, HEAD_DIM)
    cached_keys = key_cache.reshape(seq_count, CTX, KV_HEADS, HEAD_DIM)
    cached_values = value_cache.reshape(seq_count, CTX, KV_HEADS, HEAD_DIM)
    fresh_keys = new_key.reshape(seq_count, KV_HEADS, HEAD_DIM)
    fresh_values = new_value.astype(jnp.float32).reshape(seq_count, KV_HEADS, HEAD_DIM)
    score_scale = 1.0 / math.sqrt(HEAD_DIM)
    scores = (
        jnp.einsum("sgrd,scgd->sgrc", query_blocks, cached_keys, preferred_element_type=jnp.float32)
        * score_scale
    )
    own_score = (
        jnp.einsum("sgrd,sgd->sgr", query_blocks, fresh_keys, preferred_element_type=jnp.float32)
        * score_scale
    )
    positions = jnp.arange(CTX, dtype=jnp.int32)
    visible = positions[None, :] < cache_lengths[:, None]
    scores = jnp.where(visible[:, None, None, :], scores, -1e30)
    largest = jnp.maximum(jnp.max(scores, axis=-1), own_score)
    cached_exp = jnp.exp(scores - largest[..., None])
    own_exp = jnp.exp(own_score - largest)
    prob_total = jnp.sum(cached_exp, axis=-1) + own_exp
    cached_prob = (cached_exp / prob_total[..., None]).astype(jnp.bfloat16)
    own_prob = (own_exp / prob_total).astype(jnp.bfloat16).astype(jnp.float32)
    context = jnp.einsum(
        "sgrc,scgd->sgrd", cached_prob, cached_values, preferred_element_type=jnp.float32
    )
    context = context + own_prob[..., None] * fresh_values[:, :, None, :]
    return context.reshape(seq_count, HEADS * HEAD_DIM).astype(jnp.bfloat16)


def dense_mixing(normed, router_weight, expert_ids):
    logits = jnp.dot(normed, router_weight, preferred_element_type=jnp.float32)
    expert_range = jnp.arange(router_weight.shape[1], dtype=jnp.int32)
    picked = jnp.any(expert_ids[:, :, None] == expert_range[None, None, :], axis=1)
    masked = jnp.where(picked, logits, -jnp.inf)
    raised = jnp.exp(masked - jnp.max(masked, axis=-1, keepdims=True))
    return raised / jnp.sum(raised, axis=-1, keepdims=True)


MESH = pl.DeviceIdType.MESH
AHEAD = 4
NEAR = 4
LAG = 2


def greet(targets):
    barrier = pltpu.get_barrier_semaphore()

    expected = 0
    for condition, target in targets:
        signal = functools.partial(
            pl.semaphore_signal, barrier, inc=1, device_id=target, device_id_type=MESH
        )
        if condition is None:
            signal()
            expected = expected + 1
        else:
            pl.when(condition)(signal)
            expected = expected + condition.astype(jnp.int32)
    pl.semaphore_wait(barrier, expected)


def move_kernel(
    groups, count,
    gate_ref, up_ref, down_ref, rows_ref,
    hidden_ref, down_out, gate_out, up_out, rows_out,
    send_w, recv_w, send_x, recv_x, local_sem, send_rows, recv_rows,
):
    me = lax.axis_index("expert")
    group = lax.axis_index("groups")
    parts = max(1, groups // 2)
    part_rows = gate_ref.shape[1] // parts
    part_columns = down_ref.shape[2] // groups
    line = count // 4
    layer = me // 4

    others = [(None, (group, me ^ r)) for r in range(1, count)]
    others += [(None, (lax.rem(group + h, groups), me)) for h in range(1, groups)]
    greet(others)

    def remote(src, dst, send, recv, target):
        return pltpu.make_async_remote_copy(
            src_ref=src, dst_ref=dst, send_sem=send, recv_sem=recv, device_id=target, device_id_type=MESH
        )

    def rows_of(owner):
        return pl.ds(pl.multiple_of((owner // 2) * part_rows, part_rows), part_rows)

    def columns_of(owner):
        return pl.ds(pl.multiple_of(owner * part_columns, part_columns), part_columns)

    def row_copy(kind, block, target, own=False):
        source = rows_ref if own else rows_out.at[block]
        return remote(
            source, rows_out.at[block], send_rows.at[kind, block], recv_rows.at[block], (group, target)
        )

    def row_wait(block):
        row_copy(0, block, me ^ 1).wait_recv()

    own_rows = pltpu.make_async_copy(rows_ref, rows_out.at[me], local_sem.at[3])
    own_rows.start()
    has_up, has_down = me + 4 < count, me >= 4

    @pl.when(has_up)
    def _():
        row_copy(0, me, me + 4, True).start()

    @pl.when(has_down)
    def _():
        row_copy(1, me, me - 4, True).start()

    row_copy(2, me, me ^ 2, True).start()
    row_copy(3, me, me ^ 1, True).start()

    def line_step(step):
        below, above = me - 4 * (step + 1), me + 4 * (step + 1)

        @pl.when(below >= 0)
        def _():
            row_wait(below)

            @pl.when(has_up)
            def _():
                row_copy(0, below, me + 4).start()

            row_copy(2, below, me ^ 2).start()
            row_copy(3, below, me ^ 1).start()

        @pl.when(above < count)
        def _():
            row_wait(above)

            @pl.when(has_down)
            def _():
                row_copy(1, above, me - 4).start()

            row_copy(2, above, me ^ 2).start()
            row_copy(3, above, me ^ 1).start()

    def side_step(index):
        block = lax.rem(me, 4) ^ 2
        block = block + 4 * index
        row_wait(block)
        row_copy(3, block, me ^ 1).start()

    def across(kind, r, refs_in, refs_out, which):
        target = me ^ r
        if r < NEAR:
            a, b = ((gate_ref, gate_out), (down_ref, down_out), (up_ref, up_out))[kind]
            send = send_x.at[0, r, 0] if kind == 2 else send_w.at[kind, r]
            recv = recv_x.at[0, r, 0] if kind == 2 else recv_w.at[kind, r]
            return remote(a.at[target], b.at[me], send, recv, (group, target))
        if kind == 0:
            return remote(
                refs_in[which].at[target, rows_of(group)], refs_out[which].at[me, rows_of(group)],
                send_w.at[0, r], recv_w.at[0, r], (group, target),
            )
        return remote(
            down_ref.at[target, :, columns_of(group)], down_out.at[me, :, columns_of(group)],
            send_w.at[1, r], recv_w.at[1, r], (group, target),
        )

    ins, outs = (gate_ref, up_ref), (gate_out, up_out)

    def by_matrix(act):
        pl.when(lax.rem(group, 2) == 0)(functools.partial(act, 0))
        pl.when(lax.rem(group, 2) == 1)(functools.partial(act, 1))

    def start_weight(kind, r):
        if kind == 0 and r >= NEAR:
            by_matrix(lambda which: across(0, r, ins, outs, which).start())
        else:
            across(kind, r, ins, outs, 0).start()

    def onward(kind, r, h, which):
        held = me ^ r
        place = outs[which].at[held, rows_of(group)] if kind == 0 else down_out.at[held, :, columns_of(group)]
        return remote(
            place, place, send_x.at[kind, r, h - 1], recv_x.at[kind, r, h - 1],
            (lax.rem(group + h, groups), me),
        )

    def pass_on(kind, r):
        across(kind, r, ins, outs, 0).wait_recv()
        for h in range(1, groups if r >= NEAR else 1):
            if kind == 0:
                by_matrix(lambda which: onward(0, r, h, which).start())
            else:
                onward(1, r, h, 0).start()

    own_copies = [
        pltpu.make_async_copy(a.at[me], b.at[me], local_sem.at[i])
        for i, (a, b) in enumerate(((gate_ref, gate_out), (up_ref, up_out), (down_ref, down_out)))
    ]
    width = gate_ref.shape[1] * count

    def ready():
        for index in range(line):
            for y in range(2):
                row_wait(4 * index + 2 * y + (lax.rem(me, 2) ^ 1))
        own_rows.wait()
        for copy in own_copies[:2]:
            copy.wait()
        for r in order:
            for h in range(1, groups if r >= NEAR else 1):
                onward(0, r, h, 0).wait_recv()

    def expert_rows(quarter):
        @pl.loop(0, count // 16)
        def _(step):
            at = quarter * (count // 4) + step * 4
            rows = rows_out[pl.ds(at, 4)].reshape(-1, rows_out.shape[2])
            tokens = rows[:, :width]
            shares = rows[:, width:].astype(jnp.float32)
            lane = lax.broadcasted_iota(jnp.int32, shares.shape, 1)
            own = jnp.logical_or(lane == me, lane == me + count)
            own_mix = jnp.sum(jnp.where(own, shares, 0.0), axis=1, keepdims=True)
            gate = gate_out[...].reshape(width, -1)
            gate_proj = jnp.dot(tokens, gate, preferred_element_type=jnp.float32)
            up = up_out[...].reshape(width, -1)
            up_proj = jnp.dot(tokens, up, preferred_element_type=jnp.float32)
            hidden = gate_proj / (1.0 + jnp.exp(-gate_proj)) * up_proj * own_mix
            place = pl.ds(pl.multiple_of(at * rows_out.shape[1], rows.shape[0]), rows.shape[0])
            hidden_ref[place, :] = hidden.astype(hidden_ref.dtype)

    half = count // 2
    order = [r for i in range(half) for r in ((half + i, i) if i else (half,))]
    first = [(kind, r) for r in order for kind in ((0, 2) if r < NEAR else (0,))]
    items = first + [(1, r) for r in order]
    spacing = len(items) // (line + 1)
    side_at = 2 + spacing * (line - 1) + 3

    def advance(i):
        pass_on(*items[i])
        before_last = len(items) - 1 - i
        if before_last % 2 == 0 and before_last < 8:
            if before_last == 6:
                ready()
            expert_rows(3 - before_last // 2)

    for i, item in enumerate(items):
        start_weight(*item)
        if i >= 2 and (i - 2) % spacing == 0 and (i - 2) // spacing < line - 1:
            line_step((i - 2) // spacing)
        if i == side_at:
            for index in range(line):
                side_step(index)
        if i == AHEAD:
            for copy in own_copies:
                copy.start()
        if i >= AHEAD:
            advance(i - AHEAD)
    for i in range(len(items) - AHEAD, len(items)):
        advance(i)

    own_copies[2].wait()
    for kind, r in items:
        across(kind, r, ins, outs, 0).wait_send()
        for h in range(1, groups if r >= NEAR else 1):
            onward(kind, r, h, 0).wait_send()
            if kind == 1:
                onward(kind, r, h, 0).wait_recv()
    for index in range(line):
        block = lax.rem(me, 4) + 4 * index

        @pl.when(jnp.logical_and(has_up, index <= layer))
        def _():
            row_copy(0, block, me ^ 1).wait_send()

        @pl.when(jnp.logical_and(has_down, index >= layer))
        def _():
            row_copy(1, block, me ^ 1).wait_send()

        row_copy(2, block, me ^ 1).wait_send()
        row_copy(3, block, me ^ 1).wait_send()
        row_copy(3, block ^ 2, me ^ 1).wait_send()


def move(groups, gate_train, up_train, down_train, row_block):
    count = gate_train.shape[0]
    anywhere = pl.BlockSpec(memory_space=pl.ANY)
    DMA = pltpu.SemaphoreType.DMA
    return pl.pallas_call(
        functools.partial(move_kernel, groups, count),
        out_shape=[
            jax.ShapeDtypeStruct((count * row_block.shape[0], gate_train.shape[2]), jnp.bfloat16),
            jax.ShapeDtypeStruct(down_train.shape, down_train.dtype),
        ],
        in_specs=[anywhere, anywhere, anywhere, pl.BlockSpec(memory_space=pltpu.VMEM)],
        out_specs=[pl.BlockSpec(memory_space=pltpu.VMEM), anywhere],
        scratch_shapes=[
            pltpu.VMEM(gate_train.shape, gate_train.dtype),
            pltpu.VMEM(up_train.shape, up_train.dtype),
            pltpu.VMEM((count,) + row_block.shape, row_block.dtype),
            DMA((2, count)), DMA((2, count)),
            DMA((2, count, max(1, groups - 1))), DMA((2, count, max(1, groups - 1))),
            DMA((4,)), DMA((4, count)), DMA((count,)),
        ],
        compiler_params=pltpu.CompilerParams(collective_id=0, has_side_effects=True, vmem_limit_bytes=60 * 2**20),
    )(gate_train, up_train, down_train, row_block)


def sum_kernel(
    count, part_ref, out_ref, core_in, side_in, up_in, down_in, side_out, up_out, down_out,
    core_send, core_recv, side_send, side_recv, up_send, up_recv, down_send, down_recv,
):
    me = lax.axis_index("expert")
    group = lax.axis_index("groups")
    line, layer = count // 4, me // 4
    place = lax.rem(me, 4)
    side, core = place // 2, lax.rem(place, 2)
    has_up, has_down = me + 4 < count, me >= 4
    greet([
        (None, (group, me ^ 1)), (None, (group, me ^ 2)),
        (has_up, (group, me + 4)), (has_down, (group, me - 4)),
    ])
    chunk = 16
    row_count = part_ref.shape[1]

    def remote(src, dst, send, recv, target):
        return pltpu.make_async_remote_copy(
            src_ref=src, dst_ref=dst, send_sem=send, recv_sem=recv, device_id=(group, target), device_id_type=MESH
        )

    def add(target, *sources):
        @pl.loop(0, row_count // chunk)
        def _(step):
            rows = pl.ds(pl.multiple_of(step * chunk, chunk), chunk)
            total = sources[0][rows, :].astype(jnp.float32)
            for source in sources[1:]:
                total = total + source[rows, :].astype(jnp.float32)
            target[rows, :] = total.astype(target.dtype)

    def core_copy(at, y):
        slot = at * 2 + y
        return remote(
            part_ref.at[at * 4 + y * 2 + (core ^ 1)], core_in.at[slot], core_send.at[slot], core_recv.at[slot], me ^ 1
        )

    def side_copy(at):
        return remote(side_out.at[at], side_in.at[at], side_send.at[at], side_recv.at[at], me ^ 2)

    def up_copy(at):
        return remote(up_out.at[at], up_in.at[at], up_send.at[at], up_recv.at[at], me + 4)

    def down_copy(at):
        return remote(down_out.at[at], down_in.at[at], down_send.at[at], down_recv.at[at], me - 4)

    def in_order(act):
        for d in range(line - 1, 0, -1):
            pl.when(layer + d < line)(functools.partial(act, layer + d, 1))
            pl.when(layer - d >= 0)(functools.partial(act, layer - d, -1))
        act(layer, 0)

    in_order(lambda at, way: core_copy(at, side ^ 1).start())
    in_order(lambda at, way: core_copy(at, side).start())

    def to_side(at, way):
        core_copy(at, side ^ 1).wait_recv()
        add(side_out.at[at], part_ref.at[at * 4 + (side ^ 1) * 2 + core], core_in.at[at * 2 + (side ^ 1)])
        side_copy(at).start()

    in_order(to_side)

    def along(at, way):
        core_copy(at, side).wait_recv()
        side_copy(at).wait_recv()
        mine = (part_ref.at[at * 4 + place], core_in.at[at * 2 + side], side_in.at[at])
        if way == 1:
            @pl.when(has_down)
            def _():
                up_copy(at).wait_recv()
                add(up_out.at[at], *mine, up_in.at[at])

            @pl.when(jnp.logical_not(has_down))
            def _():
                add(up_out.at[at], *mine)

            up_copy(at).start()
        elif way == -1:
            @pl.when(has_up)
            def _():
                down_copy(at).wait_recv()
                add(down_out.at[at], *mine, down_in.at[at])

            @pl.when(jnp.logical_not(has_up))
            def _():
                add(down_out.at[at], *mine)

            down_copy(at).start()
        else:
            @pl.when(has_down)
            def _():
                up_copy(at).wait_recv()

            @pl.when(has_up)
            def _():
                down_copy(at).wait_recv()

            both = jnp.logical_and(has_down, has_up)

            @pl.when(both)
            def _():
                add(out_ref, *mine, up_in.at[at], down_in.at[at])

            @pl.when(jnp.logical_and(has_down, jnp.logical_not(has_up)))
            def _():
                add(out_ref, *mine, up_in.at[at])

            @pl.when(jnp.logical_and(has_up, jnp.logical_not(has_down)))
            def _():
                add(out_ref, *mine, down_in.at[at])

            @pl.when(jnp.logical_not(jnp.logical_or(has_up, has_down)))
            def _():
                add(out_ref, *mine)

    in_order(along)

    def finish(at, way):
        core_copy(at, side ^ 1).wait_send()
        core_copy(at, side).wait_send()
        side_copy(at).wait_send()
        if way == 1:
            up_copy(at).wait_send()
        if way == -1:
            down_copy(at).wait_send()

    in_order(finish)


def summed(partial_out, count):
    rows, width = partial_out.shape[0] // count, partial_out.shape[1]
    line = count // 4
    DMA = pltpu.SemaphoreType.DMA
    block = lambda amount: pltpu.VMEM((amount, rows, width), jnp.bfloat16)
    return pl.pallas_call(
        functools.partial(sum_kernel, count),
        out_shape=jax.ShapeDtypeStruct((rows, width), jnp.bfloat16),
        in_specs=[pl.BlockSpec(memory_space=pltpu.VMEM)],
        out_specs=pl.BlockSpec(memory_space=pltpu.VMEM),
        scratch_shapes=[block(count // 2)] + [block(line)] * 6
        + [DMA((count // 2,)), DMA((count // 2,))] + [DMA((line,))] * 6,
        compiler_params=pltpu.CompilerParams(collective_id=1, has_side_effects=True, vmem_limit_bytes=60 * 2**20),
    )(partial_out.reshape(count, rows, width))


def dims_fit(groups, count, gate_train, down_train, row_count):
    rows, width = gate_train.shape[1], gate_train.shape[2]
    part = down_train.shape[1]
    return (
        groups == 2
        and count % 8 == 0
        and 2 * count <= 128
        and rows % 128 == 0
        and part % 16 == 0
        and part * count == width
        and width % 256 == 0
        and row_count % 16 == 0
        and (count * row_count) % 512 == 0
    )


def fused_kernel(
    count, first_columns, lengths_ref, queries_ref, keys_ref, values_ref, new_key_ref, new_value_ref,
    hidden_in_ref, gain_in_ref, router_in_ref, ids_in_ref, gate_ref, up_ref, down_in_ref,
    attended_ref, out_ref,
    queries, keys, cached, new_key, new_value, hid_ref, gain_ref, router_ref, ids_ref, down,
    load, stage, wt, rows, acc, units, part, core_in, side_out, side_in,
    early_up_out, early_up_in, early_down_out, early_down_in,
    late_up_out, late_up_in, late_down_out, late_down_in, last_out, last_in,
    small_sem, load_sem, send_w, recv_w, send_x, recv_x, send_rows, recv_rows,
    core_send, core_recv, line_send, line_recv, last_send, last_recv,
):
    me = lax.axis_index("expert")
    group = lax.axis_index("groups")
    other_group = 1 - group
    line = count // 4
    layer = me // 4
    row_count, width = hid_ref.shape
    depth = gate_ref.shape[1]
    share = stage.shape[2] // count
    total_f = stage.shape[2]
    tokens = count * row_count

    def loading(m, e):
        return pltpu.make_async_copy((gate_ref, up_ref)[m].at[e], load.at[m, e], load_sem.at[m, e])

    small = [
        pltpu.make_async_copy(src, dst, small_sem.at[i])
        for i, (src, dst) in enumerate((
            (hidden_in_ref, hid_ref), (gain_in_ref, gain_ref), (router_in_ref, router_ref), (ids_in_ref, ids_ref),
            (queries_ref, queries), (keys_ref, keys), (values_ref, cached), (new_key_ref, new_key),
            (new_value_ref, new_value), (down_in_ref, down),
        ))
    ]
    for copy in small[:4]:
        copy.start()
    for e in range(count):
        for m in range(2):
            loading(m, e).start()
    for copy in small[4:]:
        copy.start()

    barrier = pltpu.get_barrier_semaphore()
    peers = [(group, me ^ r) for r in range(1, count)] + [(other_group, me)]
    for peer in peers:
        pl.semaphore_signal(barrier, inc=1, device_id=peer, device_id_type=MESH)

    for copy in small[:4]:
        copy.wait()
    values = hid_ref[...].astype(jnp.float32)
    mean_square = jnp.mean(values * values, axis=-1, keepdims=True)
    gain = gain_ref[...].astype(jnp.float32).reshape(1, width)
    normed = (values * lax.rsqrt(mean_square + EPSILON) * gain).astype(jnp.bfloat16)
    rows[me, :, :width] = normed
    by_last = (((1,), (1,)), ((), ()))
    logits = lax.dot_general(normed, router_ref[...], by_last, preferred_element_type=jnp.float32)
    ids = ids_ref[...]
    lane = lax.broadcasted_iota(jnp.int32, (count, row_count), 0)
    named = ids[0:1, :] == lane
    for k in range(1, ids.shape[0]):
        named = jnp.logical_or(named, ids[k : k + 1, :] == lane)
    named = jnp.where(named, 1.0, 0.0).astype(jnp.bfloat16)
    diagonal = lax.broadcasted_iota(jnp.int32, (row_count, row_count), 0) == lax.broadcasted_iota(
        jnp.int32, (row_count, row_count), 1
    )
    diagonal = jnp.where(diagonal, 1.0, 0.0).astype(jnp.bfloat16)
    picked = lax.dot_general(diagonal, named, by_last, preferred_element_type=jnp.float32) > 0.5
    masked = jnp.where(picked, logits, -jnp.inf)
    raised = jnp.exp(masked - jnp.max(masked, axis=-1, keepdims=True))
    mixing = raised / jnp.sum(raised, axis=-1, keepdims=True)
    high = mixing.astype(jnp.bfloat16)
    low = (mixing - high.astype(jnp.float32)).astype(jnp.bfloat16)
    source = lax.broadcasted_iota(jnp.int32, (count, 128), 0)
    place = lax.broadcasted_iota(jnp.int32, (count, 128), 1)
    at_high = jnp.where(place == source, 1.0, 0.0).astype(jnp.bfloat16)
    at_low = jnp.where(place == source + count, 1.0, 0.0).astype(jnp.bfloat16)
    shares = jnp.dot(high, at_high, preferred_element_type=jnp.float32) + jnp.dot(
        low, at_low, preferred_element_type=jnp.float32
    )
    rows[me, :, width:] = shares.astype(jnp.bfloat16)

    pl.semaphore_wait(barrier, len(peers))

    def remote(src, dst, send, recv, target):
        return pltpu.make_async_remote_copy(
            src_ref=src, dst_ref=dst, send_sem=send, recv_sem=recv, device_id=target, device_id_type=MESH
        )

    def row_copy(kind, block, target):
        return remote(
            rows.at[block], rows.at[block], send_rows.at[kind, block], recv_rows.at[block], (group, target)
        )

    def row_wait(block):
        row_copy(0, block, me ^ 1).wait_recv()

    has_up, has_down = me + 4 < count, me >= 4

    @pl.when(has_up)
    def _():
        row_copy(0, me, me + 4).start()

    @pl.when(has_down)
    def _():
        row_copy(1, me, me - 4).start()

    row_copy(2, me, me ^ 2).start()
    row_copy(3, me, me ^ 1).start()

    def line_step(step):
        below, above = me - 4 * (step + 1), me + 4 * (step + 1)

        @pl.when(below >= 0)
        def _():
            row_wait(below)

            @pl.when(has_up)
            def _():
                row_copy(0, below, me + 4).start()

            row_copy(2, below, me ^ 2).start()
            row_copy(3, below, me ^ 1).start()

        @pl.when(above < count)
        def _():
            row_wait(above)

            @pl.when(has_down)
            def _():
                row_copy(1, above, me - 4).start()

            row_copy(2, above, me ^ 2).start()
            row_copy(3, above, me ^ 1).start()

    def side_step():
        for index in range(line):
            block = (lax.rem(me, 4) ^ 2) + 4 * index
            row_wait(block)
            row_copy(3, block, me ^ 1).start()

    def rows_ready():
        for index in range(line):
            for y in range(2):
                row_wait(4 * index + 2 * y + (lax.rem(me, 2) ^ 1))

    def lanes_of(owner):
        return pl.ds(pl.multiple_of(owner * depth, depth), depth)

    def across(m, r):
        target = me ^ r
        index = m if r < NEAR else group
        slot = m if r < NEAR else 0
        return remote(
            stage.at[index, target], wt.at[index, :, lanes_of(me)],
            send_w.at[slot, r], recv_w.at[slot, r], (group, target),
        )

    def onward(r):
        held = me ^ r
        ref = wt.at[group, :, lanes_of(held)]
        return remote(ref, ref, send_x.at[r], recv_x.at[r], (other_group, me))

    def start_weight(r):
        for m in range(2 if r < NEAR else 1):
            across(m, r).start()

    def pass_on(r):
        for m in range(2 if r < NEAR else 1):
            across(m, r).wait_recv()
        if r >= NEAR:
            onward(r).start()

    @pl.loop(0, count)
    def _(e):
        for m in range(2):
            loading(m, e).wait()
            turned = load[m, e].T.reshape(count, share, depth)
            stage[m, :, pl.ds(pl.multiple_of(e * share, share), share), :] = turned

    for m in range(2):
        wt[m, :, lanes_of(me)] = stage[m, me]

    tile = 256
    tiles = total_f // tile
    chunk = 512
    chunks = tokens // chunk
    blocks = chunk // row_count

    def accumulate(r, first):
        for q in (r, r ^ 1):
            if q >= NEAR:
                onward(q).wait_recv()
        base = pl.multiple_of(((me ^ r) // 2) * (2 * depth), 2 * depth)

        @pl.loop(0, 2 * tiles)
        def _(step):
            m, n = step // tiles, step % tiles
            weight = wt[m, pl.ds(pl.multiple_of(n * tile, tile), tile), pl.ds(base, 2 * depth)]

            @pl.loop(0, chunks)
            def _(c):
                x = rows[pl.ds(c * blocks, blocks), :, pl.ds(base, 2 * depth)].reshape(chunk, 2 * depth)
                product = lax.dot_general(
                    x, weight, by_last, preferred_element_type=jnp.float32
                )
                at = pl.ds(pl.multiple_of(c * chunk, chunk), chunk)
                if first:
                    acc[step, at, :] = product
                else:
                    acc[step, at, :] = acc[step, at, :] + product

    def attend_here():
        for copy in small[4:9]:
            copy.wait()
        seq_count = queries.shape[0]
        group_size = HEADS // KV_HEADS
        shape = (group_size * seq_count, 1)
        seq = jnp.bitwise_and(lax.broadcasted_iota(jnp.int32, shape, 0), seq_count - 1)
        lengths = jnp.zeros(shape, jnp.int32)
        for s in range(seq_count):
            lengths = jnp.where(seq == s, lengths_ref[s], lengths)
        span = seq_count * CTX
        position = lax.broadcasted_iota(jnp.int32, (shape[0], span), 1) - seq * CTX
        visible = jnp.logical_and(position >= 0, position < lengths)
        score_scale = 1.0 / math.sqrt(HEAD_DIM)

        def columns_of(index):
            return slice(index * HEAD_DIM, (index + 1) * HEAD_DIM)

        for g in range(KV_HEADS):
            mine = [queries[:, columns_of(g * group_size + h)].astype(jnp.float32) for h in range(group_size)]
            asked = jnp.concatenate(mine, axis=0)
            key = keys[:, :, columns_of(g)].reshape(span, HEAD_DIM)
            value = cached[:, :, columns_of(g)].reshape(span, HEAD_DIM)
            fresh_key = jnp.concatenate([new_key[:, columns_of(g)].astype(jnp.float32)] * group_size, axis=0)
            fresh_value = jnp.concatenate([new_value[:, columns_of(g)].astype(jnp.float32)] * group_size, axis=0)
            scores = score_scale * lax.dot_general(
                asked.astype(jnp.bfloat16), key, by_last, preferred_element_type=jnp.float32
            )
            scores = jnp.where(visible, scores, -1e30)
            own_score = jnp.sum(asked * fresh_key, axis=-1, keepdims=True) * score_scale
            largest = jnp.maximum(jnp.max(scores, axis=-1, keepdims=True), own_score)
            cached_exp = jnp.exp(scores - largest)
            own_exp = jnp.exp(own_score - largest)
            prob_total = jnp.sum(cached_exp, axis=-1, keepdims=True) + own_exp
            cached_prob = (cached_exp / prob_total).astype(jnp.bfloat16)
            own_prob = (own_exp / prob_total).astype(jnp.bfloat16).astype(jnp.float32)
            context = jnp.dot(cached_prob, value, preferred_element_type=jnp.float32) + own_prob * fresh_value
            for h in range(group_size):
                attended_ref[:, columns_of(g * group_size + h)] = context[
                    h * seq_count : (h + 1) * seq_count, :
                ].astype(attended_ref.dtype)

    half = count // 2
    order = [r for i in range(half) for r in ((half + i, i) if i else (half,))]
    passed, pending, done = {0}, [], 0
    side_at = 2 * line

    def after(i):
        nonlocal done
        r = order[i]
        pass_on(r)
        passed.add(r)
        if r ^ 1 in passed:
            pending.append((i, r))

    started_rows = False

    def compute(i):
        nonlocal done, started_rows
        while pending and (pending[0][0] + LAG <= i):
            _, r = pending.pop(0)
            if not started_rows:
                rows_ready()
                started_rows = True
            accumulate(r, done == 0)
            done += 1

    for i, r in enumerate(order):
        start_weight(r)
        if i % 2 == 1 and i // 2 < line - 1:
            line_step(i // 2)
        if i == side_at:
            side_step()
        if i == AHEAD - 1:
            attend_here()
        if i >= AHEAD:
            after(i - AHEAD)
            if i > side_at:
                compute(i - AHEAD)
    for i in range(len(order) - AHEAD, len(order)):
        after(i)
        compute(i)
    compute(len(order) + LAG)

    spread_at = lax.broadcasted_iota(jnp.int32, (128, total_f), 0)
    column = lax.broadcasted_iota(jnp.int32, (128, total_f), 1)
    expert = jnp.where(spread_at < count, spread_at, spread_at - count)
    inside = jnp.logical_and(column >= expert * share, column < expert * share + share)
    spread = jnp.where(jnp.logical_and(inside, spread_at < 2 * count), 1.0, 0.0).astype(jnp.bfloat16)

    place_in_layer = lax.rem(me, 4)
    side, core = place_in_layer // 2, lax.rem(place_in_layer, 2)
    first, second = pl.ds(0, first_columns), pl.ds(first_columns, width - first_columns)
    small[9].wait()
    table = []
    for own in range(line):
        seen = []
        for d in range(line - 1, 0, -1):
            seen += [own + d] * (own + d < line) + [own - d] * (own - d >= 0)
        table.append(seen + [own])

    def turn(j):
        at = jnp.int32(0)
        for own in range(line):
            at = at + (layer == own).astype(jnp.int32) * table[own][j]
        return at

    def make_part(at):
        @pl.loop(0, 4)
        def _(b):
            block = at * 4 + b
            mix = jnp.dot(rows[block, :, width:], spread, preferred_element_type=jnp.float32)
            here = pl.ds(pl.multiple_of(block * row_count, row_count), row_count)
            there = pl.ds(pl.multiple_of(b * row_count, row_count), row_count)
            for n in range(tiles):
                gate_proj = acc[n, here, :]
                up_proj = acc[tiles + n, here, :]
                columns = slice(n * tile, (n + 1) * tile)
                hidden = gate_proj / (1.0 + jnp.exp(-gate_proj)) * up_proj * mix[:, columns]
                units[there, columns] = hidden.astype(units.dtype)

        @pl.loop(0, width // tile)
        def _(n):
            columns = pl.ds(pl.multiple_of(n * tile, tile), tile)
            product = jnp.dot(units[...], down[:, columns], preferred_element_type=jnp.float32)
            part[pl.ds(at * 4, 4), :, columns] = product.astype(part.dtype).reshape(4, row_count, tile)

    def add(target, *sources):
        @pl.loop(0, row_count // 16)
        def _(step):
            here = pl.ds(pl.multiple_of(step * 16, 16), 16)
            total = sources[0][here, :].astype(jnp.float32)
            for source in sources[1:]:
                total = total + source[here, :].astype(jnp.float32)
            target[here, :] = total.astype(target.dtype)

    def core_copy(at, y):
        slot = at * 2 + y
        return remote(
            part.at[at * 4 + y * 2 + (core ^ 1)], core_in.at[slot], core_send.at[slot], core_recv.at[slot], (group, me ^ 1)
        )

    def line_copy(kind, at):
        src, dst, target = (
            (side_out, side_in, me ^ 2),
            (early_up_out, early_up_in, me + 4),
            (early_down_out, early_down_in, me - 4),
            (late_up_out, late_up_in, me + 4),
            (late_down_out, late_down_in, me - 4),
        )[kind]
        return remote(src.at[at], dst.at[at], line_send.at[kind, at], line_recv.at[kind, at], (group, target))

    def last_copy():
        return remote(last_out, last_in, last_send.at[0], last_recv.at[0], (group, me ^ 2))

    def held(at, y, columns):
        return part.at[at * 4 + y * 2 + core, :, columns], core_in.at[at * 2 + y, :, columns]

    def to_side(at):
        for y in range(2):
            core_copy(at, y).wait_recv()
        add(side_out.at[at], *held(at, side ^ 1, first))
        line_copy(0, at).start()

    def step_along(at, kinds, sources):
        for kind, has_source, moving in ((kinds[0], has_down, at > layer), (kinds[1], has_up, at < layer)):
            @pl.when(jnp.logical_and(moving, has_source))
            def _():
                line_copy(kind, at).wait_recv()
                sources(kind, True)
                line_copy(kind, at).start()

            @pl.when(jnp.logical_and(moving, jnp.logical_not(has_source)))
            def _():
                sources(kind, False)
                line_copy(kind, at).start()

    def early(at):
        def sources(kind, arriving):
            out, arrived = ((early_up_out, early_up_in), (early_down_out, early_down_in))[kind - 1]
            for y in range(2):
                more = (arrived.at[at, y],) if arriving else ()
                add(out.at[at, y], *held(at, y, second), *more)

        step_along(at, (1, 2), sources)

    def late(at):
        line_copy(0, at).wait_recv()

        def sources(kind, arriving):
            out, arrived = ((late_up_out, late_up_in), (late_down_out, late_down_in))[kind - 3]
            more = (arrived.at[at],) if arriving else ()
            add(out.at[at], *held(at, side, first), side_in.at[at], *more)

        step_along(at, (3, 4), sources)

    def arrived_from(kinds, act):
        @pl.when(has_down)
        def _():
            line_copy(kinds[0], layer).wait_recv()

        @pl.when(has_up)
        def _():
            line_copy(kinds[1], layer).wait_recv()

        for down_too, up_too in ((True, True), (True, False), (False, True)):
            matches = jnp.logical_and(has_down == down_too, has_up == up_too)
            pl.when(matches)(functools.partial(act, down_too, up_too))

    for j in range(line):
        at = turn(j)
        make_part(at)
        core_copy(at, side ^ 1).start()
        core_copy(at, side).start()
        if j:
            to_side(turn(j - 1))
    to_side(turn(line - 1))
    for j in range(line - 1):
        early(turn(j))
    for j in range(line - 1):
        late(turn(j))
    line_copy(0, layer).wait_recv()

    def sum_early(down_too, up_too):
        for y, target in ((side ^ 1, last_out), (side, out_ref.at[:, second])):
            more = [ref.at[layer, y] for ref, on in ((early_up_in, down_too), (early_down_in, up_too)) if on]
            add(target, *held(layer, y, second), *more)

    def sum_late(down_too, up_too):
        more = [ref.at[layer] for ref, on in ((late_up_in, down_too), (late_down_in, up_too)) if on]
        add(out_ref.at[:, first], *held(layer, side, first), side_in.at[layer], *more)

    arrived_from((1, 2), sum_early)
    last_copy().start()
    arrived_from((3, 4), sum_late)
    last_copy().wait_recv()
    add(out_ref.at[:, second], out_ref.at[:, second], last_in)

    last_copy().wait_send()
    for at in range(line):
        for y in range(2):
            core_copy(at, y).wait_send()
        line_copy(0, at).wait_send()
        for up_kind in (1, 3):
            pl.when(at > layer)(line_copy(up_kind, at).wait_send)
            pl.when(at < layer)(line_copy(up_kind + 1, at).wait_send)
    for r in order:
        for m in range(2 if r < NEAR else 1):
            across(m, r).wait_send()
        if r >= NEAR:
            onward(r).wait_send()
    for index in range(line):
        block = lax.rem(me, 4) + 4 * index

        @pl.when(jnp.logical_and(has_up, index <= layer))
        def _():
            row_copy(0, block, me ^ 1).wait_send()

        @pl.when(jnp.logical_and(has_down, index >= layer))
        def _():
            row_copy(1, block, me ^ 1).wait_send()

        row_copy(2, block, me ^ 1).wait_send()
        row_copy(3, block, me ^ 1).wait_send()
        row_copy(3, block ^ 2, me ^ 1).wait_send()


def fused(
    queries, key_cache, value_cache, new_key, new_value, cache_lengths,
    hidden_in, norm_gain, router_weight, expert_ids, gate_train, up_train, down_train,
):
    count, depth, total_f = gate_train.shape
    row_count, width = hidden_in.shape
    line = count // 4
    first_columns = pl.cdiv(width * 6, 10 * 128) * 128
    second_columns = width - first_columns
    anywhere = pl.BlockSpec(memory_space=pl.ANY)
    near = pl.BlockSpec(memory_space=pltpu.VMEM)
    DMA = pltpu.SemaphoreType.DMA
    like = lambda x: pltpu.VMEM(x.shape, x.dtype)
    held = lambda *shape: pltpu.VMEM(shape, jnp.bfloat16)
    router_turned, ids_turned = router_weight.T, expert_ids.T
    down_rows = down_train.reshape(-1, width)
    return pl.pallas_call(
        functools.partial(fused_kernel, count, first_columns),
        out_shape=[
            jax.ShapeDtypeStruct(queries.shape, jnp.bfloat16),
            jax.ShapeDtypeStruct((row_count, width), jnp.bfloat16),
        ],
        in_specs=[pl.BlockSpec(memory_space=pltpu.SMEM)] + [anywhere] * 12,
        out_specs=[near, near],
        scratch_shapes=[
            like(queries), like(key_cache), like(value_cache), like(new_key), like(new_value),
            like(hidden_in), like(norm_gain), like(router_turned), like(ids_turned), like(down_rows),
            held(2, count, depth, total_f),
            held(2, count, total_f, depth),
            held(2, total_f, count * depth),
            held(count, row_count, width + 128),
            pltpu.VMEM((2 * total_f // 256, count * row_count, 256), jnp.float32),
            held(4 * row_count, total_f),
            held(count, row_count, width),
            held(2 * line, row_count, width),
            held(line, row_count, first_columns), held(line, row_count, first_columns),
            *[held(line, 2, row_count, second_columns)] * 4,
            *[held(line, row_count, first_columns)] * 4,
            held(row_count, second_columns), held(row_count, second_columns),
            DMA((10,)), DMA((2, count)), DMA((2, count)), DMA((2, count)), DMA((count,)), DMA((count,)),
            DMA((4, count)), DMA((count,)),
            DMA((2 * line,)), DMA((2 * line,)), DMA((5, line)), DMA((5, line)), DMA((1,)), DMA((1,)),
        ],
        compiler_params=pltpu.CompilerParams(collective_id=2, has_side_effects=True, vmem_limit_bytes=63 * 2**20),
    )(
        cache_lengths, queries, key_cache, value_cache, new_key, new_value,
        hidden_in, norm_gain, router_turned, ids_turned, gate_train, up_train, down_rows,
    )


def local(
    queries,
    key_cache,
    value_cache,
    new_key,
    new_value,
    cache_lengths,
    hidden_in,
    norm_gain,
    router_weight,
    expert_ids,
    gate_train,
    up_train,
    down_train,
):
    width = hidden_in.shape[1]
    expert_count = router_weight.shape[1]
    groups = lax.axis_size("groups")
    if dims_fit(groups, expert_count, gate_train, down_train, hidden_in.shape[0]) and queries.shape[0] == 8:
        return tuple(fused(
            queries, key_cache, value_cache, new_key, new_value, cache_lengths,
            hidden_in, norm_gain, router_weight, expert_ids, gate_train, up_train, down_train,
        ))
    normed = rms_normed(hidden_in, norm_gain)
    mixing = dense_mixing(normed, router_weight, expert_ids)
    mixing_high = mixing.astype(jnp.bfloat16)
    mixing_low = (mixing - mixing_high.astype(jnp.float32)).astype(jnp.bfloat16)
    spare = -2 * expert_count % 128
    row_block = jnp.concatenate(
        [normed, mixing_high, mixing_low, jnp.zeros((normed.shape[0], spare), jnp.bfloat16)], axis=1
    )
    hidden_units, down_moved = move(groups, gate_train, up_train, down_train, row_block)
    down_moved = down_moved.reshape(-1, width)
    attended = attend(queries, key_cache, value_cache, new_key, new_value, cache_lengths)
    partial_out = jnp.dot(hidden_units, down_moved, preferred_element_type=jnp.float32).astype(jnp.bfloat16)
    mixed_out = summed(partial_out, expert_count)
    return (attended, mixed_out)


def solution(mesh):
    placed = (
        P(("groups", "expert"), None),
        P(("groups", "expert"), None, None),
        P(("groups", "expert"), None, None),
        P(("groups", "expert"), None),
        P(("groups", "expert"), None),
        P(("groups", "expert")),
        P(("groups", "expert"), None),
        P(),
        P(),
        P(("groups", "expert"), None),
        P(None, "expert", None),
        P(None, "expert", None),
        P(None, "expert", None),
    )
    return jax.shard_map(
        local,
        mesh=mesh,
        in_specs=placed,
        out_specs=(P(("groups", "expert"), None), P(("groups", "expert"), None)),
        check_vma=False,
    )
```

```python
import functools
import math

import jax
import jax.numpy as jnp
from jax import lax
from jax.experimental import pallas as pl
from jax.experimental.pallas import tpu as pltpu
from jax.sharding import PartitionSpec as P

HEADS = 32
KV_HEADS = 4
HEAD_DIM = 128
CTX = 64


EPSILON = 1e-06


def rms_normed(hidden_in, norm_gain):
    values = hidden_in.astype(jnp.float32)
    mean_square = jnp.mean(values * values, axis=-1, keepdims=True)
    return (values * lax.rsqrt(mean_square + EPSILON) * norm_gain.astype(jnp.float32)).astype(
        jnp.bfloat16
    )


def attend(queries, key_cache, value_cache, new_key, new_value, cache_lengths):
    seq_count = queries.shape[0]
    group_size = HEADS // KV_HEADS
    query_blocks = queries.reshape(seq_count, KV_HEADS, group_size, HEAD_DIM)
    cached_keys = key_cache.reshape(seq_count, CTX, KV_HEADS, HEAD_DIM)
    cached_values = value_cache.reshape(seq_count, CTX, KV_HEADS, HEAD_DIM)
    fresh_keys = new_key.reshape(seq_count, KV_HEADS, HEAD_DIM)
    fresh_values = new_value.astype(jnp.float32).reshape(seq_count, KV_HEADS, HEAD_DIM)
    score_scale = 1.0 / math.sqrt(HEAD_DIM)
    scores = (
        jnp.einsum("sgrd,scgd->sgrc", query_blocks, cached_keys, preferred_element_type=jnp.float32)
        * score_scale
    )
    own_score = (
        jnp.einsum("sgrd,sgd->sgr", query_blocks, fresh_keys, preferred_element_type=jnp.float32)
        * score_scale
    )
    positions = jnp.arange(CTX, dtype=jnp.int32)
    visible = positions[None, :] < cache_lengths[:, None]
    scores = jnp.where(visible[:, None, None, :], scores, -1e30)
    largest = jnp.maximum(jnp.max(scores, axis=-1), own_score)
    cached_exp = jnp.exp(scores - largest[..., None])
    own_exp = jnp.exp(own_score - largest)
    prob_total = jnp.sum(cached_exp, axis=-1) + own_exp
    cached_prob = (cached_exp / prob_total[..., None]).astype(jnp.bfloat16)
    own_prob = (own_exp / prob_total).astype(jnp.bfloat16).astype(jnp.float32)
    context = jnp.einsum(
        "sgrc,scgd->sgrd", cached_prob, cached_values, preferred_element_type=jnp.float32
    )
    context = context + own_prob[..., None] * fresh_values[:, :, None, :]
    return context.reshape(seq_count, HEADS * HEAD_DIM).astype(jnp.bfloat16)


def dense_mixing(normed, router_weight, expert_ids):
    logits = jnp.dot(normed, router_weight, preferred_element_type=jnp.float32)
    expert_range = jnp.arange(router_weight.shape[1], dtype=jnp.int32)
    picked = jnp.any(expert_ids[:, :, None] == expert_range[None, None, :], axis=1)
    masked = jnp.where(picked, logits, -jnp.inf)
    raised = jnp.exp(masked - jnp.max(masked, axis=-1, keepdims=True))
    return raised / jnp.sum(raised, axis=-1, keepdims=True)


MESH = pl.DeviceIdType.MESH
AHEAD = 4
NEAR = 4
LAG = 2
FUSED_AHEAD = 2
ROW_SPACING = 2


def greet(targets):
    barrier = pltpu.get_barrier_semaphore()

    expected = 0
    for condition, target in targets:
        signal = functools.partial(
            pl.semaphore_signal, barrier, inc=1, device_id=target, device_id_type=MESH
        )
        if condition is None:
            signal()
            expected = expected + 1
        else:
            pl.when(condition)(signal)
            expected = expected + condition.astype(jnp.int32)
    pl.semaphore_wait(barrier, expected)


def move_kernel(
    groups, count,
    gate_ref, up_ref, down_ref, rows_ref,
    hidden_ref, down_out, gate_out, up_out, rows_out,
    send_w, recv_w, send_x, recv_x, local_sem, send_rows, recv_rows,
):
    me = lax.axis_index("expert")
    group = lax.axis_index("groups")
    parts = max(1, groups // 2)
    part_rows = gate_ref.shape[1] // parts
    part_columns = down_ref.shape[2] // groups
    line = count // 4
    layer = me // 4

    others = [(None, (group, me ^ r)) for r in range(1, count)]
    others += [(None, (lax.rem(group + h, groups), me)) for h in range(1, groups)]
    greet(others)

    def remote(src, dst, send, recv, target):
        return pltpu.make_async_remote_copy(
            src_ref=src, dst_ref=dst, send_sem=send, recv_sem=recv, device_id=target, device_id_type=MESH
        )

    def rows_of(owner):
        return pl.ds(pl.multiple_of((owner // 2) * part_rows, part_rows), part_rows)

    def columns_of(owner):
        return pl.ds(pl.multiple_of(owner * part_columns, part_columns), part_columns)

    def row_copy(kind, block, target, own=False):
        source = rows_ref if own else rows_out.at[block]
        return remote(
            source, rows_out.at[block], send_rows.at[kind, block], recv_rows.at[block], (group, target)
        )

    def row_wait(block):
        row_copy(0, block, me ^ 1).wait_recv()

    own_rows = pltpu.make_async_copy(rows_ref, rows_out.at[me], local_sem.at[3])
    own_rows.start()
    has_up, has_down = me + 4 < count, me >= 4

    @pl.when(has_up)
    def _():
        row_copy(0, me, me + 4, True).start()

    @pl.when(has_down)
    def _():
        row_copy(1, me, me - 4, True).start()

    row_copy(2, me, me ^ 2, True).start()
    row_copy(3, me, me ^ 1, True).start()

    def line_step(step):
        below, above = me - 4 * (step + 1), me + 4 * (step + 1)

        @pl.when(below >= 0)
        def _():
            row_wait(below)

            @pl.when(has_up)
            def _():
                row_copy(0, below, me + 4).start()

            row_copy(2, below, me ^ 2).start()
            row_copy(3, below, me ^ 1).start()

        @pl.when(above < count)
        def _():
            row_wait(above)

            @pl.when(has_down)
            def _():
                row_copy(1, above, me - 4).start()

            row_copy(2, above, me ^ 2).start()
            row_copy(3, above, me ^ 1).start()

    def side_step(index):
        block = lax.rem(me, 4) ^ 2
        block = block + 4 * index
        row_wait(block)
        row_copy(3, block, me ^ 1).start()

    def across(kind, r, refs_in, refs_out, which):
        target = me ^ r
        if r < NEAR:
            a, b = ((gate_ref, gate_out), (down_ref, down_out), (up_ref, up_out))[kind]
            send = send_x.at[0, r, 0] if kind == 2 else send_w.at[kind, r]
            recv = recv_x.at[0, r, 0] if kind == 2 else recv_w.at[kind, r]
            return remote(a.at[target], b.at[me], send, recv, (group, target))
        if kind == 0:
            return remote(
                refs_in[which].at[target, rows_of(group)], refs_out[which].at[me, rows_of(group)],
                send_w.at[0, r], recv_w.at[0, r], (group, target),
            )
        return remote(
            down_ref.at[target, :, columns_of(group)], down_out.at[me, :, columns_of(group)],
            send_w.at[1, r], recv_w.at[1, r], (group, target),
        )

    ins, outs = (gate_ref, up_ref), (gate_out, up_out)

    def by_matrix(act):
        pl.when(lax.rem(group, 2) == 0)(functools.partial(act, 0))
        pl.when(lax.rem(group, 2) == 1)(functools.partial(act, 1))

    def start_weight(kind, r):
        if kind == 0 and r >= NEAR:
            by_matrix(lambda which: across(0, r, ins, outs, which).start())
        else:
            across(kind, r, ins, outs, 0).start()

    def onward(kind, r, h, which):
        held = me ^ r
        place = outs[which].at[held, rows_of(group)] if kind == 0 else down_out.at[held, :, columns_of(group)]
        return remote(
            place, place, send_x.at[kind, r, h - 1], recv_x.at[kind, r, h - 1],
            (lax.rem(group + h, groups), me),
        )

    def pass_on(kind, r):
        across(kind, r, ins, outs, 0).wait_recv()
        for h in range(1, groups if r >= NEAR else 1):
            if kind == 0:
                by_matrix(lambda which: onward(0, r, h, which).start())
            else:
                onward(1, r, h, 0).start()

    own_copies = [
        pltpu.make_async_copy(a.at[me], b.at[me], local_sem.at[i])
        for i, (a, b) in enumerate(((gate_ref, gate_out), (up_ref, up_out), (down_ref, down_out)))
    ]
    width = gate_ref.shape[1] * count

    def ready():
        for index in range(line):
            for y in range(2):
                row_wait(4 * index + 2 * y + (lax.rem(me, 2) ^ 1))
        own_rows.wait()
        for copy in own_copies[:2]:
            copy.wait()
        for r in order:
            for h in range(1, groups if r >= NEAR else 1):
                onward(0, r, h, 0).wait_recv()

    def expert_rows(quarter):
        @pl.loop(0, count // 16)
        def _(step):
            at = quarter * (count // 4) + step * 4
            rows = rows_out[pl.ds(at, 4)].reshape(-1, rows_out.shape[2])
            tokens = rows[:, :width]
            shares = rows[:, width:].astype(jnp.float32)
            lane = lax.broadcasted_iota(jnp.int32, shares.shape, 1)
            own = jnp.logical_or(lane == me, lane == me + count)
            own_mix = jnp.sum(jnp.where(own, shares, 0.0), axis=1, keepdims=True)
            gate = gate_out[...].reshape(width, -1)
            gate_proj = jnp.dot(tokens, gate, preferred_element_type=jnp.float32)
            up = up_out[...].reshape(width, -1)
            up_proj = jnp.dot(tokens, up, preferred_element_type=jnp.float32)
            hidden = gate_proj / (1.0 + jnp.exp(-gate_proj)) * up_proj * own_mix
            place = pl.ds(pl.multiple_of(at * rows_out.shape[1], rows.shape[0]), rows.shape[0])
            hidden_ref[place, :] = hidden.astype(hidden_ref.dtype)

    half = count // 2
    order = [r for i in range(half) for r in ((half + i, i) if i else (half,))]
    first = [(kind, r) for r in order for kind in ((0, 2) if r < NEAR else (0,))]
    items = first + [(1, r) for r in order]
    spacing = len(items) // (line + 1)
    side_at = 2 + spacing * (line - 1) + 3

    def advance(i):
        pass_on(*items[i])
        before_last = len(items) - 1 - i
        if before_last % 2 == 0 and before_last < 8:
            if before_last == 6:
                ready()
            expert_rows(3 - before_last // 2)

    for i, item in enumerate(items):
        start_weight(*item)
        if i >= 2 and (i - 2) % spacing == 0 and (i - 2) // spacing < line - 1:
            line_step((i - 2) // spacing)
        if i == side_at:
            for index in range(line):
                side_step(index)
        if i == AHEAD:
            for copy in own_copies:
                copy.start()
        if i >= AHEAD:
            advance(i - AHEAD)
    for i in range(len(items) - AHEAD, len(items)):
        advance(i)

    own_copies[2].wait()
    for kind, r in items:
        across(kind, r, ins, outs, 0).wait_send()
        for h in range(1, groups if r >= NEAR else 1):
            onward(kind, r, h, 0).wait_send()
            if kind == 1:
                onward(kind, r, h, 0).wait_recv()
    for index in range(line):
        block = lax.rem(me, 4) + 4 * index

        @pl.when(jnp.logical_and(has_up, index <= layer))
        def _():
            row_copy(0, block, me ^ 1).wait_send()

        @pl.when(jnp.logical_and(has_down, index >= layer))
        def _():
            row_copy(1, block, me ^ 1).wait_send()

        row_copy(2, block, me ^ 1).wait_send()
        row_copy(3, block, me ^ 1).wait_send()
        row_copy(3, block ^ 2, me ^ 1).wait_send()


def move(groups, gate_train, up_train, down_train, row_block):
    count = gate_train.shape[0]
    anywhere = pl.BlockSpec(memory_space=pl.ANY)
    DMA = pltpu.SemaphoreType.DMA
    return pl.pallas_call(
        functools.partial(move_kernel, groups, count),
        out_shape=[
            jax.ShapeDtypeStruct((count * row_block.shape[0], gate_train.shape[2]), jnp.bfloat16),
            jax.ShapeDtypeStruct(down_train.shape, down_train.dtype),
        ],
        in_specs=[anywhere, anywhere, anywhere, pl.BlockSpec(memory_space=pltpu.VMEM)],
        out_specs=[pl.BlockSpec(memory_space=pltpu.VMEM), anywhere],
        scratch_shapes=[
            pltpu.VMEM(gate_train.shape, gate_train.dtype),
            pltpu.VMEM(up_train.shape, up_train.dtype),
            pltpu.VMEM((count,) + row_block.shape, row_block.dtype),
            DMA((2, count)), DMA((2, count)),
            DMA((2, count, max(1, groups - 1))), DMA((2, count, max(1, groups - 1))),
            DMA((4,)), DMA((4, count)), DMA((count,)),
        ],
        compiler_params=pltpu.CompilerParams(collective_id=0, has_side_effects=True, vmem_limit_bytes=60 * 2**20),
    )(gate_train, up_train, down_train, row_block)


def sum_kernel(
    count, part_ref, out_ref, core_in, side_in, up_in, down_in, side_out, up_out, down_out,
    core_send, core_recv, side_send, side_recv, up_send, up_recv, down_send, down_recv,
):
    me = lax.axis_index("expert")
    group = lax.axis_index("groups")
    line, layer = count // 4, me // 4
    place = lax.rem(me, 4)
    side, core = place // 2, lax.rem(place, 2)
    has_up, has_down = me + 4 < count, me >= 4
    greet([
        (None, (group, me ^ 1)), (None, (group, me ^ 2)),
        (has_up, (group, me + 4)), (has_down, (group, me - 4)),
    ])
    chunk = 16
    row_count = part_ref.shape[1]

    def remote(src, dst, send, recv, target):
        return pltpu.make_async_remote_copy(
            src_ref=src, dst_ref=dst, send_sem=send, recv_sem=recv, device_id=(group, target), device_id_type=MESH
        )

    def add(target, *sources):
        @pl.loop(0, row_count // chunk)
        def _(step):
            rows = pl.ds(pl.multiple_of(step * chunk, chunk), chunk)
            total = sources[0][rows, :].astype(jnp.float32)
            for source in sources[1:]:
                total = total + source[rows, :].astype(jnp.float32)
            target[rows, :] = total.astype(target.dtype)

    def core_copy(at, y):
        slot = at * 2 + y
        return remote(
            part_ref.at[at * 4 + y * 2 + (core ^ 1)], core_in.at[slot], core_send.at[slot], core_recv.at[slot], me ^ 1
        )

    def side_copy(at):
        return remote(side_out.at[at], side_in.at[at], side_send.at[at], side_recv.at[at], me ^ 2)

    def up_copy(at):
        return remote(up_out.at[at], up_in.at[at], up_send.at[at], up_recv.at[at], me + 4)

    def down_copy(at):
        return remote(down_out.at[at], down_in.at[at], down_send.at[at], down_recv.at[at], me - 4)

    def in_order(act):
        for d in range(line - 1, 0, -1):
            pl.when(layer + d < line)(functools.partial(act, layer + d, 1))
            pl.when(layer - d >= 0)(functools.partial(act, layer - d, -1))
        act(layer, 0)

    in_order(lambda at, way: core_copy(at, side ^ 1).start())
    in_order(lambda at, way: core_copy(at, side).start())

    def to_side(at, way):
        core_copy(at, side ^ 1).wait_recv()
        add(side_out.at[at], part_ref.at[at * 4 + (side ^ 1) * 2 + core], core_in.at[at * 2 + (side ^ 1)])
        side_copy(at).start()

    in_order(to_side)

    def along(at, way):
        core_copy(at, side).wait_recv()
        side_copy(at).wait_recv()
        mine = (part_ref.at[at * 4 + place], core_in.at[at * 2 + side], side_in.at[at])
        if way == 1:
            @pl.when(has_down)
            def _():
                up_copy(at).wait_recv()
                add(up_out.at[at], *mine, up_in.at[at])

            @pl.when(jnp.logical_not(has_down))
            def _():
                add(up_out.at[at], *mine)

            up_copy(at).start()
        elif way == -1:
            @pl.when(has_up)
            def _():
                down_copy(at).wait_recv()
                add(down_out.at[at], *mine, down_in.at[at])

            @pl.when(jnp.logical_not(has_up))
            def _():
                add(down_out.at[at], *mine)

            down_copy(at).start()
        else:
            @pl.when(has_down)
            def _():
                up_copy(at).wait_recv()

            @pl.when(has_up)
            def _():
                down_copy(at).wait_recv()

            both = jnp.logical_and(has_down, has_up)

            @pl.when(both)
            def _():
                add(out_ref, *mine, up_in.at[at], down_in.at[at])

            @pl.when(jnp.logical_and(has_down, jnp.logical_not(has_up)))
            def _():
                add(out_ref, *mine, up_in.at[at])

            @pl.when(jnp.logical_and(has_up, jnp.logical_not(has_down)))
            def _():
                add(out_ref, *mine, down_in.at[at])

            @pl.when(jnp.logical_not(jnp.logical_or(has_up, has_down)))
            def _():
                add(out_ref, *mine)

    in_order(along)

    def finish(at, way):
        core_copy(at, side ^ 1).wait_send()
        core_copy(at, side).wait_send()
        side_copy(at).wait_send()
        if way == 1:
            up_copy(at).wait_send()
        if way == -1:
            down_copy(at).wait_send()

    in_order(finish)


def summed(partial_out, count):
    rows, width = partial_out.shape[0] // count, partial_out.shape[1]
    line = count // 4
    DMA = pltpu.SemaphoreType.DMA
    block = lambda amount: pltpu.VMEM((amount, rows, width), jnp.bfloat16)
    return pl.pallas_call(
        functools.partial(sum_kernel, count),
        out_shape=jax.ShapeDtypeStruct((rows, width), jnp.bfloat16),
        in_specs=[pl.BlockSpec(memory_space=pltpu.VMEM)],
        out_specs=pl.BlockSpec(memory_space=pltpu.VMEM),
        scratch_shapes=[block(count // 2)] + [block(line)] * 6
        + [DMA((count // 2,)), DMA((count // 2,))] + [DMA((line,))] * 6,
        compiler_params=pltpu.CompilerParams(collective_id=1, has_side_effects=True, vmem_limit_bytes=60 * 2**20),
    )(partial_out.reshape(count, rows, width))


def dims_fit(groups, count, gate_train, down_train, row_count):
    rows, width = gate_train.shape[1], gate_train.shape[2]
    part = down_train.shape[1]
    return (
        groups == 2
        and count % 8 == 0
        and 2 * count <= 128
        and rows % 128 == 0
        and part % 16 == 0
        and part * count == width
        and width % 256 == 0
        and row_count % 16 == 0
        and (count * row_count) % 512 == 0
    )


def fused_kernel(
    count, first_columns, lengths_ref, queries_ref, keys_ref, values_ref, new_key_ref, new_value_ref,
    hidden_in_ref, gain_in_ref, router_in_ref, ids_in_ref, gate_ref, up_ref, down_in_ref,
    attended_ref, out_ref,
    queries, keys, cached, new_key, new_value, hid_ref, gain_ref, router_ref, ids_ref, down,
    load, stage, wt, rows, acc, units, part, core_in, side_out, side_in,
    early_up_out, early_up_in, early_down_out, early_down_in,
    late_up_out, late_up_in, late_down_out, late_down_in, last_out, last_in,
    small_sem, load_sem, send_w, recv_w, send_x, recv_x, send_rows, recv_rows,
    core_send, core_recv, line_send, line_recv, last_send, last_recv,
):
    me = lax.axis_index("expert")
    group = lax.axis_index("groups")
    other_group = 1 - group
    line = count // 4
    layer = me // 4
    row_count, width = hid_ref.shape
    depth = gate_ref.shape[1]
    share = stage.shape[2] // count
    total_f = stage.shape[2]
    tokens = count * row_count

    def loading(m, e):
        return pltpu.make_async_copy((gate_ref, up_ref)[m].at[e], load.at[m, e], load_sem.at[m, e])

    small = [
        pltpu.make_async_copy(src, dst, small_sem.at[i])
        for i, (src, dst) in enumerate((
            (hidden_in_ref, hid_ref), (gain_in_ref, gain_ref), (router_in_ref, router_ref), (ids_in_ref, ids_ref),
            (queries_ref, queries), (keys_ref, keys), (values_ref, cached), (new_key_ref, new_key),
            (new_value_ref, new_value), (down_in_ref, down),
        ))
    ]
    for copy in small[:4]:
        copy.start()
    for e in range(count):
        for m in range(2):
            loading(m, e).start()
    for copy in small[4:]:
        copy.start()

    barrier = pltpu.get_barrier_semaphore()
    peers = [(group, me ^ r) for r in range(1, count)] + [(other_group, me)]
    for peer in peers:
        pl.semaphore_signal(barrier, inc=1, device_id=peer, device_id_type=MESH)

    for copy in small[:4]:
        copy.wait()
    values = hid_ref[...].astype(jnp.float32)
    mean_square = jnp.mean(values * values, axis=-1, keepdims=True)
    gain = gain_ref[...].astype(jnp.float32).reshape(1, width)
    normed = (values * lax.rsqrt(mean_square + EPSILON) * gain).astype(jnp.bfloat16)
    rows[me, :, :width] = normed
    by_last = (((1,), (1,)), ((), ()))
    logits = lax.dot_general(normed, router_ref[...], by_last, preferred_element_type=jnp.float32)
    ids = ids_ref[...]
    lane = lax.broadcasted_iota(jnp.int32, (count, row_count), 0)
    named = ids[0:1, :] == lane
    for k in range(1, ids.shape[0]):
        named = jnp.logical_or(named, ids[k : k + 1, :] == lane)
    named = jnp.where(named, 1.0, 0.0).astype(jnp.bfloat16)
    diagonal = lax.broadcasted_iota(jnp.int32, (row_count, row_count), 0) == lax.broadcasted_iota(
        jnp.int32, (row_count, row_count), 1
    )
    diagonal = jnp.where(diagonal, 1.0, 0.0).astype(jnp.bfloat16)
    picked = lax.dot_general(diagonal, named, by_last, preferred_element_type=jnp.float32) > 0.5
    masked = jnp.where(picked, logits, -jnp.inf)
    raised = jnp.exp(masked - jnp.max(masked, axis=-1, keepdims=True))
    mixing = raised / jnp.sum(raised, axis=-1, keepdims=True)
    high = mixing.astype(jnp.bfloat16)
    low = (mixing - high.astype(jnp.float32)).astype(jnp.bfloat16)
    source = lax.broadcasted_iota(jnp.int32, (count, 128), 0)
    place = lax.broadcasted_iota(jnp.int32, (count, 128), 1)
    at_high = jnp.where(place == source, 1.0, 0.0).astype(jnp.bfloat16)
    at_low = jnp.where(place == source + count, 1.0, 0.0).astype(jnp.bfloat16)
    shares = jnp.dot(high, at_high, preferred_element_type=jnp.float32) + jnp.dot(
        low, at_low, preferred_element_type=jnp.float32
    )
    rows[me, :, width:] = shares.astype(jnp.bfloat16)

    @pl.loop(0, count)
    def _(e):
        for m in range(2):
            loading(m, e).wait()
            turned = load[m, e].T.reshape(count, share, depth)
            stage[m, :, pl.ds(pl.multiple_of(e * share, share), share), :] = turned

    pl.semaphore_wait(barrier, len(peers))

    def remote(src, dst, send, recv, target):
        return pltpu.make_async_remote_copy(
            src_ref=src, dst_ref=dst, send_sem=send, recv_sem=recv, device_id=target, device_id_type=MESH
        )

    def row_copy(kind, block, target):
        return remote(
            rows.at[block], rows.at[block], send_rows.at[kind, block], recv_rows.at[block], (group, target)
        )

    def row_wait(block):
        row_copy(0, block, me ^ 1).wait_recv()

    has_up, has_down = me + 4 < count, me >= 4

    @pl.when(has_up)
    def _():
        row_copy(0, me, me + 4).start()

    @pl.when(has_down)
    def _():
        row_copy(1, me, me - 4).start()

    row_copy(2, me, me ^ 2).start()
    row_copy(3, me, me ^ 1).start()

    def line_step(step):
        below, above = me - 4 * (step + 1), me + 4 * (step + 1)

        @pl.when(below >= 0)
        def _():
            row_wait(below)

            @pl.when(has_up)
            def _():
                row_copy(0, below, me + 4).start()

            row_copy(2, below, me ^ 2).start()
            row_copy(3, below, me ^ 1).start()

        @pl.when(above < count)
        def _():
            row_wait(above)

            @pl.when(has_down)
            def _():
                row_copy(1, above, me - 4).start()

            row_copy(2, above, me ^ 2).start()
            row_copy(3, above, me ^ 1).start()

    def side_step():
        for index in range(line):
            block = (lax.rem(me, 4) ^ 2) + 4 * index
            row_wait(block)
            row_copy(3, block, me ^ 1).start()

    def rows_ready():
        for index in range(line):
            for y in range(2):
                row_wait(4 * index + 2 * y + (lax.rem(me, 2) ^ 1))

    def lanes_of(owner):
        return pl.ds(pl.multiple_of(owner * depth, depth), depth)

    def across(m, r):
        target = me ^ r
        index = m if r < NEAR else group
        slot = m if r < NEAR else 0
        return remote(
            stage.at[index, target], wt.at[index, :, lanes_of(me)],
            send_w.at[slot, r], recv_w.at[slot, r], (group, target),
        )

    def onward(r):
        held = me ^ r
        ref = wt.at[group, :, lanes_of(held)]
        return remote(ref, ref, send_x.at[r], recv_x.at[r], (other_group, me))

    def start_weight(r):
        for m in range(2 if r < NEAR else 1):
            across(m, r).start()

    def pass_on(r):
        for m in range(2 if r < NEAR else 1):
            across(m, r).wait_recv()
        if r >= NEAR:
            onward(r).start()

    for m in range(2):
        wt[m, :, lanes_of(me)] = stage[m, me]

    tile = 256
    tiles = total_f // tile
    chunk = 512
    chunks = tokens // chunk
    blocks = chunk // row_count

    def accumulate(r, first):
        base = pl.multiple_of(((me ^ r) // 2) * (2 * depth), 2 * depth)

        def add_product(m):
            @pl.loop(0, chunks)
            def _(c):
                x = rows[pl.ds(c * blocks, blocks), :, pl.ds(base, 2 * depth)].reshape(chunk, 2 * depth)
                weight = wt[m, :, pl.ds(base, 2 * depth)]
                product = lax.dot_general(x, weight, by_last, preferred_element_type=jnp.float32)
                at = pl.ds(pl.multiple_of(c * chunk, chunk), chunk)
                if first:
                    acc[m, at, :] = product
                else:
                    acc[m, at, :] = acc[m, at, :] + product

        add_product(group)
        for q in (r, r ^ 1):
            if q >= NEAR:
                onward(q).wait_recv()
        add_product(other_group)

    def attend_here():
        for copy in small[4:9]:
            copy.wait()
        seq_count = queries.shape[0]
        group_size = HEADS // KV_HEADS
        shape = (group_size * seq_count, 1)
        seq = jnp.bitwise_and(lax.broadcasted_iota(jnp.int32, shape, 0), seq_count - 1)
        lengths = jnp.zeros(shape, jnp.int32)
        for s in range(seq_count):
            lengths = jnp.where(seq == s, lengths_ref[s], lengths)
        span = seq_count * CTX
        position = lax.broadcasted_iota(jnp.int32, (shape[0], span), 1) - seq * CTX
        visible = jnp.logical_and(position >= 0, position < lengths)
        score_scale = 1.0 / math.sqrt(HEAD_DIM)

        def columns_of(index):
            return slice(index * HEAD_DIM, (index + 1) * HEAD_DIM)

        for g in range(KV_HEADS):
            mine = [queries[:, columns_of(g * group_size + h)].astype(jnp.float32) for h in range(group_size)]
            asked = jnp.concatenate(mine, axis=0)
            key = keys[:, :, columns_of(g)].reshape(span, HEAD_DIM)
            value = cached[:, :, columns_of(g)].reshape(span, HEAD_DIM)
            fresh_key = jnp.concatenate([new_key[:, columns_of(g)].astype(jnp.float32)] * group_size, axis=0)
            fresh_value = jnp.concatenate([new_value[:, columns_of(g)].astype(jnp.float32)] * group_size, axis=0)
            scores = score_scale * lax.dot_general(
                asked.astype(jnp.bfloat16), key, by_last, preferred_element_type=jnp.float32
            )
            scores = jnp.where(visible, scores, -1e30)
            own_score = jnp.sum(asked * fresh_key, axis=-1, keepdims=True) * score_scale
            largest = jnp.maximum(jnp.max(scores, axis=-1, keepdims=True), own_score)
            cached_exp = jnp.exp(scores - largest)
            own_exp = jnp.exp(own_score - largest)
            prob_total = jnp.sum(cached_exp, axis=-1, keepdims=True) + own_exp
            cached_prob = (cached_exp / prob_total).astype(jnp.bfloat16)
            own_prob = (own_exp / prob_total).astype(jnp.bfloat16).astype(jnp.float32)
            context = jnp.dot(cached_prob, value, preferred_element_type=jnp.float32) + own_prob * fresh_value
            for h in range(group_size):
                attended_ref[:, columns_of(g * group_size + h)] = context[
                    h * seq_count : (h + 1) * seq_count, :
                ].astype(attended_ref.dtype)

    by_distance = [[NEAR * d + i for i in range(NEAR)] for d in range(1, line)]
    by_distance = by_distance[1:] + by_distance[:1]
    far = []
    for i in range(0, NEAR, 2):
        pairs = [group_of[i : i + 2] for group_of in by_distance]
        far += [pair[0] for pair in pairs[:-1]] + [pairs[0][1], pairs[-1][0]]
        far += [pair[1] for pair in pairs[1:]]
    order = list(range(1, NEAR)) + far
    row_at = [1 + ROW_SPACING * step for step in range(line - 1)]
    side_at = row_at[-1] + 1
    compute_from = side_at + 1

    for r in range(1, NEAR):
        start_weight(r)

    complete = []

    def advance(i):
        r = far[i]
        pass_on(r)
        if r ^ 1 in far[:i]:
            complete.append((i, r))

    def rows_and_near():
        rows_ready()
        for r in range(1, NEAR):
            pass_on(r)
        accumulate(0, True)
        for r in range(2, NEAR, 2):
            accumulate(r, False)

    def compute(i):
        while complete and complete[0][0] + LAG <= i:
            accumulate(complete.pop(0)[1], False)

    for i, r in enumerate(far):
        if i in row_at:
            line_step(row_at.index(i))
        if i == side_at:
            side_step()
        start_weight(r)
        if i == 0:
            attend_here()
        if i == compute_from:
            rows_and_near()
        if i >= FUSED_AHEAD:
            advance(i - FUSED_AHEAD)
        if i > compute_from:
            compute(i - FUSED_AHEAD)
    for i in range(len(far) - FUSED_AHEAD, len(far)):
        advance(i)
        compute(i)
    compute(len(far) + LAG)

    spread_at = lax.broadcasted_iota(jnp.int32, (128, total_f), 0)
    column = lax.broadcasted_iota(jnp.int32, (128, total_f), 1)
    expert = jnp.where(spread_at < count, spread_at, spread_at - count)
    inside = jnp.logical_and(column >= expert * share, column < expert * share + share)
    spread = jnp.where(jnp.logical_and(inside, spread_at < 2 * count), 1.0, 0.0).astype(jnp.bfloat16)

    place_in_layer = lax.rem(me, 4)
    side, core = place_in_layer // 2, lax.rem(place_in_layer, 2)
    first, second = pl.ds(0, first_columns), pl.ds(first_columns, width - first_columns)
    small[9].wait()
    table = []
    for own in range(line):
        seen = []
        for d in range(line - 1, 0, -1):
            seen += [own + d] * (own + d < line) + [own - d] * (own - d >= 0)
        table.append(seen + [own])

    def turn(j):
        at = jnp.int32(0)
        for own in range(line):
            at = at + (layer == own).astype(jnp.int32) * table[own][j]
        return at

    def make_part(at):
        @pl.loop(0, 4)
        def _(b):
            block = at * 4 + b
            mix = jnp.dot(rows[block, :, width:], spread, preferred_element_type=jnp.float32)
            here = pl.ds(pl.multiple_of(block * row_count, row_count), row_count)
            there = pl.ds(pl.multiple_of(b * row_count, row_count), row_count)
            for n in range(tiles):
                columns = slice(n * tile, (n + 1) * tile)
                gate_proj = acc[0, here, columns]
                up_proj = acc[1, here, columns]
                hidden = gate_proj / (1.0 + jnp.exp(-gate_proj)) * up_proj * mix[:, columns]
                units[there, columns] = hidden.astype(units.dtype)

        wide = 2 * tile

        @pl.loop(0, width // wide)
        def _(n):
            columns = pl.ds(pl.multiple_of(n * wide, wide), wide)
            product = jnp.dot(units[...], down[:, columns], preferred_element_type=jnp.float32)
            part[pl.ds(at * 4, 4), :, columns] = product.astype(part.dtype).reshape(4, row_count, wide)

    def add(target, *sources):
        @pl.loop(0, row_count // 16)
        def _(step):
            here = pl.ds(pl.multiple_of(step * 16, 16), 16)
            total = sources[0][here, :].astype(jnp.float32)
            for source in sources[1:]:
                total = total + source[here, :].astype(jnp.float32)
            target[here, :] = total.astype(target.dtype)

    def core_copy(at, y):
        slot = at * 2 + y
        return remote(
            part.at[at * 4 + y * 2 + (core ^ 1)], core_in.at[slot], core_send.at[slot], core_recv.at[slot], (group, me ^ 1)
        )

    def line_copy(kind, at):
        src, dst, target = (
            (side_out, side_in, me ^ 2),
            (early_up_out, early_up_in, me + 4),
            (early_down_out, early_down_in, me - 4),
            (late_up_out, late_up_in, me + 4),
            (late_down_out, late_down_in, me - 4),
        )[kind]
        return remote(src.at[at], dst.at[at], line_send.at[kind, at], line_recv.at[kind, at], (group, target))

    def last_copy():
        return remote(last_out, last_in, last_send.at[0], last_recv.at[0], (group, me ^ 2))

    def held(at, y, columns):
        return part.at[at * 4 + y * 2 + core, :, columns], core_in.at[at * 2 + y, :, columns]

    def to_side(at):
        for y in range(2):
            core_copy(at, y).wait_recv()
        add(side_out.at[at], *held(at, side ^ 1, first))
        line_copy(0, at).start()

    def step_along(at, kinds, sources, starting, passing):
        for kind, has_source, moving in ((kinds[0], has_down, at > layer), (kinds[1], has_up, at < layer)):
            def pass_sum():
                line_copy(kind, at).wait_recv()
                sources(kind, True)
                line_copy(kind, at).start()

            def start_sum():
                sources(kind, False)
                line_copy(kind, at).start()

            if passing:
                pl.when(jnp.logical_and(moving, has_source))(pass_sum)
            if starting:
                pl.when(jnp.logical_and(moving, jnp.logical_not(has_source)))(start_sum)

    def early(at, starting):
        def sources(kind, arriving):
            out, arrived = ((early_up_out, early_up_in), (early_down_out, early_down_in))[kind - 1]
            for y in range(2):
                more = (arrived.at[at, y],) if arriving else ()
                add(out.at[at, y], *held(at, y, second), *more)

        step_along(at, (1, 2), sources, starting, not starting)

    def late(at):
        line_copy(0, at).wait_recv()

        def sources(kind, arriving):
            out, arrived = ((late_up_out, late_up_in), (late_down_out, late_down_in))[kind - 3]
            more = (arrived.at[at],) if arriving else ()
            add(out.at[at], *held(at, side, first), side_in.at[at], *more)

        step_along(at, (3, 4), sources, True, True)

    def arrived_from(kinds, act):
        @pl.when(has_down)
        def _():
            line_copy(kinds[0], layer).wait_recv()

        @pl.when(has_up)
        def _():
            line_copy(kinds[1], layer).wait_recv()

        for down_too, up_too in ((True, True), (True, False), (False, True)):
            matches = jnp.logical_and(has_down == down_too, has_up == up_too)
            pl.when(matches)(functools.partial(act, down_too, up_too))

    for j in range(line):
        at = turn(j)
        make_part(at)
        core_copy(at, side ^ 1).start()
        core_copy(at, side).start()
        if j:
            to_side(turn(j - 1))
            early(turn(j - 1), True)
    to_side(turn(line - 1))
    for j in range(line - 1):
        early(turn(j), False)
    for j in range(line - 1):
        late(turn(j))
    line_copy(0, layer).wait_recv()

    def sum_early(down_too, up_too):
        for y, target in ((side ^ 1, last_out), (side, out_ref.at[:, second])):
            more = [ref.at[layer, y] for ref, on in ((early_up_in, down_too), (early_down_in, up_too)) if on]
            add(target, *held(layer, y, second), *more)

    def sum_late(down_too, up_too):
        more = [ref.at[layer] for ref, on in ((late_up_in, down_too), (late_down_in, up_too)) if on]
        add(out_ref.at[:, first], *held(layer, side, first), side_in.at[layer], *more)

    arrived_from((1, 2), sum_early)
    last_copy().start()
    arrived_from((3, 4), sum_late)
    last_copy().wait_recv()
    add(out_ref.at[:, second], out_ref.at[:, second], last_in)

    last_copy().wait_send()
    for at in range(line):
        for y in range(2):
            core_copy(at, y).wait_send()
        line_copy(0, at).wait_send()
        for up_kind in (1, 3):
            pl.when(at > layer)(line_copy(up_kind, at).wait_send)
            pl.when(at < layer)(line_copy(up_kind + 1, at).wait_send)
    for r in order:
        for m in range(2 if r < NEAR else 1):
            across(m, r).wait_send()
        if r >= NEAR:
            onward(r).wait_send()
    for index in range(line):
        block = lax.rem(me, 4) + 4 * index

        @pl.when(jnp.logical_and(has_up, index <= layer))
        def _():
            row_copy(0, block, me ^ 1).wait_send()

        @pl.when(jnp.logical_and(has_down, index >= layer))
        def _():
            row_copy(1, block, me ^ 1).wait_send()

        row_copy(2, block, me ^ 1).wait_send()
        row_copy(3, block, me ^ 1).wait_send()
        row_copy(3, block ^ 2, me ^ 1).wait_send()


def fused(
    queries, key_cache, value_cache, new_key, new_value, cache_lengths,
    hidden_in, norm_gain, router_weight, expert_ids, gate_train, up_train, down_train,
):
    count, depth, total_f = gate_train.shape
    row_count, width = hidden_in.shape
    line = count // 4
    first_columns = width * 13 // (16 * 128) * 128
    second_columns = width - first_columns
    anywhere = pl.BlockSpec(memory_space=pl.ANY)
    near = pl.BlockSpec(memory_space=pltpu.VMEM)
    DMA = pltpu.SemaphoreType.DMA
    like = lambda x: pltpu.VMEM(x.shape, x.dtype)
    held = lambda *shape: pltpu.VMEM(shape, jnp.bfloat16)
    router_turned, ids_turned = router_weight.T, expert_ids.T
    down_rows = down_train.reshape(-1, width)
    return pl.pallas_call(
        functools.partial(fused_kernel, count, first_columns),
        out_shape=[
            jax.ShapeDtypeStruct(queries.shape, jnp.bfloat16),
            jax.ShapeDtypeStruct((row_count, width), jnp.bfloat16),
        ],
        in_specs=[pl.BlockSpec(memory_space=pltpu.SMEM)] + [anywhere] * 12,
        out_specs=[near, near],
        scratch_shapes=[
            like(queries), like(key_cache), like(value_cache), like(new_key), like(new_value),
            like(hidden_in), like(norm_gain), like(router_turned), like(ids_turned), like(down_rows),
            held(2, count, depth, total_f),
            held(2, count, total_f, depth),
            held(2, total_f, count * depth),
            held(count, row_count, width + 128),
            pltpu.VMEM((2, count * row_count, total_f), jnp.float32),
            held(4 * row_count, total_f),
            held(count, row_count, width),
            held(2 * line, row_count, width),
            held(line, row_count, first_columns), held(line, row_count, first_columns),
            *[held(line, 2, row_count, second_columns)] * 4,
            *[held(line, row_count, first_columns)] * 4,
            held(row_count, second_columns), held(row_count, second_columns),
            DMA((10,)), DMA((2, count)), DMA((2, count)), DMA((2, count)), DMA((count,)), DMA((count,)),
            DMA((4, count)), DMA((count,)),
            DMA((2 * line,)), DMA((2 * line,)), DMA((5, line)), DMA((5, line)), DMA((1,)), DMA((1,)),
        ],
        compiler_params=pltpu.CompilerParams(collective_id=2, has_side_effects=True, vmem_limit_bytes=63 * 2**20),
    )(
        cache_lengths, queries, key_cache, value_cache, new_key, new_value,
        hidden_in, norm_gain, router_turned, ids_turned, gate_train, up_train, down_rows,
    )


def local(
    queries,
    key_cache,
    value_cache,
    new_key,
    new_value,
    cache_lengths,
    hidden_in,
    norm_gain,
    router_weight,
    expert_ids,
    gate_train,
    up_train,
    down_train,
):
    width = hidden_in.shape[1]
    expert_count = router_weight.shape[1]
    groups = lax.axis_size("groups")
    if dims_fit(groups, expert_count, gate_train, down_train, hidden_in.shape[0]) and queries.shape[0] == 8:
        return tuple(fused(
            queries, key_cache, value_cache, new_key, new_value, cache_lengths,
            hidden_in, norm_gain, router_weight, expert_ids, gate_train, up_train, down_train,
        ))
    normed = rms_normed(hidden_in, norm_gain)
    mixing = dense_mixing(normed, router_weight, expert_ids)
    mixing_high = mixing.astype(jnp.bfloat16)
    mixing_low = (mixing - mixing_high.astype(jnp.float32)).astype(jnp.bfloat16)
    spare = -2 * expert_count % 128
    row_block = jnp.concatenate(
        [normed, mixing_high, mixing_low, jnp.zeros((normed.shape[0], spare), jnp.bfloat16)], axis=1
    )
    hidden_units, down_moved = move(groups, gate_train, up_train, down_train, row_block)
    down_moved = down_moved.reshape(-1, width)
    attended = attend(queries, key_cache, value_cache, new_key, new_value, cache_lengths)
    partial_out = jnp.dot(hidden_units, down_moved, preferred_element_type=jnp.float32).astype(jnp.bfloat16)
    mixed_out = summed(partial_out, expert_count)
    return (attended, mixed_out)


def solution(mesh):
    placed = (
        P(("groups", "expert"), None),
        P(("groups", "expert"), None, None),
        P(("groups", "expert"), None, None),
        P(("groups", "expert"), None),
        P(("groups", "expert"), None),
        P(("groups", "expert")),
        P(("groups", "expert"), None),
        P(),
        P(),
        P(("groups", "expert"), None),
        P(None, "expert", None),
        P(None, "expert", None),
        P(None, "expert", None),
    )
    return jax.shard_map(
        local,
        mesh=mesh,
        in_specs=placed,
        out_specs=(P(("groups", "expert"), None), P(("groups", "expert"), None)),
        check_vma=False,
    )
```

```python
import functools
import math

import jax
import jax.numpy as jnp
from jax import lax
from jax.experimental import pallas as pl
from jax.experimental.pallas import tpu as pltpu
from jax.sharding import PartitionSpec as P

HEADS = 32
KV_HEADS = 4
HEAD_DIM = 128
CTX = 64


EPSILON = 1e-06


def rms_normed(hidden_in, norm_gain):
    values = hidden_in.astype(jnp.float32)
    mean_square = jnp.mean(values * values, axis=-1, keepdims=True)
    return (values * lax.rsqrt(mean_square + EPSILON) * norm_gain.astype(jnp.float32)).astype(
        jnp.bfloat16
    )


def attend(queries, key_cache, value_cache, new_key, new_value, cache_lengths):
    seq_count = queries.shape[0]
    group_size = HEADS // KV_HEADS
    query_blocks = queries.reshape(seq_count, KV_HEADS, group_size, HEAD_DIM)
    cached_keys = key_cache.reshape(seq_count, CTX, KV_HEADS, HEAD_DIM)
    cached_values = value_cache.reshape(seq_count, CTX, KV_HEADS, HEAD_DIM)
    fresh_keys = new_key.reshape(seq_count, KV_HEADS, HEAD_DIM)
    fresh_values = new_value.astype(jnp.float32).reshape(seq_count, KV_HEADS, HEAD_DIM)
    score_scale = 1.0 / math.sqrt(HEAD_DIM)
    scores = (
        jnp.einsum("sgrd,scgd->sgrc", query_blocks, cached_keys, preferred_element_type=jnp.float32)
        * score_scale
    )
    own_score = (
        jnp.einsum("sgrd,sgd->sgr", query_blocks, fresh_keys, preferred_element_type=jnp.float32)
        * score_scale
    )
    positions = jnp.arange(CTX, dtype=jnp.int32)
    visible = positions[None, :] < cache_lengths[:, None]
    scores = jnp.where(visible[:, None, None, :], scores, -1e30)
    largest = jnp.maximum(jnp.max(scores, axis=-1), own_score)
    cached_exp = jnp.exp(scores - largest[..., None])
    own_exp = jnp.exp(own_score - largest)
    prob_total = jnp.sum(cached_exp, axis=-1) + own_exp
    cached_prob = (cached_exp / prob_total[..., None]).astype(jnp.bfloat16)
    own_prob = (own_exp / prob_total).astype(jnp.bfloat16).astype(jnp.float32)
    context = jnp.einsum(
        "sgrc,scgd->sgrd", cached_prob, cached_values, preferred_element_type=jnp.float32
    )
    context = context + own_prob[..., None] * fresh_values[:, :, None, :]
    return context.reshape(seq_count, HEADS * HEAD_DIM).astype(jnp.bfloat16)


def dense_mixing(normed, router_weight, expert_ids):
    logits = jnp.dot(normed, router_weight, preferred_element_type=jnp.float32)
    expert_range = jnp.arange(router_weight.shape[1], dtype=jnp.int32)
    picked = jnp.any(expert_ids[:, :, None] == expert_range[None, None, :], axis=1)
    masked = jnp.where(picked, logits, -jnp.inf)
    raised = jnp.exp(masked - jnp.max(masked, axis=-1, keepdims=True))
    return raised / jnp.sum(raised, axis=-1, keepdims=True)


MESH = pl.DeviceIdType.MESH
AHEAD = 4
NEAR = 4
LAG = 2
FUSED_AHEAD = 4
ROW_FIRST = 2
ROW_SPACING = 4
SIDE_AFTER = 2
PIECES = 2
FIRST = 2


def greet(targets):
    barrier = pltpu.get_barrier_semaphore()

    expected = 0
    for condition, target in targets:
        signal = functools.partial(
            pl.semaphore_signal, barrier, inc=1, device_id=target, device_id_type=MESH
        )
        if condition is None:
            signal()
            expected = expected + 1
        else:
            pl.when(condition)(signal)
            expected = expected + condition.astype(jnp.int32)
    pl.semaphore_wait(barrier, expected)


def move_kernel(
    groups, count,
    gate_ref, up_ref, down_ref, rows_ref,
    hidden_ref, down_out, gate_out, up_out, rows_out,
    send_w, recv_w, send_x, recv_x, local_sem, send_rows, recv_rows,
):
    me = lax.axis_index("expert")
    group = lax.axis_index("groups")
    parts = max(1, groups // 2)
    part_rows = gate_ref.shape[1] // parts
    part_columns = down_ref.shape[2] // groups
    line = count // 4
    layer = me // 4

    others = [(None, (group, me ^ r)) for r in range(1, count)]
    others += [(None, (lax.rem(group + h, groups), me)) for h in range(1, groups)]
    greet(others)

    def remote(src, dst, send, recv, target):
        return pltpu.make_async_remote_copy(
            src_ref=src, dst_ref=dst, send_sem=send, recv_sem=recv, device_id=target, device_id_type=MESH
        )

    def rows_of(owner):
        return pl.ds(pl.multiple_of((owner // 2) * part_rows, part_rows), part_rows)

    def columns_of(owner):
        return pl.ds(pl.multiple_of(owner * part_columns, part_columns), part_columns)

    def row_copy(kind, block, target, own=False):
        source = rows_ref if own else rows_out.at[block]
        return remote(
            source, rows_out.at[block], send_rows.at[kind, block], recv_rows.at[block], (group, target)
        )

    def row_wait(block):
        row_copy(0, block, me ^ 1).wait_recv()

    own_rows = pltpu.make_async_copy(rows_ref, rows_out.at[me], local_sem.at[3])
    own_rows.start()
    has_up, has_down = me + 4 < count, me >= 4

    @pl.when(has_up)
    def _():
        row_copy(0, me, me + 4, True).start()

    @pl.when(has_down)
    def _():
        row_copy(1, me, me - 4, True).start()

    row_copy(2, me, me ^ 2, True).start()
    row_copy(3, me, me ^ 1, True).start()

    def line_step(step):
        below, above = me - 4 * (step + 1), me + 4 * (step + 1)

        @pl.when(below >= 0)
        def _():
            row_wait(below)

            @pl.when(has_up)
            def _():
                row_copy(0, below, me + 4).start()

            row_copy(2, below, me ^ 2).start()
            row_copy(3, below, me ^ 1).start()

        @pl.when(above < count)
        def _():
            row_wait(above)

            @pl.when(has_down)
            def _():
                row_copy(1, above, me - 4).start()

            row_copy(2, above, me ^ 2).start()
            row_copy(3, above, me ^ 1).start()

    def side_step(index):
        block = lax.rem(me, 4) ^ 2
        block = block + 4 * index
        row_wait(block)
        row_copy(3, block, me ^ 1).start()

    def across(kind, r, refs_in, refs_out, which):
        target = me ^ r
        if r < NEAR:
            a, b = ((gate_ref, gate_out), (down_ref, down_out), (up_ref, up_out))[kind]
            send = send_x.at[0, r, 0] if kind == 2 else send_w.at[kind, r]
            recv = recv_x.at[0, r, 0] if kind == 2 else recv_w.at[kind, r]
            return remote(a.at[target], b.at[me], send, recv, (group, target))
        if kind == 0:
            return remote(
                refs_in[which].at[target, rows_of(group)], refs_out[which].at[me, rows_of(group)],
                send_w.at[0, r], recv_w.at[0, r], (group, target),
            )
        return remote(
            down_ref.at[target, :, columns_of(group)], down_out.at[me, :, columns_of(group)],
            send_w.at[1, r], recv_w.at[1, r], (group, target),
        )

    ins, outs = (gate_ref, up_ref), (gate_out, up_out)

    def by_matrix(act):
        pl.when(lax.rem(group, 2) == 0)(functools.partial(act, 0))
        pl.when(lax.rem(group, 2) == 1)(functools.partial(act, 1))

    def start_weight(kind, r):
        if kind == 0 and r >= NEAR:
            by_matrix(lambda which: across(0, r, ins, outs, which).start())
        else:
            across(kind, r, ins, outs, 0).start()

    def onward(kind, r, h, which):
        held = me ^ r
        place = outs[which].at[held, rows_of(group)] if kind == 0 else down_out.at[held, :, columns_of(group)]
        return remote(
            place, place, send_x.at[kind, r, h - 1], recv_x.at[kind, r, h - 1],
            (lax.rem(group + h, groups), me),
        )

    def pass_on(kind, r):
        across(kind, r, ins, outs, 0).wait_recv()
        for h in range(1, groups if r >= NEAR else 1):
            if kind == 0:
                by_matrix(lambda which: onward(0, r, h, which).start())
            else:
                onward(1, r, h, 0).start()

    own_copies = [
        pltpu.make_async_copy(a.at[me], b.at[me], local_sem.at[i])
        for i, (a, b) in enumerate(((gate_ref, gate_out), (up_ref, up_out), (down_ref, down_out)))
    ]
    width = gate_ref.shape[1] * count

    def ready():
        for index in range(line):
            for y in range(2):
                row_wait(4 * index + 2 * y + (lax.rem(me, 2) ^ 1))
        own_rows.wait()
        for copy in own_copies[:2]:
            copy.wait()
        for r in order:
            for h in range(1, groups if r >= NEAR else 1):
                onward(0, r, h, 0).wait_recv()

    def expert_rows(quarter):
        @pl.loop(0, count // 16)
        def _(step):
            at = quarter * (count // 4) + step * 4
            rows = rows_out[pl.ds(at, 4)].reshape(-1, rows_out.shape[2])
            tokens = rows[:, :width]
            shares = rows[:, width:].astype(jnp.float32)
            lane = lax.broadcasted_iota(jnp.int32, shares.shape, 1)
            own = jnp.logical_or(lane == me, lane == me + count)
            own_mix = jnp.sum(jnp.where(own, shares, 0.0), axis=1, keepdims=True)
            gate = gate_out[...].reshape(width, -1)
            gate_proj = jnp.dot(tokens, gate, preferred_element_type=jnp.float32)
            up = up_out[...].reshape(width, -1)
            up_proj = jnp.dot(tokens, up, preferred_element_type=jnp.float32)
            hidden = gate_proj / (1.0 + jnp.exp(-gate_proj)) * up_proj * own_mix
            place = pl.ds(pl.multiple_of(at * rows_out.shape[1], rows.shape[0]), rows.shape[0])
            hidden_ref[place, :] = hidden.astype(hidden_ref.dtype)

    half = count // 2
    order = [r for i in range(half) for r in ((half + i, i) if i else (half,))]
    first = [(kind, r) for r in order for kind in ((0, 2) if r < NEAR else (0,))]
    items = first + [(1, r) for r in order]
    spacing = len(items) // (line + 1)
    side_at = 2 + spacing * (line - 1) + 3

    def advance(i):
        pass_on(*items[i])
        before_last = len(items) - 1 - i
        if before_last % 2 == 0 and before_last < 8:
            if before_last == 6:
                ready()
            expert_rows(3 - before_last // 2)

    for i, item in enumerate(items):
        start_weight(*item)
        if i >= 2 and (i - 2) % spacing == 0 and (i - 2) // spacing < line - 1:
            line_step((i - 2) // spacing)
        if i == side_at:
            for index in range(line):
                side_step(index)
        if i == AHEAD:
            for copy in own_copies:
                copy.start()
        if i >= AHEAD:
            advance(i - AHEAD)
    for i in range(len(items) - AHEAD, len(items)):
        advance(i)

    own_copies[2].wait()
    for kind, r in items:
        across(kind, r, ins, outs, 0).wait_send()
        for h in range(1, groups if r >= NEAR else 1):
            onward(kind, r, h, 0).wait_send()
            if kind == 1:
                onward(kind, r, h, 0).wait_recv()
    for index in range(line):
        block = lax.rem(me, 4) + 4 * index

        @pl.when(jnp.logical_and(has_up, index <= layer))
        def _():
            row_copy(0, block, me ^ 1).wait_send()

        @pl.when(jnp.logical_and(has_down, index >= layer))
        def _():
            row_copy(1, block, me ^ 1).wait_send()

        row_copy(2, block, me ^ 1).wait_send()
        row_copy(3, block, me ^ 1).wait_send()
        row_copy(3, block ^ 2, me ^ 1).wait_send()


def move(groups, gate_train, up_train, down_train, row_block):
    count = gate_train.shape[0]
    anywhere = pl.BlockSpec(memory_space=pl.ANY)
    DMA = pltpu.SemaphoreType.DMA
    return pl.pallas_call(
        functools.partial(move_kernel, groups, count),
        out_shape=[
            jax.ShapeDtypeStruct((count * row_block.shape[0], gate_train.shape[2]), jnp.bfloat16),
            jax.ShapeDtypeStruct(down_train.shape, down_train.dtype),
        ],
        in_specs=[anywhere, anywhere, anywhere, pl.BlockSpec(memory_space=pltpu.VMEM)],
        out_specs=[pl.BlockSpec(memory_space=pltpu.VMEM), anywhere],
        scratch_shapes=[
            pltpu.VMEM(gate_train.shape, gate_train.dtype),
            pltpu.VMEM(up_train.shape, up_train.dtype),
            pltpu.VMEM((count,) + row_block.shape, row_block.dtype),
            DMA((2, count)), DMA((2, count)),
            DMA((2, count, max(1, groups - 1))), DMA((2, count, max(1, groups - 1))),
            DMA((4,)), DMA((4, count)), DMA((count,)),
        ],
        compiler_params=pltpu.CompilerParams(collective_id=0, has_side_effects=True, vmem_limit_bytes=60 * 2**20),
    )(gate_train, up_train, down_train, row_block)


def sum_kernel(
    count, part_ref, out_ref, core_in, side_in, up_in, down_in, side_out, up_out, down_out,
    core_send, core_recv, side_send, side_recv, up_send, up_recv, down_send, down_recv,
):
    me = lax.axis_index("expert")
    group = lax.axis_index("groups")
    line, layer = count // 4, me // 4
    place = lax.rem(me, 4)
    side, core = place // 2, lax.rem(place, 2)
    has_up, has_down = me + 4 < count, me >= 4
    greet([
        (None, (group, me ^ 1)), (None, (group, me ^ 2)),
        (has_up, (group, me + 4)), (has_down, (group, me - 4)),
    ])
    chunk = 16
    row_count = part_ref.shape[1]

    def remote(src, dst, send, recv, target):
        return pltpu.make_async_remote_copy(
            src_ref=src, dst_ref=dst, send_sem=send, recv_sem=recv, device_id=(group, target), device_id_type=MESH
        )

    def add(target, *sources):
        @pl.loop(0, row_count // chunk)
        def _(step):
            rows = pl.ds(pl.multiple_of(step * chunk, chunk), chunk)
            total = sources[0][rows, :].astype(jnp.float32)
            for source in sources[1:]:
                total = total + source[rows, :].astype(jnp.float32)
            target[rows, :] = total.astype(target.dtype)

    def core_copy(at, y):
        slot = at * 2 + y
        return remote(
            part_ref.at[at * 4 + y * 2 + (core ^ 1)], core_in.at[slot], core_send.at[slot], core_recv.at[slot], me ^ 1
        )

    def side_copy(at):
        return remote(side_out.at[at], side_in.at[at], side_send.at[at], side_recv.at[at], me ^ 2)

    def up_copy(at):
        return remote(up_out.at[at], up_in.at[at], up_send.at[at], up_recv.at[at], me + 4)

    def down_copy(at):
        return remote(down_out.at[at], down_in.at[at], down_send.at[at], down_recv.at[at], me - 4)

    def in_order(act):
        for d in range(line - 1, 0, -1):
            pl.when(layer + d < line)(functools.partial(act, layer + d, 1))
            pl.when(layer - d >= 0)(functools.partial(act, layer - d, -1))
        act(layer, 0)

    in_order(lambda at, way: core_copy(at, side ^ 1).start())
    in_order(lambda at, way: core_copy(at, side).start())

    def to_side(at, way):
        core_copy(at, side ^ 1).wait_recv()
        add(side_out.at[at], part_ref.at[at * 4 + (side ^ 1) * 2 + core], core_in.at[at * 2 + (side ^ 1)])
        side_copy(at).start()

    in_order(to_side)

    def along(at, way):
        core_copy(at, side).wait_recv()
        side_copy(at).wait_recv()
        mine = (part_ref.at[at * 4 + place], core_in.at[at * 2 + side], side_in.at[at])
        if way == 1:
            @pl.when(has_down)
            def _():
                up_copy(at).wait_recv()
                add(up_out.at[at], *mine, up_in.at[at])

            @pl.when(jnp.logical_not(has_down))
            def _():
                add(up_out.at[at], *mine)

            up_copy(at).start()
        elif way == -1:
            @pl.when(has_up)
            def _():
                down_copy(at).wait_recv()
                add(down_out.at[at], *mine, down_in.at[at])

            @pl.when(jnp.logical_not(has_up))
            def _():
                add(down_out.at[at], *mine)

            down_copy(at).start()
        else:
            @pl.when(has_down)
            def _():
                up_copy(at).wait_recv()

            @pl.when(has_up)
            def _():
                down_copy(at).wait_recv()

            both = jnp.logical_and(has_down, has_up)

            @pl.when(both)
            def _():
                add(out_ref, *mine, up_in.at[at], down_in.at[at])

            @pl.when(jnp.logical_and(has_down, jnp.logical_not(has_up)))
            def _():
                add(out_ref, *mine, up_in.at[at])

            @pl.when(jnp.logical_and(has_up, jnp.logical_not(has_down)))
            def _():
                add(out_ref, *mine, down_in.at[at])

            @pl.when(jnp.logical_not(jnp.logical_or(has_up, has_down)))
            def _():
                add(out_ref, *mine)

    in_order(along)

    def finish(at, way):
        core_copy(at, side ^ 1).wait_send()
        core_copy(at, side).wait_send()
        side_copy(at).wait_send()
        if way == 1:
            up_copy(at).wait_send()
        if way == -1:
            down_copy(at).wait_send()

    in_order(finish)


def summed(partial_out, count):
    rows, width = partial_out.shape[0] // count, partial_out.shape[1]
    line = count // 4
    DMA = pltpu.SemaphoreType.DMA
    block = lambda amount: pltpu.VMEM((amount, rows, width), jnp.bfloat16)
    return pl.pallas_call(
        functools.partial(sum_kernel, count),
        out_shape=jax.ShapeDtypeStruct((rows, width), jnp.bfloat16),
        in_specs=[pl.BlockSpec(memory_space=pltpu.VMEM)],
        out_specs=pl.BlockSpec(memory_space=pltpu.VMEM),
        scratch_shapes=[block(count // 2)] + [block(line)] * 6
        + [DMA((count // 2,)), DMA((count // 2,))] + [DMA((line,))] * 6,
        compiler_params=pltpu.CompilerParams(collective_id=1, has_side_effects=True, vmem_limit_bytes=60 * 2**20),
    )(partial_out.reshape(count, rows, width))


def dims_fit(groups, count, gate_train, down_train, row_count):
    rows, width = gate_train.shape[1], gate_train.shape[2]
    part = down_train.shape[1]
    return (
        groups == 2
        and count % 8 == 0
        and 2 * count <= 128
        and rows % 128 == 0
        and part % 16 == 0
        and part * count == width
        and width % 256 == 0
        and row_count % 16 == 0
        and (count * row_count) % 512 == 0
    )


def fused_kernel(
    count, first_columns, lengths_ref, queries_ref, keys_ref, values_ref, new_key_ref, new_value_ref,
    hidden_in_ref, gain_in_ref, router_in_ref, ids_in_ref, gate_ref, up_ref, down_in_ref,
    attended_ref, out_ref,
    queries, keys, cached, new_key, new_value, hid_ref, gain_ref, router_ref, ids_ref, down,
    load, stage, wt, rows, acc, units, part, core_in, side_out, side_in,
    early_up_out, early_up_in, early_down_out, early_down_in,
    late_up_out, late_up_in, late_down_out, late_down_in, last_out, last_in,
    small_sem, load_sem, send_w, recv_w, send_x, recv_x, send_rows, recv_rows,
    core_send, core_recv, line_send, line_recv, last_send, last_recv,
):
    me = lax.axis_index("expert")
    group = lax.axis_index("groups")
    other_group = 1 - group
    line = count // 4
    layer = me // 4
    row_count, width = hid_ref.shape
    depth = gate_ref.shape[1]
    share = stage.shape[2] // count
    total_f = stage.shape[2]
    tokens = count * row_count

    def loading(m, e):
        return pltpu.make_async_copy((gate_ref, up_ref)[m].at[e], load.at[m, e], load_sem.at[m, e])

    small = [
        pltpu.make_async_copy(src, dst, small_sem.at[i])
        for i, (src, dst) in enumerate((
            (hidden_in_ref, hid_ref), (gain_in_ref, gain_ref), (router_in_ref, router_ref), (ids_in_ref, ids_ref),
            (queries_ref, queries), (keys_ref, keys), (values_ref, cached), (new_key_ref, new_key),
            (new_value_ref, new_value), (down_in_ref, down),
        ))
    ]
    for copy in small[:4]:
        copy.start()
    for e in range(count):
        for m in range(2):
            loading(m, e).start()
    for copy in small[4:]:
        copy.start()

    barrier = pltpu.get_barrier_semaphore()
    peers = [(group, me ^ r) for r in range(1, count)] + [(other_group, me)]
    for peer in peers:
        pl.semaphore_signal(barrier, inc=1, device_id=peer, device_id_type=MESH)

    @pl.loop(0, count)
    def _(e):
        for m in range(2):
            loading(m, e).wait()
            turned = load[m, e].T.reshape(count, share, depth)
            stage[m, :, pl.ds(pl.multiple_of(e * share, share), share), :] = turned

    pl.semaphore_wait(barrier, len(peers))

    def remote(src, dst, send, recv, target):
        return pltpu.make_async_remote_copy(
            src_ref=src, dst_ref=dst, send_sem=send, recv_sem=recv, device_id=target, device_id_type=MESH
        )

    pieces = PIECES
    piece_rows = total_f // pieces

    def lanes_of(owner):
        return pl.ds(pl.multiple_of(owner * depth, depth), depth)

    def rows_of(piece):
        return pl.ds(piece * piece_rows, piece_rows)

    def near_copy(m, r):
        return remote(
            stage.at[m, me ^ r], wt.at[m, :, lanes_of(me)], send_w.at[m, r], recv_w.at[m, r], (group, me ^ r)
        )

    def far_copy(r, piece):
        return remote(
            stage.at[group, me ^ r, rows_of(piece)], wt.at[group, rows_of(piece), lanes_of(me)],
            send_w.at[piece, r], recv_w.at[piece, r], (group, me ^ r),
        )

    def onward(r, piece):
        ref = wt.at[group, rows_of(piece), lanes_of(me ^ r)]
        return remote(ref, ref, send_x.at[piece, r], recv_x.at[piece, r], (other_group, me))

    by_distance = [[NEAR * d + i for i in range(NEAR)] for d in range(1, line)]
    by_distance = by_distance[1:] + by_distance[:1]
    far = []
    for i in range(0, NEAR, 2):
        pairs = [group_of[i : i + 2] for group_of in by_distance]
        far += [pair[0] for pair in pairs[:-1]] + [pairs[0][1], pairs[-1][0]]
        far += [pair[1] for pair in pairs[1:]]
    items = [(r, piece) for r in far for piece in range(pieces)]
    for item in items[:FIRST]:
        far_copy(*item).start()
    for copy in small[:4]:
        copy.wait()
    values = hid_ref[...].astype(jnp.float32)
    mean_square = jnp.mean(values * values, axis=-1, keepdims=True)
    gain = gain_ref[...].astype(jnp.float32).reshape(1, width)
    normed = (values * lax.rsqrt(mean_square + EPSILON) * gain).astype(jnp.bfloat16)
    rows[me, :, :width] = normed
    by_last = (((1,), (1,)), ((), ()))
    logits = lax.dot_general(normed, router_ref[...], by_last, preferred_element_type=jnp.float32)
    ids = ids_ref[...]
    lane = lax.broadcasted_iota(jnp.int32, (count, row_count), 0)
    named = ids[0:1, :] == lane
    for k in range(1, ids.shape[0]):
        named = jnp.logical_or(named, ids[k : k + 1, :] == lane)
    named = jnp.where(named, 1.0, 0.0).astype(jnp.bfloat16)
    diagonal = lax.broadcasted_iota(jnp.int32, (row_count, row_count), 0) == lax.broadcasted_iota(
        jnp.int32, (row_count, row_count), 1
    )
    diagonal = jnp.where(diagonal, 1.0, 0.0).astype(jnp.bfloat16)
    picked = lax.dot_general(diagonal, named, by_last, preferred_element_type=jnp.float32) > 0.5
    masked = jnp.where(picked, logits, -jnp.inf)
    raised = jnp.exp(masked - jnp.max(masked, axis=-1, keepdims=True))
    mixing = raised / jnp.sum(raised, axis=-1, keepdims=True)
    high = mixing.astype(jnp.bfloat16)
    low = (mixing - high.astype(jnp.float32)).astype(jnp.bfloat16)
    source = lax.broadcasted_iota(jnp.int32, (count, 128), 0)
    place = lax.broadcasted_iota(jnp.int32, (count, 128), 1)
    at_high = jnp.where(place == source, 1.0, 0.0).astype(jnp.bfloat16)
    at_low = jnp.where(place == source + count, 1.0, 0.0).astype(jnp.bfloat16)
    shares = jnp.dot(high, at_high, preferred_element_type=jnp.float32) + jnp.dot(
        low, at_low, preferred_element_type=jnp.float32
    )
    rows[me, :, width:] = shares.astype(jnp.bfloat16)

    def row_copy(kind, block, target):
        return remote(
            rows.at[block], rows.at[block], send_rows.at[kind, block], recv_rows.at[block], (group, target)
        )

    def row_wait(block):
        row_copy(0, block, me ^ 1).wait_recv()

    has_up, has_down = me + 4 < count, me >= 4

    @pl.when(has_up)
    def _():
        row_copy(0, me, me + 4).start()

    @pl.when(has_down)
    def _():
        row_copy(1, me, me - 4).start()

    row_copy(2, me, me ^ 2).start()
    row_copy(3, me, me ^ 1).start()

    def line_step(step):
        below, above = me - 4 * (step + 1), me + 4 * (step + 1)

        @pl.when(below >= 0)
        def _():
            row_wait(below)

            @pl.when(has_up)
            def _():
                row_copy(0, below, me + 4).start()

            row_copy(2, below, me ^ 2).start()
            row_copy(3, below, me ^ 1).start()

        @pl.when(above < count)
        def _():
            row_wait(above)

            @pl.when(has_down)
            def _():
                row_copy(1, above, me - 4).start()

            row_copy(2, above, me ^ 2).start()
            row_copy(3, above, me ^ 1).start()

    def side_step():
        for index in range(line):
            block = (lax.rem(me, 4) ^ 2) + 4 * index
            row_wait(block)
            row_copy(3, block, me ^ 1).start()

    def rows_ready():
        for index in range(line):
            for y in range(2):
                row_wait(4 * index + 2 * y + (lax.rem(me, 2) ^ 1))

    for m in range(2):
        wt[m, :, lanes_of(me)] = stage[m, me]

    tile = 256
    tiles = total_f // tile
    chunk = 512
    chunks = tokens // chunk
    blocks = chunk // row_count

    def accumulate(r, first):
        base = pl.multiple_of(((me ^ r) // 2) * (2 * depth), 2 * depth)

        def add_product(m):
            @pl.loop(0, chunks)
            def _(c):
                x = rows[pl.ds(c * blocks, blocks), :, pl.ds(base, 2 * depth)].reshape(chunk, 2 * depth)
                weight = wt[m, :, pl.ds(base, 2 * depth)]
                product = lax.dot_general(x, weight, by_last, preferred_element_type=jnp.float32)
                at = pl.ds(pl.multiple_of(c * chunk, chunk), chunk)
                if first:
                    acc[m, at, :] = product
                else:
                    acc[m, at, :] = acc[m, at, :] + product

        add_product(group)
        for q in (r, r ^ 1):
            for piece in range(pieces if q >= NEAR else 0):
                onward(q, piece).wait_recv()
        add_product(other_group)

    def attend_here():
        for copy in small[4:9]:
            copy.wait()
        seq_count = queries.shape[0]
        group_size = HEADS // KV_HEADS
        shape = (group_size * seq_count, 1)
        seq = jnp.bitwise_and(lax.broadcasted_iota(jnp.int32, shape, 0), seq_count - 1)
        lengths = jnp.zeros(shape, jnp.int32)
        for s in range(seq_count):
            lengths = jnp.where(seq == s, lengths_ref[s], lengths)
        span = seq_count * CTX
        position = lax.broadcasted_iota(jnp.int32, (shape[0], span), 1) - seq * CTX
        visible = jnp.logical_and(position >= 0, position < lengths)
        score_scale = 1.0 / math.sqrt(HEAD_DIM)

        def columns_of(index):
            return slice(index * HEAD_DIM, (index + 1) * HEAD_DIM)

        for g in range(KV_HEADS):
            mine = [queries[:, columns_of(g * group_size + h)].astype(jnp.float32) for h in range(group_size)]
            asked = jnp.concatenate(mine, axis=0)
            key = keys[:, :, columns_of(g)].reshape(span, HEAD_DIM)
            value = cached[:, :, columns_of(g)].reshape(span, HEAD_DIM)
            fresh_key = jnp.concatenate([new_key[:, columns_of(g)].astype(jnp.float32)] * group_size, axis=0)
            fresh_value = jnp.concatenate([new_value[:, columns_of(g)].astype(jnp.float32)] * group_size, axis=0)
            scores = score_scale * lax.dot_general(
                asked.astype(jnp.bfloat16), key, by_last, preferred_element_type=jnp.float32
            )
            scores = jnp.where(visible, scores, -1e30)
            own_score = jnp.sum(asked * fresh_key, axis=-1, keepdims=True) * score_scale
            largest = jnp.maximum(jnp.max(scores, axis=-1, keepdims=True), own_score)
            cached_exp = jnp.exp(scores - largest)
            own_exp = jnp.exp(own_score - largest)
            prob_total = jnp.sum(cached_exp, axis=-1, keepdims=True) + own_exp
            cached_prob = (cached_exp / prob_total).astype(jnp.bfloat16)
            own_prob = (own_exp / prob_total).astype(jnp.bfloat16).astype(jnp.float32)
            context = jnp.dot(cached_prob, value, preferred_element_type=jnp.float32) + own_prob * fresh_value
            for h in range(group_size):
                attended_ref[:, columns_of(g * group_size + h)] = context[
                    h * seq_count : (h + 1) * seq_count, :
                ].astype(attended_ref.dtype)

    row_at = [ROW_FIRST + ROW_SPACING * step for step in range(line - 1)]
    side_at = row_at[-1] + SIDE_AFTER
    compute_from = side_at + SIDE_AFTER

    for r in range(1, NEAR):
        for m in range(2):
            near_copy(m, r).start()

    complete = []

    def advance(i):
        r, piece = items[i]
        far_copy(r, piece).wait_recv()
        onward(r, piece).start()
        if all((r ^ 1, q) in items[:i] for q in range(pieces)) and piece == pieces - 1:
            complete.append((i, r))

    def rows_and_near():
        rows_ready()
        for r in range(1, NEAR):
            for m in range(2):
                near_copy(m, r).wait_recv()
        accumulate(0, True)
        for r in range(2, NEAR, 2):
            accumulate(r, False)

    def compute(i):
        while complete and complete[0][0] + LAG <= i:
            accumulate(complete.pop(0)[1], False)

    for i, item in enumerate(items):
        if i in row_at:
            line_step(row_at.index(i))
        if i == side_at:
            side_step()
        if i >= FIRST:
            far_copy(*item).start()
        if i == 0:
            attend_here()
        if i == compute_from:
            rows_and_near()
        if i >= FUSED_AHEAD:
            advance(i - FUSED_AHEAD)
        if i > compute_from:
            compute(i - FUSED_AHEAD)
    for i in range(len(items) - FUSED_AHEAD, len(items)):
        advance(i)
        compute(i)
    compute(len(items) + LAG)

    spread_at = lax.broadcasted_iota(jnp.int32, (128, total_f), 0)
    column = lax.broadcasted_iota(jnp.int32, (128, total_f), 1)
    expert = jnp.where(spread_at < count, spread_at, spread_at - count)
    inside = jnp.logical_and(column >= expert * share, column < expert * share + share)
    spread = jnp.where(jnp.logical_and(inside, spread_at < 2 * count), 1.0, 0.0).astype(jnp.bfloat16)

    place_in_layer = lax.rem(me, 4)
    side, core = place_in_layer // 2, lax.rem(place_in_layer, 2)
    first, second = pl.ds(0, first_columns), pl.ds(first_columns, width - first_columns)
    small[9].wait()
    table = []
    for own in range(line):
        seen = []
        for d in range(line - 1, 0, -1):
            seen += [own + d] * (own + d < line) + [own - d] * (own - d >= 0)
        table.append(seen + [own])

    def turn(j):
        at = jnp.int32(0)
        for own in range(line):
            at = at + (layer == own).astype(jnp.int32) * table[own][j]
        return at

    def make_part(at):
        @pl.loop(0, 4)
        def _(b):
            block = at * 4 + b
            mix = jnp.dot(rows[block, :, width:], spread, preferred_element_type=jnp.float32)
            here = pl.ds(pl.multiple_of(block * row_count, row_count), row_count)
            there = pl.ds(pl.multiple_of(b * row_count, row_count), row_count)
            for n in range(tiles):
                columns = slice(n * tile, (n + 1) * tile)
                gate_proj = acc[0, here, columns]
                up_proj = acc[1, here, columns]
                hidden = gate_proj / (1.0 + jnp.exp(-gate_proj)) * up_proj * mix[:, columns]
                units[there, columns] = hidden.astype(units.dtype)

        wide = 2 * tile

        @pl.loop(0, width // wide)
        def _(n):
            columns = pl.ds(pl.multiple_of(n * wide, wide), wide)
            product = jnp.dot(units[...], down[:, columns], preferred_element_type=jnp.float32)
            part[pl.ds(at * 4, 4), :, columns] = product.astype(part.dtype).reshape(4, row_count, wide)

    def add(target, *sources):
        @pl.loop(0, row_count // 16)
        def _(step):
            here = pl.ds(pl.multiple_of(step * 16, 16), 16)
            total = sources[0][here, :].astype(jnp.float32)
            for source in sources[1:]:
                total = total + source[here, :].astype(jnp.float32)
            target[here, :] = total.astype(target.dtype)

    def core_copy(at, y):
        slot = at * 2 + y
        return remote(
            part.at[at * 4 + y * 2 + (core ^ 1)], core_in.at[slot], core_send.at[slot], core_recv.at[slot], (group, me ^ 1)
        )

    def line_copy(kind, at):
        src, dst, target = (
            (side_out, side_in, me ^ 2),
            (early_up_out, early_up_in, me + 4),
            (early_down_out, early_down_in, me - 4),
            (late_up_out, late_up_in, me + 4),
            (late_down_out, late_down_in, me - 4),
        )[kind]
        return remote(src.at[at], dst.at[at], line_send.at[kind, at], line_recv.at[kind, at], (group, target))

    def last_copy():
        return remote(last_out, last_in, last_send.at[0], last_recv.at[0], (group, me ^ 2))

    def held(at, y, columns):
        return part.at[at * 4 + y * 2 + core, :, columns], core_in.at[at * 2 + y, :, columns]

    def to_side(at):
        for y in range(2):
            core_copy(at, y).wait_recv()
        add(side_out.at[at], *held(at, side ^ 1, first))
        line_copy(0, at).start()

    def step_along(at, kinds, sources, starting, passing):
        for kind, has_source, moving in ((kinds[0], has_down, at > layer), (kinds[1], has_up, at < layer)):
            def pass_sum():
                line_copy(kind, at).wait_recv()
                sources(kind, True)
                line_copy(kind, at).start()

            def start_sum():
                sources(kind, False)
                line_copy(kind, at).start()

            if passing:
                pl.when(jnp.logical_and(moving, has_source))(pass_sum)
            if starting:
                pl.when(jnp.logical_and(moving, jnp.logical_not(has_source)))(start_sum)

    def early(at, starting):
        def sources(kind, arriving):
            out, arrived = ((early_up_out, early_up_in), (early_down_out, early_down_in))[kind - 1]
            for y in range(2):
                more = (arrived.at[at, y],) if arriving else ()
                add(out.at[at, y], *held(at, y, second), *more)

        step_along(at, (1, 2), sources, starting, not starting)

    def late(at):
        line_copy(0, at).wait_recv()

        def sources(kind, arriving):
            out, arrived = ((late_up_out, late_up_in), (late_down_out, late_down_in))[kind - 3]
            more = (arrived.at[at],) if arriving else ()
            add(out.at[at], *held(at, side, first), side_in.at[at], *more)

        step_along(at, (3, 4), sources, True, True)

    def arrived_from(kinds, act):
        @pl.when(has_down)
        def _():
            line_copy(kinds[0], layer).wait_recv()

        @pl.when(has_up)
        def _():
            line_copy(kinds[1], layer).wait_recv()

        for down_too, up_too in ((True, True), (True, False), (False, True)):
            matches = jnp.logical_and(has_down == down_too, has_up == up_too)
            pl.when(matches)(functools.partial(act, down_too, up_too))

    for j in range(line):
        at = turn(j)
        make_part(at)
        core_copy(at, side ^ 1).start()
        core_copy(at, side).start()
        if j:
            to_side(turn(j - 1))
            early(turn(j - 1), True)
    to_side(turn(line - 1))
    for j in range(line - 1):
        early(turn(j), False)
    for j in range(line - 1):
        late(turn(j))
    line_copy(0, layer).wait_recv()

    def sum_early(down_too, up_too):
        for y, target in ((side ^ 1, last_out), (side, out_ref.at[:, second])):
            more = [ref.at[layer, y] for ref, on in ((early_up_in, down_too), (early_down_in, up_too)) if on]
            add(target, *held(layer, y, second), *more)

    def sum_late(down_too, up_too):
        more = [ref.at[layer] for ref, on in ((late_up_in, down_too), (late_down_in, up_too)) if on]
        add(out_ref.at[:, first], *held(layer, side, first), side_in.at[layer], *more)

    arrived_from((1, 2), sum_early)
    last_copy().start()
    arrived_from((3, 4), sum_late)
    last_copy().wait_recv()
    add(out_ref.at[:, second], out_ref.at[:, second], last_in)

    last_copy().wait_send()
    for at in range(line):
        for y in range(2):
            core_copy(at, y).wait_send()
        line_copy(0, at).wait_send()
        for up_kind in (1, 3):
            pl.when(at > layer)(line_copy(up_kind, at).wait_send)
            pl.when(at < layer)(line_copy(up_kind + 1, at).wait_send)
    for r in range(1, NEAR):
        for m in range(2):
            near_copy(m, r).wait_send()
    for item in items:
        far_copy(*item).wait_send()
        onward(*item).wait_send()
    for index in range(line):
        block = lax.rem(me, 4) + 4 * index

        @pl.when(jnp.logical_and(has_up, index <= layer))
        def _():
            row_copy(0, block, me ^ 1).wait_send()

        @pl.when(jnp.logical_and(has_down, index >= layer))
        def _():
            row_copy(1, block, me ^ 1).wait_send()

        row_copy(2, block, me ^ 1).wait_send()
        row_copy(3, block, me ^ 1).wait_send()
        row_copy(3, block ^ 2, me ^ 1).wait_send()


def fused(
    queries, key_cache, value_cache, new_key, new_value, cache_lengths,
    hidden_in, norm_gain, router_weight, expert_ids, gate_train, up_train, down_train,
):
    count, depth, total_f = gate_train.shape
    row_count, width = hidden_in.shape
    line = count // 4
    first_columns = width * 13 // (16 * 128) * 128
    second_columns = width - first_columns
    anywhere = pl.BlockSpec(memory_space=pl.ANY)
    near = pl.BlockSpec(memory_space=pltpu.VMEM)
    DMA = pltpu.SemaphoreType.DMA
    like = lambda x: pltpu.VMEM(x.shape, x.dtype)
    held = lambda *shape: pltpu.VMEM(shape, jnp.bfloat16)
    router_turned, ids_turned = router_weight.T, expert_ids.T
    down_rows = down_train.reshape(-1, width)
    return pl.pallas_call(
        functools.partial(fused_kernel, count, first_columns),
        out_shape=[
            pltpu.VMEM(queries.shape, jnp.bfloat16),
            pltpu.VMEM((row_count, width), jnp.bfloat16),
        ],
        in_specs=[pl.BlockSpec(memory_space=pltpu.SMEM)] + [anywhere] * 12,
        out_specs=[near, near],
        scratch_shapes=[
            like(queries), like(key_cache), like(value_cache), like(new_key), like(new_value),
            like(hidden_in), like(norm_gain), like(router_turned), like(ids_turned), like(down_rows),
            held(2, count, depth, total_f),
            held(2, count, total_f, depth),
            held(2, total_f, count * depth),
            held(count, row_count, width + 128),
            pltpu.VMEM((2, count * row_count, total_f), jnp.float32),
            held(4 * row_count, total_f),
            held(count, row_count, width),
            held(2 * line, row_count, width),
            held(line, row_count, first_columns), held(line, row_count, first_columns),
            *[held(line, 2, row_count, second_columns)] * 4,
            *[held(line, row_count, first_columns)] * 4,
            held(row_count, second_columns), held(row_count, second_columns),
            DMA((10,)), DMA((2, count)), *[DMA((max(2, PIECES), count))] * 2, *[DMA((PIECES, count))] * 2,
            DMA((4, count)), DMA((count,)),
            DMA((2 * line,)), DMA((2 * line,)), DMA((5, line)), DMA((5, line)), DMA((1,)), DMA((1,)),
        ],
        compiler_params=pltpu.CompilerParams(collective_id=2, has_side_effects=True, vmem_limit_bytes=63 * 2**20),
    )(
        cache_lengths, queries, key_cache, value_cache, new_key, new_value,
        hidden_in, norm_gain, router_turned, ids_turned, gate_train, up_train, down_rows,
    )


def local(
    queries,
    key_cache,
    value_cache,
    new_key,
    new_value,
    cache_lengths,
    hidden_in,
    norm_gain,
    router_weight,
    expert_ids,
    gate_train,
    up_train,
    down_train,
):
    width = hidden_in.shape[1]
    expert_count = router_weight.shape[1]
    groups = lax.axis_size("groups")
    if dims_fit(groups, expert_count, gate_train, down_train, hidden_in.shape[0]) and queries.shape[0] == 8:
        return tuple(fused(
            queries, key_cache, value_cache, new_key, new_value, cache_lengths,
            hidden_in, norm_gain, router_weight, expert_ids, gate_train, up_train, down_train,
        ))
    normed = rms_normed(hidden_in, norm_gain)
    mixing = dense_mixing(normed, router_weight, expert_ids)
    mixing_high = mixing.astype(jnp.bfloat16)
    mixing_low = (mixing - mixing_high.astype(jnp.float32)).astype(jnp.bfloat16)
    spare = -2 * expert_count % 128
    row_block = jnp.concatenate(
        [normed, mixing_high, mixing_low, jnp.zeros((normed.shape[0], spare), jnp.bfloat16)], axis=1
    )
    hidden_units, down_moved = move(groups, gate_train, up_train, down_train, row_block)
    down_moved = down_moved.reshape(-1, width)
    attended = attend(queries, key_cache, value_cache, new_key, new_value, cache_lengths)
    partial_out = jnp.dot(hidden_units, down_moved, preferred_element_type=jnp.float32).astype(jnp.bfloat16)
    mixed_out = summed(partial_out, expert_count)
    return (attended, mixed_out)


def solution(mesh):
    placed = (
        P(("groups", "expert"), None),
        P(("groups", "expert"), None, None),
        P(("groups", "expert"), None, None),
        P(("groups", "expert"), None),
        P(("groups", "expert"), None),
        P(("groups", "expert")),
        P(("groups", "expert"), None),
        P(),
        P(),
        P(("groups", "expert"), None),
        P(None, "expert", None),
        P(None, "expert", None),
        P(None, "expert", None),
    )
    return jax.shard_map(
        local,
        mesh=mesh,
        in_specs=placed,
        out_specs=(P(("groups", "expert"), None), P(("groups", "expert"), None)),
        check_vma=False,
    )
```

```python
import functools
import math

import jax
import jax.numpy as jnp
from jax import lax
from jax.experimental import pallas as pl
from jax.experimental.pallas import tpu as pltpu
from jax.sharding import PartitionSpec as P

HEADS = 32
KV_HEADS = 4
HEAD_DIM = 128
CTX = 64


EPSILON = 1e-06


def rms_normed(hidden_in, norm_gain):
    values = hidden_in.astype(jnp.float32)
    mean_square = jnp.mean(values * values, axis=-1, keepdims=True)
    return (values * lax.rsqrt(mean_square + EPSILON) * norm_gain.astype(jnp.float32)).astype(
        jnp.bfloat16
    )


def attend(queries, key_cache, value_cache, new_key, new_value, cache_lengths):
    seq_count = queries.shape[0]
    group_size = HEADS // KV_HEADS
    query_blocks = queries.reshape(seq_count, KV_HEADS, group_size, HEAD_DIM)
    cached_keys = key_cache.reshape(seq_count, CTX, KV_HEADS, HEAD_DIM)
    cached_values = value_cache.reshape(seq_count, CTX, KV_HEADS, HEAD_DIM)
    fresh_keys = new_key.reshape(seq_count, KV_HEADS, HEAD_DIM)
    fresh_values = new_value.astype(jnp.float32).reshape(seq_count, KV_HEADS, HEAD_DIM)
    score_scale = 1.0 / math.sqrt(HEAD_DIM)
    scores = (
        jnp.einsum("sgrd,scgd->sgrc", query_blocks, cached_keys, preferred_element_type=jnp.float32)
        * score_scale
    )
    own_score = (
        jnp.einsum("sgrd,sgd->sgr", query_blocks, fresh_keys, preferred_element_type=jnp.float32)
        * score_scale
    )
    positions = jnp.arange(CTX, dtype=jnp.int32)
    visible = positions[None, :] < cache_lengths[:, None]
    scores = jnp.where(visible[:, None, None, :], scores, -1e30)
    largest = jnp.maximum(jnp.max(scores, axis=-1), own_score)
    cached_exp = jnp.exp(scores - largest[..., None])
    own_exp = jnp.exp(own_score - largest)
    prob_total = jnp.sum(cached_exp, axis=-1) + own_exp
    cached_prob = (cached_exp / prob_total[..., None]).astype(jnp.bfloat16)
    own_prob = (own_exp / prob_total).astype(jnp.bfloat16).astype(jnp.float32)
    context = jnp.einsum(
        "sgrc,scgd->sgrd", cached_prob, cached_values, preferred_element_type=jnp.float32
    )
    context = context + own_prob[..., None] * fresh_values[:, :, None, :]
    return context.reshape(seq_count, HEADS * HEAD_DIM).astype(jnp.bfloat16)


def dense_mixing(normed, router_weight, expert_ids):
    logits = jnp.dot(normed, router_weight, preferred_element_type=jnp.float32)
    expert_range = jnp.arange(router_weight.shape[1], dtype=jnp.int32)
    picked = jnp.any(expert_ids[:, :, None] == expert_range[None, None, :], axis=1)
    masked = jnp.where(picked, logits, -jnp.inf)
    raised = jnp.exp(masked - jnp.max(masked, axis=-1, keepdims=True))
    return raised / jnp.sum(raised, axis=-1, keepdims=True)


MESH = pl.DeviceIdType.MESH
AHEAD = 4
NEAR = 4
LAG = 2
FUSED_AHEAD = 4
ROW_FIRST = 2
ROW_SPACING = 4
SIDE_AFTER = 2
PIECES = 2
FIRST = 2


def greet(targets):
    barrier = pltpu.get_barrier_semaphore()

    expected = 0
    for condition, target in targets:
        signal = functools.partial(
            pl.semaphore_signal, barrier, inc=1, device_id=target, device_id_type=MESH
        )
        if condition is None:
            signal()
            expected = expected + 1
        else:
            pl.when(condition)(signal)
            expected = expected + condition.astype(jnp.int32)
    pl.semaphore_wait(barrier, expected)


def move_kernel(
    groups, count,
    gate_ref, up_ref, down_ref, rows_ref,
    hidden_ref, down_out, gate_out, up_out, rows_out,
    send_w, recv_w, send_x, recv_x, local_sem, send_rows, recv_rows,
):
    me = lax.axis_index("expert")
    group = lax.axis_index("groups")
    parts = max(1, groups // 2)
    part_rows = gate_ref.shape[1] // parts
    part_columns = down_ref.shape[2] // groups
    line = count // 4
    layer = me // 4

    others = [(None, (group, me ^ r)) for r in range(1, count)]
    others += [(None, (lax.rem(group + h, groups), me)) for h in range(1, groups)]
    greet(others)

    def remote(src, dst, send, recv, target):
        return pltpu.make_async_remote_copy(
            src_ref=src, dst_ref=dst, send_sem=send, recv_sem=recv, device_id=target, device_id_type=MESH
        )

    def rows_of(owner):
        return pl.ds(pl.multiple_of((owner // 2) * part_rows, part_rows), part_rows)

    def columns_of(owner):
        return pl.ds(pl.multiple_of(owner * part_columns, part_columns), part_columns)

    def row_copy(kind, block, target, own=False):
        source = rows_ref if own else rows_out.at[block]
        return remote(
            source, rows_out.at[block], send_rows.at[kind, block], recv_rows.at[block], (group, target)
        )

    def row_wait(block):
        row_copy(0, block, me ^ 1).wait_recv()

    own_rows = pltpu.make_async_copy(rows_ref, rows_out.at[me], local_sem.at[3])
    own_rows.start()
    has_up, has_down = me + 4 < count, me >= 4

    @pl.when(has_up)
    def _():
        row_copy(0, me, me + 4, True).start()

    @pl.when(has_down)
    def _():
        row_copy(1, me, me - 4, True).start()

    row_copy(2, me, me ^ 2, True).start()
    row_copy(3, me, me ^ 1, True).start()

    def line_step(step):
        below, above = me - 4 * (step + 1), me + 4 * (step + 1)

        @pl.when(below >= 0)
        def _():
            row_wait(below)

            @pl.when(has_up)
            def _():
                row_copy(0, below, me + 4).start()

            row_copy(2, below, me ^ 2).start()
            row_copy(3, below, me ^ 1).start()

        @pl.when(above < count)
        def _():
            row_wait(above)

            @pl.when(has_down)
            def _():
                row_copy(1, above, me - 4).start()

            row_copy(2, above, me ^ 2).start()
            row_copy(3, above, me ^ 1).start()

    def side_step(index):
        block = lax.rem(me, 4) ^ 2
        block = block + 4 * index
        row_wait(block)
        row_copy(3, block, me ^ 1).start()

    def across(kind, r, refs_in, refs_out, which):
        target = me ^ r
        if r < NEAR:
            a, b = ((gate_ref, gate_out), (down_ref, down_out), (up_ref, up_out))[kind]
            send = send_x.at[0, r, 0] if kind == 2 else send_w.at[kind, r]
            recv = recv_x.at[0, r, 0] if kind == 2 else recv_w.at[kind, r]
            return remote(a.at[target], b.at[me], send, recv, (group, target))
        if kind == 0:
            return remote(
                refs_in[which].at[target, rows_of(group)], refs_out[which].at[me, rows_of(group)],
                send_w.at[0, r], recv_w.at[0, r], (group, target),
            )
        return remote(
            down_ref.at[target, :, columns_of(group)], down_out.at[me, :, columns_of(group)],
            send_w.at[1, r], recv_w.at[1, r], (group, target),
        )

    ins, outs = (gate_ref, up_ref), (gate_out, up_out)

    def by_matrix(act):
        pl.when(lax.rem(group, 2) == 0)(functools.partial(act, 0))
        pl.when(lax.rem(group, 2) == 1)(functools.partial(act, 1))

    def start_weight(kind, r):
        if kind == 0 and r >= NEAR:
            by_matrix(lambda which: across(0, r, ins, outs, which).start())
        else:
            across(kind, r, ins, outs, 0).start()

    def onward(kind, r, h, which):
        held = me ^ r
        place = outs[which].at[held, rows_of(group)] if kind == 0 else down_out.at[held, :, columns_of(group)]
        return remote(
            place, place, send_x.at[kind, r, h - 1], recv_x.at[kind, r, h - 1],
            (lax.rem(group + h, groups), me),
        )

    def pass_on(kind, r):
        across(kind, r, ins, outs, 0).wait_recv()
        for h in range(1, groups if r >= NEAR else 1):
            if kind == 0:
                by_matrix(lambda which: onward(0, r, h, which).start())
            else:
                onward(1, r, h, 0).start()

    own_copies = [
        pltpu.make_async_copy(a.at[me], b.at[me], local_sem.at[i])
        for i, (a, b) in enumerate(((gate_ref, gate_out), (up_ref, up_out), (down_ref, down_out)))
    ]
    width = gate_ref.shape[1] * count

    def ready():
        for index in range(line):
            for y in range(2):
                row_wait(4 * index + 2 * y + (lax.rem(me, 2) ^ 1))
        own_rows.wait()
        for copy in own_copies[:2]:
            copy.wait()
        for r in order:
            for h in range(1, groups if r >= NEAR else 1):
                onward(0, r, h, 0).wait_recv()

    def expert_rows(quarter):
        @pl.loop(0, count // 16)
        def _(step):
            at = quarter * (count // 4) + step * 4
            rows = rows_out[pl.ds(at, 4)].reshape(-1, rows_out.shape[2])
            tokens = rows[:, :width]
            shares = rows[:, width:].astype(jnp.float32)
            lane = lax.broadcasted_iota(jnp.int32, shares.shape, 1)
            own = jnp.logical_or(lane == me, lane == me + count)
            own_mix = jnp.sum(jnp.where(own, shares, 0.0), axis=1, keepdims=True)
            gate = gate_out[...].reshape(width, -1)
            gate_proj = jnp.dot(tokens, gate, preferred_element_type=jnp.float32)
            up = up_out[...].reshape(width, -1)
            up_proj = jnp.dot(tokens, up, preferred_element_type=jnp.float32)
            hidden = gate_proj / (1.0 + jnp.exp(-gate_proj)) * up_proj * own_mix
            place = pl.ds(pl.multiple_of(at * rows_out.shape[1], rows.shape[0]), rows.shape[0])
            hidden_ref[place, :] = hidden.astype(hidden_ref.dtype)

    half = count // 2
    order = [r for i in range(half) for r in ((half + i, i) if i else (half,))]
    first = [(kind, r) for r in order for kind in ((0, 2) if r < NEAR else (0,))]
    items = first + [(1, r) for r in order]
    spacing = len(items) // (line + 1)
    side_at = 2 + spacing * (line - 1) + 3

    def advance(i):
        pass_on(*items[i])
        before_last = len(items) - 1 - i
        if before_last % 2 == 0 and before_last < 8:
            if before_last == 6:
                ready()
            expert_rows(3 - before_last // 2)

    for i, item in enumerate(items):
        start_weight(*item)
        if i >= 2 and (i - 2) % spacing == 0 and (i - 2) // spacing < line - 1:
            line_step((i - 2) // spacing)
        if i == side_at:
            for index in range(line):
                side_step(index)
        if i == AHEAD:
            for copy in own_copies:
                copy.start()
        if i >= AHEAD:
            advance(i - AHEAD)
    for i in range(len(items) - AHEAD, len(items)):
        advance(i)

    own_copies[2].wait()
    for kind, r in items:
        across(kind, r, ins, outs, 0).wait_send()
        for h in range(1, groups if r >= NEAR else 1):
            onward(kind, r, h, 0).wait_send()
            if kind == 1:
                onward(kind, r, h, 0).wait_recv()
    for index in range(line):
        block = lax.rem(me, 4) + 4 * index

        @pl.when(jnp.logical_and(has_up, index <= layer))
        def _():
            row_copy(0, block, me ^ 1).wait_send()

        @pl.when(jnp.logical_and(has_down, index >= layer))
        def _():
            row_copy(1, block, me ^ 1).wait_send()

        row_copy(2, block, me ^ 1).wait_send()
        row_copy(3, block, me ^ 1).wait_send()
        row_copy(3, block ^ 2, me ^ 1).wait_send()


def move(groups, gate_train, up_train, down_train, row_block):
    count = gate_train.shape[0]
    anywhere = pl.BlockSpec(memory_space=pl.ANY)
    DMA = pltpu.SemaphoreType.DMA
    return pl.pallas_call(
        functools.partial(move_kernel, groups, count),
        out_shape=[
            jax.ShapeDtypeStruct((count * row_block.shape[0], gate_train.shape[2]), jnp.bfloat16),
            jax.ShapeDtypeStruct(down_train.shape, down_train.dtype),
        ],
        in_specs=[anywhere, anywhere, anywhere, pl.BlockSpec(memory_space=pltpu.VMEM)],
        out_specs=[pl.BlockSpec(memory_space=pltpu.VMEM), anywhere],
        scratch_shapes=[
            pltpu.VMEM(gate_train.shape, gate_train.dtype),
            pltpu.VMEM(up_train.shape, up_train.dtype),
            pltpu.VMEM((count,) + row_block.shape, row_block.dtype),
            DMA((2, count)), DMA((2, count)),
            DMA((2, count, max(1, groups - 1))), DMA((2, count, max(1, groups - 1))),
            DMA((4,)), DMA((4, count)), DMA((count,)),
        ],
        compiler_params=pltpu.CompilerParams(collective_id=0, has_side_effects=True, vmem_limit_bytes=60 * 2**20),
    )(gate_train, up_train, down_train, row_block)


def sum_kernel(
    count, part_ref, out_ref, core_in, side_in, up_in, down_in, side_out, up_out, down_out,
    core_send, core_recv, side_send, side_recv, up_send, up_recv, down_send, down_recv,
):
    me = lax.axis_index("expert")
    group = lax.axis_index("groups")
    line, layer = count // 4, me // 4
    place = lax.rem(me, 4)
    side, core = place // 2, lax.rem(place, 2)
    has_up, has_down = me + 4 < count, me >= 4
    greet([
        (None, (group, me ^ 1)), (None, (group, me ^ 2)),
        (has_up, (group, me + 4)), (has_down, (group, me - 4)),
    ])
    chunk = 16
    row_count = part_ref.shape[1]

    def remote(src, dst, send, recv, target):
        return pltpu.make_async_remote_copy(
            src_ref=src, dst_ref=dst, send_sem=send, recv_sem=recv, device_id=(group, target), device_id_type=MESH
        )

    def add(target, *sources):
        @pl.loop(0, row_count // chunk)
        def _(step):
            rows = pl.ds(pl.multiple_of(step * chunk, chunk), chunk)
            total = sources[0][rows, :].astype(jnp.float32)
            for source in sources[1:]:
                total = total + source[rows, :].astype(jnp.float32)
            target[rows, :] = total.astype(target.dtype)

    def core_copy(at, y):
        slot = at * 2 + y
        return remote(
            part_ref.at[at * 4 + y * 2 + (core ^ 1)], core_in.at[slot], core_send.at[slot], core_recv.at[slot], me ^ 1
        )

    def side_copy(at):
        return remote(side_out.at[at], side_in.at[at], side_send.at[at], side_recv.at[at], me ^ 2)

    def up_copy(at):
        return remote(up_out.at[at], up_in.at[at], up_send.at[at], up_recv.at[at], me + 4)

    def down_copy(at):
        return remote(down_out.at[at], down_in.at[at], down_send.at[at], down_recv.at[at], me - 4)

    def in_order(act):
        for d in range(line - 1, 0, -1):
            pl.when(layer + d < line)(functools.partial(act, layer + d, 1))
            pl.when(layer - d >= 0)(functools.partial(act, layer - d, -1))
        act(layer, 0)

    in_order(lambda at, way: core_copy(at, side ^ 1).start())
    in_order(lambda at, way: core_copy(at, side).start())

    def to_side(at, way):
        core_copy(at, side ^ 1).wait_recv()
        add(side_out.at[at], part_ref.at[at * 4 + (side ^ 1) * 2 + core], core_in.at[at * 2 + (side ^ 1)])
        side_copy(at).start()

    in_order(to_side)

    def along(at, way):
        core_copy(at, side).wait_recv()
        side_copy(at).wait_recv()
        mine = (part_ref.at[at * 4 + place], core_in.at[at * 2 + side], side_in.at[at])
        if way == 1:
            @pl.when(has_down)
            def _():
                up_copy(at).wait_recv()
                add(up_out.at[at], *mine, up_in.at[at])

            @pl.when(jnp.logical_not(has_down))
            def _():
                add(up_out.at[at], *mine)

            up_copy(at).start()
        elif way == -1:
            @pl.when(has_up)
            def _():
                down_copy(at).wait_recv()
                add(down_out.at[at], *mine, down_in.at[at])

            @pl.when(jnp.logical_not(has_up))
            def _():
                add(down_out.at[at], *mine)

            down_copy(at).start()
        else:
            @pl.when(has_down)
            def _():
                up_copy(at).wait_recv()

            @pl.when(has_up)
            def _():
                down_copy(at).wait_recv()

            both = jnp.logical_and(has_down, has_up)

            @pl.when(both)
            def _():
                add(out_ref, *mine, up_in.at[at], down_in.at[at])

            @pl.when(jnp.logical_and(has_down, jnp.logical_not(has_up)))
            def _():
                add(out_ref, *mine, up_in.at[at])

            @pl.when(jnp.logical_and(has_up, jnp.logical_not(has_down)))
            def _():
                add(out_ref, *mine, down_in.at[at])

            @pl.when(jnp.logical_not(jnp.logical_or(has_up, has_down)))
            def _():
                add(out_ref, *mine)

    in_order(along)

    def finish(at, way):
        core_copy(at, side ^ 1).wait_send()
        core_copy(at, side).wait_send()
        side_copy(at).wait_send()
        if way == 1:
            up_copy(at).wait_send()
        if way == -1:
            down_copy(at).wait_send()

    in_order(finish)


def summed(partial_out, count):
    rows, width = partial_out.shape[0] // count, partial_out.shape[1]
    line = count // 4
    DMA = pltpu.SemaphoreType.DMA
    block = lambda amount: pltpu.VMEM((amount, rows, width), jnp.bfloat16)
    return pl.pallas_call(
        functools.partial(sum_kernel, count),
        out_shape=jax.ShapeDtypeStruct((rows, width), jnp.bfloat16),
        in_specs=[pl.BlockSpec(memory_space=pltpu.VMEM)],
        out_specs=pl.BlockSpec(memory_space=pltpu.VMEM),
        scratch_shapes=[block(count // 2)] + [block(line)] * 6
        + [DMA((count // 2,)), DMA((count // 2,))] + [DMA((line,))] * 6,
        compiler_params=pltpu.CompilerParams(collective_id=1, has_side_effects=True, vmem_limit_bytes=60 * 2**20),
    )(partial_out.reshape(count, rows, width))


def dims_fit(groups, count, gate_train, down_train, row_count):
    rows, width = gate_train.shape[1], gate_train.shape[2]
    part = down_train.shape[1]
    return (
        groups == 2
        and count % 8 == 0
        and 2 * count <= 128
        and rows % 128 == 0
        and part % 16 == 0
        and part * count == width
        and width % 256 == 0
        and row_count % 16 == 0
        and (count * row_count) % 512 == 0
    )


def fused_kernel(
    count, first_columns, lengths_ref, queries_ref, keys_ref, values_ref, new_key_ref, new_value_ref,
    hidden_in_ref, gain_in_ref, router_in_ref, ids_in_ref, gate_ref, up_ref, down_in_ref,
    attended_ref, out_ref,
    queries, keys, cached, new_key, new_value, hid_ref, gain_ref, router_ref, ids_ref, down,
    load, stage, wt, rows, acc, units, part, core_in, side_out, side_in,
    early_up_out, early_up_in, early_down_out, early_down_in,
    late_up_out, late_up_in, late_down_out, late_down_in, last_out, last_in,
    small_sem, load_sem, send_w, recv_w, send_x, recv_x, send_rows, recv_rows,
    core_send, core_recv, line_send, line_recv, last_send, last_recv,
):
    me = lax.axis_index("expert")
    group = lax.axis_index("groups")
    other_group = 1 - group
    line = count // 4
    layer = me // 4
    row_count, width = hid_ref.shape
    depth = gate_ref.shape[1]
    share = stage.shape[2] // count
    total_f = stage.shape[2]
    tokens = count * row_count

    def loading(m, e):
        return pltpu.make_async_copy((gate_ref, up_ref)[m].at[e], load.at[m, e], load_sem.at[m, e])

    small = [
        pltpu.make_async_copy(src, dst, small_sem.at[i])
        for i, (src, dst) in enumerate((
            (hidden_in_ref, hid_ref), (gain_in_ref, gain_ref), (router_in_ref, router_ref), (ids_in_ref, ids_ref),
            (queries_ref, queries), (keys_ref, keys), (values_ref, cached), (new_key_ref, new_key),
            (new_value_ref, new_value), (down_in_ref, down),
        ))
    ]
    for copy in small[:4]:
        copy.start()
    for e in range(count):
        for m in range(2):
            loading(m, e).start()
    for copy in small[4:]:
        copy.start()

    barrier = pltpu.get_barrier_semaphore()
    peers = [(group, me ^ r) for r in range(1, count)] + [(other_group, me)]
    for peer in peers:
        pl.semaphore_signal(barrier, inc=1, device_id=peer, device_id_type=MESH)

    @pl.loop(0, count)
    def _(e):
        for m in range(2):
            loading(m, e).wait()
            turned = load[m, e].T.reshape(count, share, depth)
            stage[m, :, pl.ds(pl.multiple_of(e * share, share), share), :] = turned

    pl.semaphore_wait(barrier, len(peers))

    def remote(src, dst, send, recv, target):
        return pltpu.make_async_remote_copy(
            src_ref=src, dst_ref=dst, send_sem=send, recv_sem=recv, device_id=target, device_id_type=MESH
        )

    pieces = PIECES
    piece_rows = total_f // pieces

    def lanes_of(owner):
        return pl.ds(pl.multiple_of(owner * depth, depth), depth)

    def rows_of(piece):
        return pl.ds(piece * piece_rows, piece_rows)

    def near_copy(m, r):
        return remote(
            stage.at[m, me ^ r], wt.at[m, :, lanes_of(me)], send_w.at[m, r], recv_w.at[m, r], (group, me ^ r)
        )

    def far_copy(r, piece):
        return remote(
            stage.at[group, me ^ r, rows_of(piece)], wt.at[group, rows_of(piece), lanes_of(me)],
            send_w.at[piece, r], recv_w.at[piece, r], (group, me ^ r),
        )

    def onward(r, piece):
        ref = wt.at[group, rows_of(piece), lanes_of(me ^ r)]
        return remote(ref, ref, send_x.at[piece, r], recv_x.at[piece, r], (other_group, me))

    by_distance = [[NEAR * d + i for i in range(NEAR)] for d in range(1, line)]
    by_distance = by_distance[1:] + by_distance[:1]
    far = []
    for i in range(0, NEAR, 2):
        pairs = [group_of[i : i + 2] for group_of in by_distance]
        far += [pair[0] for pair in pairs[:-1]] + [pairs[0][1], pairs[-1][0]]
        far += [pair[1] for pair in pairs[1:]]
    items = [(r, piece) for r in far for piece in range(pieces)]
    for item in items[:FIRST]:
        far_copy(*item).start()
    for copy in small[:4]:
        copy.wait()
    values = hid_ref[...].astype(jnp.float32)
    mean_square = jnp.mean(values * values, axis=-1, keepdims=True)
    gain = gain_ref[...].astype(jnp.float32).reshape(1, width)
    normed = (values * lax.rsqrt(mean_square + EPSILON) * gain).astype(jnp.bfloat16)
    rows[me, :, :width] = normed
    by_last = (((1,), (1,)), ((), ()))
    logits = lax.dot_general(normed, router_ref[...], by_last, preferred_element_type=jnp.float32)
    ids = ids_ref[...]
    lane = lax.broadcasted_iota(jnp.int32, (count, row_count), 0)
    named = ids[0:1, :] == lane
    for k in range(1, ids.shape[0]):
        named = jnp.logical_or(named, ids[k : k + 1, :] == lane)
    named = jnp.where(named, 1.0, 0.0).astype(jnp.bfloat16)
    diagonal = lax.broadcasted_iota(jnp.int32, (row_count, row_count), 0) == lax.broadcasted_iota(
        jnp.int32, (row_count, row_count), 1
    )
    diagonal = jnp.where(diagonal, 1.0, 0.0).astype(jnp.bfloat16)
    picked = lax.dot_general(diagonal, named, by_last, preferred_element_type=jnp.float32) > 0.5
    masked = jnp.where(picked, logits, -jnp.inf)
    raised = jnp.exp(masked - jnp.max(masked, axis=-1, keepdims=True))
    mixing = raised / jnp.sum(raised, axis=-1, keepdims=True)
    high = mixing.astype(jnp.bfloat16)
    low = (mixing - high.astype(jnp.float32)).astype(jnp.bfloat16)
    source = lax.broadcasted_iota(jnp.int32, (count, 128), 0)
    place = lax.broadcasted_iota(jnp.int32, (count, 128), 1)
    at_high = jnp.where(place == source, 1.0, 0.0).astype(jnp.bfloat16)
    at_low = jnp.where(place == source + count, 1.0, 0.0).astype(jnp.bfloat16)
    shares = jnp.dot(high, at_high, preferred_element_type=jnp.float32) + jnp.dot(
        low, at_low, preferred_element_type=jnp.float32
    )
    rows[me, :, width:] = shares.astype(jnp.bfloat16)

    def row_copy(kind, block, target):
        return remote(
            rows.at[block], rows.at[block], send_rows.at[kind, block], recv_rows.at[block], (group, target)
        )

    def row_wait(block):
        row_copy(0, block, me ^ 1).wait_recv()

    has_up, has_down = me + 4 < count, me >= 4

    @pl.when(has_up)
    def _():
        row_copy(0, me, me + 4).start()

    @pl.when(has_down)
    def _():
        row_copy(1, me, me - 4).start()

    row_copy(2, me, me ^ 2).start()
    row_copy(3, me, me ^ 1).start()

    def line_step(step):
        below, above = me - 4 * (step + 1), me + 4 * (step + 1)

        @pl.when(below >= 0)
        def _():
            row_wait(below)

            @pl.when(has_up)
            def _():
                row_copy(0, below, me + 4).start()

            row_copy(2, below, me ^ 2).start()
            row_copy(3, below, me ^ 1).start()

        @pl.when(above < count)
        def _():
            row_wait(above)

            @pl.when(has_down)
            def _():
                row_copy(1, above, me - 4).start()

            row_copy(2, above, me ^ 2).start()
            row_copy(3, above, me ^ 1).start()

    def side_step():
        for index in range(line):
            block = (lax.rem(me, 4) ^ 2) + 4 * index
            row_wait(block)
            row_copy(3, block, me ^ 1).start()

    def rows_ready():
        for index in range(line):
            for y in range(2):
                row_wait(4 * index + 2 * y + (lax.rem(me, 2) ^ 1))

    for m in range(2):
        wt[m, :, lanes_of(me)] = stage[m, me]

    tile = 256
    tiles = total_f // tile
    chunk = 512
    chunks = tokens // chunk
    blocks = chunk // row_count

    def accumulate(r, first):
        base = pl.multiple_of(((me ^ r) // 2) * (2 * depth), 2 * depth)

        def add_product(m):
            @pl.loop(0, chunks)
            def _(c):
                x = rows[pl.ds(c * blocks, blocks), :, pl.ds(base, 2 * depth)].reshape(chunk, 2 * depth)
                weight = wt[m, :, pl.ds(base, 2 * depth)]
                product = lax.dot_general(x, weight, by_last, preferred_element_type=jnp.float32)
                at = pl.ds(pl.multiple_of(c * chunk, chunk), chunk)
                if first:
                    acc[m, at, :] = product
                else:
                    acc[m, at, :] = acc[m, at, :] + product

        add_product(group)
        for q in (r, r ^ 1):
            for piece in range(pieces if q >= NEAR else 0):
                onward(q, piece).wait_recv()
        add_product(other_group)

    def attend_here():
        for copy in small[4:9]:
            copy.wait()
        seq_count = queries.shape[0]
        group_size = HEADS // KV_HEADS
        shape = (group_size * seq_count, 1)
        seq = jnp.bitwise_and(lax.broadcasted_iota(jnp.int32, shape, 0), seq_count - 1)
        lengths = jnp.zeros(shape, jnp.int32)
        for s in range(seq_count):
            lengths = jnp.where(seq == s, lengths_ref[s], lengths)
        span = seq_count * CTX
        position = lax.broadcasted_iota(jnp.int32, (shape[0], span), 1) - seq * CTX
        visible = jnp.logical_and(position >= 0, position < lengths)
        score_scale = 1.0 / math.sqrt(HEAD_DIM)

        def columns_of(index):
            return slice(index * HEAD_DIM, (index + 1) * HEAD_DIM)

        for g in range(KV_HEADS):
            mine = [queries[:, columns_of(g * group_size + h)].astype(jnp.float32) for h in range(group_size)]
            asked = jnp.concatenate(mine, axis=0)
            key = keys[:, :, columns_of(g)].reshape(span, HEAD_DIM)
            value = cached[:, :, columns_of(g)].reshape(span, HEAD_DIM)
            fresh_key = jnp.concatenate([new_key[:, columns_of(g)].astype(jnp.float32)] * group_size, axis=0)
            fresh_value = jnp.concatenate([new_value[:, columns_of(g)].astype(jnp.float32)] * group_size, axis=0)
            scores = score_scale * lax.dot_general(
                asked.astype(jnp.bfloat16), key, by_last, preferred_element_type=jnp.float32
            )
            scores = jnp.where(visible, scores, -1e30)
            own_score = jnp.sum(asked * fresh_key, axis=-1, keepdims=True) * score_scale
            largest = jnp.maximum(jnp.max(scores, axis=-1, keepdims=True), own_score)
            cached_exp = jnp.exp(scores - largest)
            own_exp = jnp.exp(own_score - largest)
            prob_total = jnp.sum(cached_exp, axis=-1, keepdims=True) + own_exp
            cached_prob = (cached_exp / prob_total).astype(jnp.bfloat16)
            own_prob = (own_exp / prob_total).astype(jnp.bfloat16).astype(jnp.float32)
            context = jnp.dot(cached_prob, value, preferred_element_type=jnp.float32) + own_prob * fresh_value
            for h in range(group_size):
                attended_ref[:, columns_of(g * group_size + h)] = context[
                    h * seq_count : (h + 1) * seq_count, :
                ].astype(attended_ref.dtype)

    row_at = [ROW_FIRST + ROW_SPACING * step - step // 2 for step in range(line - 1)]
    side_at = row_at[-1] + SIDE_AFTER
    compute_from = side_at + SIDE_AFTER

    for r in range(1, NEAR):
        for m in range(2):
            near_copy(m, r).start()

    complete = []

    def advance(i):
        r, piece = items[i]
        far_copy(r, piece).wait_recv()
        onward(r, piece).start()
        if all((r ^ 1, q) in items[:i] for q in range(pieces)) and piece == pieces - 1:
            complete.append((i, r))

    def rows_and_near():
        rows_ready()
        for r in range(1, NEAR):
            for m in range(2):
                near_copy(m, r).wait_recv()
        accumulate(0, True)
        for r in range(2, NEAR, 2):
            accumulate(r, False)

    def compute(i):
        while complete and complete[0][0] + LAG <= i:
            accumulate(complete.pop(0)[1], False)

    for i, item in enumerate(items):
        if i in row_at:
            line_step(row_at.index(i))
        if i == side_at:
            side_step()
        if i >= FIRST:
            far_copy(*item).start()
        if i == 0:
            attend_here()
        if i == compute_from:
            rows_and_near()
        if i >= FUSED_AHEAD:
            advance(i - FUSED_AHEAD)
        if i > compute_from:
            compute(i - FUSED_AHEAD)
    for i in range(len(items) - FUSED_AHEAD, len(items)):
        advance(i)
        compute(i)
    compute(len(items) + LAG)

    spread_at = lax.broadcasted_iota(jnp.int32, (128, total_f), 0)
    column = lax.broadcasted_iota(jnp.int32, (128, total_f), 1)
    expert = jnp.where(spread_at < count, spread_at, spread_at - count)
    inside = jnp.logical_and(column >= expert * share, column < expert * share + share)
    spread = jnp.where(jnp.logical_and(inside, spread_at < 2 * count), 1.0, 0.0).astype(jnp.bfloat16)

    place_in_layer = lax.rem(me, 4)
    side, core = place_in_layer // 2, lax.rem(place_in_layer, 2)
    first, second = pl.ds(0, first_columns), pl.ds(first_columns, width - first_columns)
    small[9].wait()
    table = []
    for own in range(line):
        seen = []
        for d in range(line - 1, 0, -1):
            seen += [own + d] * (own + d < line) + [own - d] * (own - d >= 0)
        table.append(seen + [own])

    def turn(j):
        at = jnp.int32(0)
        for own in range(line):
            at = at + (layer == own).astype(jnp.int32) * table[own][j]
        return at

    def make_part(at):
        @pl.loop(0, 4)
        def _(b):
            block = at * 4 + b
            mix = jnp.dot(rows[block, :, width:], spread, preferred_element_type=jnp.float32)
            here = pl.ds(pl.multiple_of(block * row_count, row_count), row_count)
            there = pl.ds(pl.multiple_of(b * row_count, row_count), row_count)
            for n in range(tiles):
                columns = slice(n * tile, (n + 1) * tile)
                gate_proj = acc[0, here, columns]
                up_proj = acc[1, here, columns]
                hidden = gate_proj / (1.0 + jnp.exp(-gate_proj)) * up_proj * mix[:, columns]
                units[there, columns] = hidden.astype(units.dtype)

        wide = 2 * tile

        @pl.loop(0, width // wide)
        def _(n):
            columns = pl.ds(pl.multiple_of(n * wide, wide), wide)
            product = jnp.dot(units[...], down[:, columns], preferred_element_type=jnp.float32)
            part[pl.ds(at * 4, 4), :, columns] = product.astype(part.dtype).reshape(4, row_count, wide)

    def add(target, *sources):
        @pl.loop(0, row_count // 16)
        def _(step):
            here = pl.ds(pl.multiple_of(step * 16, 16), 16)
            total = sources[0][here, :].astype(jnp.float32)
            for source in sources[1:]:
                total = total + source[here, :].astype(jnp.float32)
            target[here, :] = total.astype(target.dtype)

    def core_copy(at, y):
        slot = at * 2 + y
        return remote(
            part.at[at * 4 + y * 2 + (core ^ 1)], core_in.at[slot], core_send.at[slot], core_recv.at[slot], (group, me ^ 1)
        )

    def line_copy(kind, at):
        src, dst, target = (
            (side_out, side_in, me ^ 2),
            (early_up_out, early_up_in, me + 4),
            (early_down_out, early_down_in, me - 4),
            (late_up_out, late_up_in, me + 4),
            (late_down_out, late_down_in, me - 4),
        )[kind]
        return remote(src.at[at], dst.at[at], line_send.at[kind, at], line_recv.at[kind, at], (group, target))

    def last_copy():
        return remote(last_out, last_in, last_send.at[0], last_recv.at[0], (group, me ^ 2))

    def held(at, y, columns):
        return part.at[at * 4 + y * 2 + core, :, columns], core_in.at[at * 2 + y, :, columns]

    def to_side(at):
        for y in range(2):
            core_copy(at, y).wait_recv()
        add(side_out.at[at], *held(at, side ^ 1, first))
        line_copy(0, at).start()

    def step_along(at, kinds, sources, starting, passing):
        for kind, has_source, moving in ((kinds[0], has_down, at > layer), (kinds[1], has_up, at < layer)):
            def pass_sum():
                line_copy(kind, at).wait_recv()
                sources(kind, True)
                line_copy(kind, at).start()

            def start_sum():
                sources(kind, False)
                line_copy(kind, at).start()

            if passing:
                pl.when(jnp.logical_and(moving, has_source))(pass_sum)
            if starting:
                pl.when(jnp.logical_and(moving, jnp.logical_not(has_source)))(start_sum)

    def early(at, starting):
        def sources(kind, arriving):
            out, arrived = ((early_up_out, early_up_in), (early_down_out, early_down_in))[kind - 1]
            for y in range(2):
                more = (arrived.at[at, y],) if arriving else ()
                add(out.at[at, y], *held(at, y, second), *more)

        step_along(at, (1, 2), sources, starting, not starting)

    def late(at):
        line_copy(0, at).wait_recv()

        def sources(kind, arriving):
            out, arrived = ((late_up_out, late_up_in), (late_down_out, late_down_in))[kind - 3]
            more = (arrived.at[at],) if arriving else ()
            add(out.at[at], *held(at, side, first), side_in.at[at], *more)

        step_along(at, (3, 4), sources, True, True)

    def arrived_from(kinds, act):
        @pl.when(has_down)
        def _():
            line_copy(kinds[0], layer).wait_recv()

        @pl.when(has_up)
        def _():
            line_copy(kinds[1], layer).wait_recv()

        for down_too, up_too in ((True, True), (True, False), (False, True)):
            matches = jnp.logical_and(has_down == down_too, has_up == up_too)
            pl.when(matches)(functools.partial(act, down_too, up_too))

    for j in range(line):
        at = turn(j)
        make_part(at)
        core_copy(at, side ^ 1).start()
        core_copy(at, side).start()
        if j:
            to_side(turn(j - 1))
            early(turn(j - 1), True)
    to_side(turn(line - 1))
    for j in range(line - 1):
        early(turn(j), False)
    for j in range(line - 1):
        late(turn(j))
    line_copy(0, layer).wait_recv()

    def sum_early(down_too, up_too):
        for y, target in ((side ^ 1, last_out), (side, out_ref.at[:, second])):
            more = [ref.at[layer, y] for ref, on in ((early_up_in, down_too), (early_down_in, up_too)) if on]
            add(target, *held(layer, y, second), *more)

    def sum_late(down_too, up_too):
        more = [ref.at[layer] for ref, on in ((late_up_in, down_too), (late_down_in, up_too)) if on]
        add(out_ref.at[:, first], *held(layer, side, first), side_in.at[layer], *more)

    arrived_from((1, 2), sum_early)
    last_copy().start()
    arrived_from((3, 4), sum_late)
    last_copy().wait_recv()
    add(out_ref.at[:, second], out_ref.at[:, second], last_in)

    last_copy().wait_send()
    for at in range(line):
        for y in range(2):
            core_copy(at, y).wait_send()
        line_copy(0, at).wait_send()
        for up_kind in (1, 3):
            pl.when(at > layer)(line_copy(up_kind, at).wait_send)
            pl.when(at < layer)(line_copy(up_kind + 1, at).wait_send)
    for r in range(1, NEAR):
        for m in range(2):
            near_copy(m, r).wait_send()
    for item in items:
        far_copy(*item).wait_send()
        onward(*item).wait_send()
    for index in range(line):
        block = lax.rem(me, 4) + 4 * index

        @pl.when(jnp.logical_and(has_up, index <= layer))
        def _():
            row_copy(0, block, me ^ 1).wait_send()

        @pl.when(jnp.logical_and(has_down, index >= layer))
        def _():
            row_copy(1, block, me ^ 1).wait_send()

        row_copy(2, block, me ^ 1).wait_send()
        row_copy(3, block, me ^ 1).wait_send()
        row_copy(3, block ^ 2, me ^ 1).wait_send()


def fused(
    queries, key_cache, value_cache, new_key, new_value, cache_lengths,
    hidden_in, norm_gain, router_weight, expert_ids, gate_train, up_train, down_train,
):
    count, depth, total_f = gate_train.shape
    row_count, width = hidden_in.shape
    line = count // 4
    first_columns = width * 13 // (16 * 128) * 128
    second_columns = width - first_columns
    anywhere = pl.BlockSpec(memory_space=pl.ANY)
    near = pl.BlockSpec(memory_space=pltpu.VMEM)
    DMA = pltpu.SemaphoreType.DMA
    like = lambda x: pltpu.VMEM(x.shape, x.dtype)
    held = lambda *shape: pltpu.VMEM(shape, jnp.bfloat16)
    router_turned, ids_turned = router_weight.T, expert_ids.T
    down_rows = down_train.reshape(-1, width)
    return pl.pallas_call(
        functools.partial(fused_kernel, count, first_columns),
        out_shape=[
            pltpu.VMEM(queries.shape, jnp.bfloat16),
            pltpu.VMEM((row_count, width), jnp.bfloat16),
        ],
        in_specs=[pl.BlockSpec(memory_space=pltpu.SMEM)] + [anywhere] * 12,
        out_specs=[near, near],
        scratch_shapes=[
            like(queries), like(key_cache), like(value_cache), like(new_key), like(new_value),
            like(hidden_in), like(norm_gain), like(router_turned), like(ids_turned), like(down_rows),
            held(2, count, depth, total_f),
            held(2, count, total_f, depth),
            held(2, total_f, count * depth),
            held(count, row_count, width + 128),
            pltpu.VMEM((2, count * row_count, total_f), jnp.float32),
            held(4 * row_count, total_f),
            held(count, row_count, width),
            held(2 * line, row_count, width),
            held(line, row_count, first_columns), held(line, row_count, first_columns),
            *[held(line, 2, row_count, second_columns)] * 4,
            *[held(line, row_count, first_columns)] * 4,
            held(row_count, second_columns), held(row_count, second_columns),
            DMA((10,)), DMA((2, count)), *[DMA((max(2, PIECES), count))] * 2, *[DMA((PIECES, count))] * 2,
            DMA((4, count)), DMA((count,)),
            DMA((2 * line,)), DMA((2 * line,)), DMA((5, line)), DMA((5, line)), DMA((1,)), DMA((1,)),
        ],
        compiler_params=pltpu.CompilerParams(collective_id=2, has_side_effects=True, vmem_limit_bytes=63 * 2**20),
    )(
        cache_lengths, queries, key_cache, value_cache, new_key, new_value,
        hidden_in, norm_gain, router_turned, ids_turned, gate_train, up_train, down_rows,
    )


def local(
    queries,
    key_cache,
    value_cache,
    new_key,
    new_value,
    cache_lengths,
    hidden_in,
    norm_gain,
    router_weight,
    expert_ids,
    gate_train,
    up_train,
    down_train,
):
    width = hidden_in.shape[1]
    expert_count = router_weight.shape[1]
    groups = lax.axis_size("groups")
    if dims_fit(groups, expert_count, gate_train, down_train, hidden_in.shape[0]) and queries.shape[0] == 8:
        return tuple(fused(
            queries, key_cache, value_cache, new_key, new_value, cache_lengths,
            hidden_in, norm_gain, router_weight, expert_ids, gate_train, up_train, down_train,
        ))
    normed = rms_normed(hidden_in, norm_gain)
    mixing = dense_mixing(normed, router_weight, expert_ids)
    mixing_high = mixing.astype(jnp.bfloat16)
    mixing_low = (mixing - mixing_high.astype(jnp.float32)).astype(jnp.bfloat16)
    spare = -2 * expert_count % 128
    row_block = jnp.concatenate(
        [normed, mixing_high, mixing_low, jnp.zeros((normed.shape[0], spare), jnp.bfloat16)], axis=1
    )
    hidden_units, down_moved = move(groups, gate_train, up_train, down_train, row_block)
    down_moved = down_moved.reshape(-1, width)
    attended = attend(queries, key_cache, value_cache, new_key, new_value, cache_lengths)
    partial_out = jnp.dot(hidden_units, down_moved, preferred_element_type=jnp.float32).astype(jnp.bfloat16)
    mixed_out = summed(partial_out, expert_count)
    return (attended, mixed_out)


def solution(mesh):
    placed = (
        P(("groups", "expert"), None),
        P(("groups", "expert"), None, None),
        P(("groups", "expert"), None, None),
        P(("groups", "expert"), None),
        P(("groups", "expert"), None),
        P(("groups", "expert")),
        P(("groups", "expert"), None),
        P(),
        P(),
        P(("groups", "expert"), None),
        P(None, "expert", None),
        P(None, "expert", None),
        P(None, "expert", None),
    )
    return jax.shard_map(
        local,
        mesh=mesh,
        in_specs=placed,
        out_specs=(P(("groups", "expert"), None), P(("groups", "expert"), None)),
        check_vma=False,
    )
```
